32 devices in a mesh: rep: 2 (over z, core), dp: 16 (over x, y).
Axes of the slice: x: 4, y: 4, z: 1, core: 2. Of those that a mesh axis runs over, the one named last changes fastest.
The devices are a block of a 4x4x8 slice.
Arguments:
- g_w_gate: bfloat16 [32, 2, 1536, 4096], P(('rep', 'dp')), parts along dimension 0
- g_w_up: bfloat16 [32, 2, 1536, 4096], P(('rep', 'dp')), parts along dimension 0
- g_w_down: bfloat16 [32, 2, 4096, 1536], P(('rep', 'dp')), parts along dimension 0
- w_gate: bfloat16 [2, 1536, 4096], replicated
- w_up: bfloat16 [2, 1536, 4096], replicated
- w_down: bfloat16 [2, 4096, 1536], replicated
- m_w_gate: float32 [2, 1536, 4096], P(None, 'dp')
- m_w_up: float32 [2, 1536, 4096], P(None, 'dp')
- m_w_down: float32 [2, 4096, 1536], P(None, 'dp')
- v_w_gate: float32 [2, 1536, 4096], P(None, 'dp')
- v_w_up: float32 [2, 1536, 4096], P(None, 'dp')
- v_w_down: float32 [2, 4096, 1536], P(None, 'dp')
Outputs:
- output 1: bfloat16 [4, 1536, 4096], P('rep'), parts along dimension 0
- output 2: bfloat16 [4, 1536, 4096], P('rep'), parts along dimension 0
- output 3: bfloat16 [4, 4096, 1536], P('rep'), parts along dimension 0
- output 4: float32 [4, 1536, 4096], P('rep', 'dp'), parts along dimension 0
- output 5: float32 [4, 1536, 4096], P('rep', 'dp'), parts along dimension 0
- output 6: float32 [4, 4096, 1536], P('rep', 'dp'), parts along dimension 0
- output 7: float32 [4, 1536, 4096], P('rep', 'dp'), parts along dimension 0
- output 8: float32 [4, 1536, 4096], P('rep', 'dp'), parts along dimension 0
- output 9: float32 [4, 4096, 1536], P('rep', 'dp'), parts along dimension 0
There are 2 independent parts. The reference program is written for one: setup_inputs(seed, part) draws one part's arguments, and reference() takes and returns one part's arrays. A program takes and returns all parts, laid end to end along the dimension named above; an argument that names none is the same for every part.
All inputs are finite; a program needn't handle non-finite values.
Results may differ from the reference program's by a relative error of at most 0.022.
Values are sent between devices in bfloat16 or wider.
A program may use at most 768 MiB of HBM per device.

```python
import jax
import jax.numpy as jnp
from jax import lax

DEVICES = 16
D = 1536
FF = 4096
LAYERS = 2
NAMES = ("w_gate", "w_up", "w_down")
SHAPES = {"w_gate": (LAYERS, D, FF), "w_up": (LAYERS, D, FF), "w_down": (LAYERS, FF, D)}


def setup_inputs(seed: int = 0, part: int = 0) -> dict:
    kz, *keys = jax.random.split(jax.random.key(seed), 1 + 5 * len(NAMES))
    loud = 2.0 ** jax.random.uniform(kz, (), jnp.float32, -1.0, 1.0)
    drawn = {}
    for name, key, both in zip(NAMES, keys[:3], keys[3:6], strict=True):
        own = jax.random.normal(jax.random.fold_in(key, part), (DEVICES, *SHAPES[name]), jnp.float32)
        shared = jax.random.normal(jax.random.fold_in(both, part), SHAPES[name], jnp.float32)
        drawn["g_" + name] = (loud * (0.7 * shared / DEVICES + 0.7 * own * DEVICES**-0.5)).astype(jnp.bfloat16)
    for name, key in zip(NAMES, keys[6:9], strict=True):
        drawn[name] = (jax.random.normal(key, SHAPES[name], jnp.float32) * SHAPES[name][1] ** -0.5).astype(jnp.bfloat16)
    for name, key in zip(NAMES, keys[9:12], strict=True):
        drawn["m_" + name] = loud * 0.5 * jax.random.normal(key, SHAPES[name], jnp.float32)
    for name, key in zip(NAMES, keys[12:15], strict=True):
        drawn["v_" + name] = loud * loud * jax.random.uniform(key, SHAPES[name], jnp.float32, 0.5, 1.5)
    return drawn


def adamw(w, m, v, g):
    m = 0.9 * m + 0.1 * g
    v = 0.95 * v + 0.05 * g * g
    step = m * lax.rsqrt(v + 1e-8) + 0.1 * w
    return (w - 0.02 * step).astype(jnp.bfloat16), m, v


def reference(g_w_gate, g_w_up, g_w_down, w_gate, w_up, w_down, m_w_gate, m_w_up, m_w_down, v_w_gate, v_w_up, v_w_down):
    def total(terms):
        return lax.scan(lambda so_far, term: (so_far + term.astype(jnp.float32), None), jnp.zeros(terms.shape[1:], jnp.float32), terms)[0]

    gradients = [total(terms).astype(jnp.bfloat16).astype(jnp.float32) for terms in (g_w_gate, g_w_up, g_w_down)]
    new = [
        adamw(w.astype(jnp.float32), m, v, g)
        for w, m, v, g in zip((w_gate, w_up, w_down), (m_w_gate, m_w_up, m_w_down), (v_w_gate, v_w_up, v_w_down), gradients, strict=True)
    ]
    return tuple(one[which] for which in range(3) for one in new)
```

```python
import functools
import math

import jax
import jax.numpy as jnp
from jax import lax
from jax.experimental import pallas as pl
from jax.experimental.pallas import tpu as pltpu
from jax.sharding import PartitionSpec as P

MESH = pl.DeviceIdType.MESH
LANES, SUBLANES = 128, 8
COLOURS = 4
CHUNK = 128


def flat(a):
    *lead, rows, columns = a.shape
    a = a.reshape(*lead, rows // SUBLANES, SUBLANES, columns // LANES, LANES)
    return jnp.swapaxes(a, -3, -2).reshape(*lead, rows * columns // LANES, LANES)


def unflat(a, rows, columns):
    *lead, _, _ = a.shape
    a = a.reshape(*lead, rows // SUBLANES, columns // LANES, SUBLANES, LANES)
    return jnp.swapaxes(a, -3, -2).reshape(*lead, rows, columns)


def moments(m, v, g):
    return 0.9 * m + 0.1 * g, 0.95 * v + 0.05 * g * g


def new_weight(w, m, v):
    step = m * lax.rsqrt(v + 1e-8) + 0.1 * w
    return (w - 0.02 * step).astype(jnp.bfloat16)


def direction(k):
    return (1 if k % 2 == 0 else -1), k // 2


def place(side):
    me = lax.axis_index("dp")
    return lax.div(me, side), lax.rem(me, side)


def at(k, first, second):
    return (first, second) if direction(k)[1] == 0 else (second, first)


def comm_kernel(side, layers, units, kept, *refs):
    weights = units // layers
    grads, olds, ms, vs = (refs[i * weights : (i + 1) * weights] for i in range(4))
    refs = refs[4 * weights :]
    x_ref, refs = refs[0], refs[1:]
    chunks = (units - kept) // layers
    zs, refs = refs[: chunks * COLOURS], refs[chunks * COLOURS :]
    gs, refs = refs[:weights], refs[weights:]
    (land1, land2, got, own, out1, in2, out2, old_v, m_v, v_v, out_w, out_g, send_sem, recv_sem, load_sem, store_sem) = refs
    rows = got.shape[2]
    last = side - 1
    xy = place(side)

    def turn(k, axis, by):
        way, first = direction(k)
        c = xy[first if axis == 0 else 1 - first]
        return lax.rem(c + way * by + 4 * side, side)

    def neighbour(k, axis):
        a, b = turn(k, 0, 1 if axis == 0 else 0), turn(k, 1, 1 if axis == 1 else 0)
        px, py = at(k, a, b)
        return {"dp": px * side + py}

    barrier = pltpu.get_barrier_semaphore()
    for k in range(COLOURS):
        pl.semaphore_signal(barrier, inc=1, device_id=neighbour(k, 0), device_id_type=MESH)
    pl.semaphore_wait(barrier, COLOURS)

    def of_weight(u, f):
        for w in range(weights):
            pl.when(lax.div(u, layers) == w)(functools.partial(f, w, lax.rem(u, layers)))

    def group(ref, lead, k, first):
        if direction(k)[1] == 0:
            return ref.at[lead, first, :, k]
        return ref.at[lead, :, first, k]

    def block(ref, lead, k, first, second):
        px, py = at(k, first, second)
        return ref.at[lead, px, py, k]

    def remote(stage, u, k, src, dst, axis):
        return pltpu.make_async_remote_copy(
            src_ref=src,
            dst_ref=dst,
            send_sem=send_sem.at[stage, lax.rem(u, 2), k],
            recv_sem=recv_sem.at[stage, u, k],
            device_id=neighbour(k, axis),
            device_id_type=MESH,
        )

    n1, n2 = last, last
    FIRST, SECOND, STEP = 0, n1, n1 + n2
    GATHER2, GATHER1 = STEP, STEP + n2
    stages = GATHER1 + n1

    def dst_of(stage, u, k):
        if stage < SECOND:
            return land1.at[u, k, stage - FIRST]
        if stage < STEP:
            return land2.at[u, k, stage - SECOND]
        raise AssertionError

    def wait_recv(stage, u, k):
        if stage < STEP:
            dst = dst_of(stage, u, k)
        elif stage < GATHER1:
            dst = block(x_ref, u, k, turn(k, 0, 0), turn(k, 1, -(stage - GATHER2) - 1))
        else:
            dst = group(x_ref, u, k, turn(k, 0, -(stage - GATHER1) - 1))
        remote(stage, u, k, dst, dst, 0).wait_recv()

    def wait_send(stage, u, k):
        small = SECOND <= stage < GATHER1
        ref = land2.at[0, k, 0] if small else land1.at[0, k, 0]
        remote(stage, u, k, ref, ref, 0).wait_send()

    def free(stage, u, k):
        pl.when(u >= 2)(lambda: wait_send(stage, u, k))

    def load(k, i, src, dst):
        return pltpu.make_async_copy(src, dst, load_sem.at[i, k])

    def stage_first(s, u):
        ks = range(COLOURS)
        if s == 0:
            def start(k, w, layer):
                remote(FIRST, u, k, group(grads[w], layer, k, turn(k, 0, -1)), land1.at[u, k, 0], 0).start()

            for k in ks:
                free(FIRST, u, k)
            def start_all(w, layer):
                for k in ks:
                    start(k, w, layer)
            of_weight(u, start_all)
            return

        def load_own(w, layer):
            for k in ks:
                load(k, 0, group(grads[w], layer, k, turn(k, 0, -1 - s)), own.at[k]).start()

        of_weight(u, load_own)
        for k in ks:
            wait_recv(FIRST + s - 1, u, k)
            load(k, 1, land1.at[u, k, s - 1], got.at[k]).start()
        slot = lax.rem(u, 2)
        for k in ks:
            free(FIRST + s, u, k)
            load(k, 0, land1.at[u, k, s - 1], own.at[k]).wait()
            load(k, 1, land1.at[u, k, s - 1], got.at[k]).wait()
            out = out1.at[s - 1, slot, k]
            per = rows // CHUNK

            def add(c, _):
                j, r = lax.div(c, per), pl.multiple_of(lax.rem(c, per) * CHUNK, CHUNK)
                total = got[k, j, pl.ds(r, CHUNK)].astype(jnp.float32) + own[k, j, pl.ds(r, CHUNK)].astype(jnp.float32)
                out[j, pl.ds(r, CHUNK)] = total.astype(jnp.bfloat16)
                return 0

            lax.fori_loop(0, side * per, add, 0)
            remote(FIRST + s, u, k, out, land1.at[u, k, s], 0).start()

    def load_second(s, u):
        ks = range(COLOURS)

        def load_own(w, layer):
            for k in ks:
                load(k, 0, block(grads[w], layer, k, turn(k, 0, 0), turn(k, 1, -1 - s)), in2.at[0, k]).start()

        of_weight(u, load_own)
        for k in ks:
            wait_recv(SECOND + s - 1, u, k)
            load(k, 1, land1.at[u, k, n1 - 1, turn(k, 1, -1 - s)], in2.at[1, k]).start()
            if s > 0:
                load(k, 2, land2.at[u, k, s - 1], in2.at[2, k]).start()

    def wait_second(s, k):
        for i in range(3 if s > 0 else 2):
            load(k, i, land2.at[0, k, 0], in2.at[i, k]).wait()

    def sum_second(s, k, r):
        total = in2[1, k, pl.ds(r, CHUNK)].astype(jnp.float32) + in2[0, k, pl.ds(r, CHUNK)].astype(jnp.float32)
        if s > 0:
            total += in2[2, k, pl.ds(r, CHUNK)].astype(jnp.float32)
        return total.astype(jnp.bfloat16)

    def stage_second(s, u):
        load_second(s, u)
        slot = lax.rem(u, 2)
        for k in range(COLOURS):
            free(SECOND + s, u, k)
            wait_second(s, k)
            out = out2.at[s, slot, k]

            def add(c, _):
                r = pl.multiple_of(c * CHUNK, CHUNK)
                out[pl.ds(r, CHUNK)] = sum_second(s, k, r)
                return 0

            lax.fori_loop(0, rows // CHUNK, add, 0)
            remote(SECOND + s, u, k, out, land2.at[u, k, s], 1).start()

    def store_w(k, u, slot):
        return pltpu.make_async_copy(out_w.at[slot, k], block(x_ref, u, k, turn(k, 0, 0), turn(k, 1, 0)), store_sem.at[0, slot, k])

    def store_g(k, slot, w, layer):
        return pltpu.make_async_copy(out_g.at[slot, k], gs[w].at[layer, k], store_sem.at[1, slot, k])

    def stage_step(u):
        ks = range(COLOURS)

        def load_state(w, layer):
            for k in ks:
                load(k, 3, block(olds[w], layer, k, turn(k, 0, 0), turn(k, 1, 0)), old_v.at[k]).start()
                load(k, 4, ms[w].at[layer, k], m_v.at[k]).start()
                load(k, 5, vs[w].at[layer, k], v_v.at[k]).start()

        of_weight(u, load_state)
        load_second(n2, u)
        slot = lax.rem(u, 2)
        for k in ks:
            free(GATHER2, u, k)

            pl.when(u >= 2)(lambda: store_g(k, slot, 0, 0).wait())

            wait_second(n2, k)
            load(k, 3, old_v.at[k], old_v.at[k]).wait()
            load(k, 4, m_v.at[k], m_v.at[k]).wait()
            load(k, 5, v_v.at[k], v_v.at[k]).wait()

            def adamw(c, _):
                r = pl.multiple_of(c * CHUNK, CHUNK)
                here = pl.ds(r, CHUNK)
                g = sum_second(n2, k, r)
                m, v = moments(m_v[k, here], v_v[k, here], g.astype(jnp.float32))
                out_w[slot, k, here] = new_weight(old_v[k, here].astype(jnp.float32), m, v)
                out_g[slot, k, here] = g
                return 0

            lax.fori_loop(0, rows // CHUNK, adamw, 0)
            remote(GATHER2, u, k, out_w.at[slot, k], block(x_ref, u, k, turn(k, 0, 0), turn(k, 1, 0)), 1).start()
            store_w(k, u, slot).start()

        def store_all(w, layer):
            for k in ks:
                store_g(k, slot, w, layer).start()

        of_weight(u, store_all)

    def stage_gather2(s, u):
        for k in range(COLOURS):
            if s == 1:
                store_w(k, u, lax.rem(u, 2)).wait()
            wait_recv(GATHER2 + s - 1, u, k)
            free(GATHER2 + s, u, k)
            it = block(x_ref, u, k, turn(k, 0, 0), turn(k, 1, -s))
            remote(GATHER2 + s, u, k, it, it, 1).start()

    def stage_gather1(s, u):
        for k in range(COLOURS):
            wait_recv(GATHER1 + s - 1, u, k)
            free(GATHER1 + s, u, k)
            it = group(x_ref, u, k, turn(k, 0, -s))
            if s == n1 - 2:
                pl.when(u < kept)(lambda: remote(GATHER1 + s, u, k, it, it, 0).start())
                for c in range(chunks):
                    z = zs[c * COLOURS + k]
                    pl.when(lax.div(u, layers) == kept // layers + c)(
                        lambda: remote(GATHER1 + s, u, k, it, z.at[lax.rem(u, layers)], 0).start()
                    )
            else:
                remote(GATHER1 + s, u, k, it, it, 0).start()

    def body(i, _):
        for s in range(stages):
            u = i - s
            count = kept if s == stages - 1 else units
            run = (
                functools.partial(stage_first, s, u)
                if s < SECOND
                else functools.partial(stage_second, s - SECOND, u)
                if s < STEP
                else functools.partial(stage_step, u)
                if s == GATHER2
                else functools.partial(stage_gather2, s - GATHER2, u)
                if s < GATHER1
                else functools.partial(stage_gather1, s - GATHER1, u)
            )
            pl.when((u >= 0) & (u < count))(run)
        return 0

    lax.fori_loop(0, stages - 1 + units, body, 0)

    def drain(u, _):
        for k in range(COLOURS):
            pl.when(u >= kept)(lambda: wait_recv(stages - 2, u, k))
            pl.when(u < kept)(lambda: wait_recv(stages - 1, u, k))
        return 0

    lax.fori_loop(0, units, drain, 0)
    for s in range(stages):
        count = kept if s == stages - 1 else units
        for u in range(max(count - 2, 0), count):
            for k in range(COLOURS):
                wait_send(s, u, k)
    for u in range(max(units - 2, 0), units):
        for k in range(COLOURS):
            store_g(k, u % 2, 0, 0).wait()


def communicate(side, grads, olds, ms, vs, kept):
    layers = grads[0].shape[0]
    weights = len(grads)
    units = weights * layers
    rows = grads[0].shape[-2]
    hops = side - 1
    chunks = (units - kept) // layers
    any_space = pl.BlockSpec(memory_space=pl.ANY)
    bf16, f32 = jnp.bfloat16, jnp.float32
    shape = jax.ShapeDtypeStruct
    outs = [
        shape((units, *grads[0].shape[1:]), bf16),
        *[shape((layers, side, rows, LANES), bf16)] * (chunks * COLOURS),
        *[shape((layers, COLOURS, rows, LANES), bf16)] * weights,
        shape((units, COLOURS, hops, side, rows, LANES), bf16),
        shape((units, COLOURS, hops, rows, LANES), bf16),
    ]
    stages = 4 * hops
    scratch = [
        pltpu.VMEM((COLOURS, side, rows, LANES), bf16),
        pltpu.VMEM((COLOURS, side, rows, LANES), bf16),
        pltpu.VMEM((hops - 1, 2, COLOURS, side, rows, LANES), bf16),
        pltpu.VMEM((3, COLOURS, rows, LANES), bf16),
        pltpu.VMEM((hops, 2, COLOURS, rows, LANES), bf16),
        pltpu.VMEM((COLOURS, rows, LANES), bf16),
        pltpu.VMEM((COLOURS, rows, LANES), f32),
        pltpu.VMEM((COLOURS, rows, LANES), f32),
        pltpu.VMEM((2, COLOURS, rows, LANES), bf16),
        pltpu.VMEM((2, COLOURS, rows, LANES), bf16),
        pltpu.SemaphoreType.DMA((stages, 2, COLOURS)),
        pltpu.SemaphoreType.DMA((stages, units, COLOURS)),
        pltpu.SemaphoreType.DMA((6, COLOURS)),
        pltpu.SemaphoreType.DMA((2, 2, COLOURS)),
    ]
    got = pl.pallas_call(
        functools.partial(comm_kernel, side, layers, units, kept),
        out_shape=outs,
        in_specs=[any_space] * (4 * weights),
        out_specs=[any_space] * len(outs),
        scratch_shapes=scratch,
        compiler_params=pltpu.CompilerParams(collective_id=0, has_side_effects=True, vmem_limit_bytes=56 << 20),
        name="sum_step_gather",
    )(*grads, *olds, *ms, *vs)
    x, got = got[0], got[1:]
    zs, got = got[: chunks * COLOURS], got[chunks * COLOURS :]
    return x, [zs[i * COLOURS : (i + 1) * COLOURS] for i in range(chunks)], got[:weights]


SLOTS = 8


def copy_kernel(side, jobs, n_in, *refs):
    ins, out, buf, in_sem, out_sem = refs[:n_in], refs[-4], refs[-3], refs[-2], refs[-1]
    pairs = jobs(ins, out)
    depth = min(SLOTS, len(pairs))

    def into(i):
        return pltpu.make_async_copy(pairs[i][0], buf.at[i % SLOTS], in_sem.at[i % SLOTS])

    def outof(i):
        return pltpu.make_async_copy(buf.at[i % SLOTS], pairs[i][1], out_sem.at[i % SLOTS])

    ahead = SLOTS // 2
    for i in range(len(pairs) + ahead):
        if i < len(pairs):
            if i >= SLOTS:
                outof(i - SLOTS).wait()
            into(i).start()
        if i >= ahead:
            into(i - ahead).wait()
            outof(i - ahead).start()
    for i in range(max(len(pairs) - SLOTS, 0), len(pairs)):
        outof(i).wait()


def copies(side, jobs, ins, shape, rows, onto=None):
    any_space = pl.BlockSpec(memory_space=pl.ANY)
    moved = 2 * 2 * math.prod(shape)
    given = [*ins] + ([] if onto is None else [onto])
    return pl.pallas_call(
        functools.partial(copy_kernel, side, jobs, len(ins)),
        out_shape=jax.ShapeDtypeStruct(shape, jnp.bfloat16),
        in_specs=[any_space] * len(given),
        out_specs=any_space,
        scratch_shapes=[
            pltpu.VMEM((SLOTS, side, rows, LANES), jnp.bfloat16),
            pltpu.SemaphoreType.DMA((SLOTS,)),
            pltpu.SemaphoreType.DMA((SLOTS,)),
        ],
        input_output_aliases={} if onto is None else {len(ins): 0},
        compiler_params=pltpu.CompilerParams(vmem_limit_bytes=16 << 20),
        cost_estimate=pl.CostEstimate(flops=moved, bytes_accessed=moved, transcendentals=0),
        name="place" if onto is None else "place_last",
    )(*given)


def solution(mesh):
    n = mesh.shape["dp"]
    side = math.isqrt(n)
    hops = side - 1

    def ring(k):
        way, axis = direction(k)
        pairs = []
        for i in range(n):
            c = [i // side, i % side]
            c[axis] = (c[axis] + way) % side
            pairs.append((i, c[0] * side + c[1]))
        return pairs

    def step(*arrays):
        terms, weights, m, v = (arrays[i : i + 3] for i in (0, 3, 6, 9))
        layers = m[0].shape[0]
        kept = layers
        rows = m[0].shape[1] * m[0].shape[2] // LANES // COLOURS
        by_block = (layers, side, side, COLOURS, rows, LANES)
        grads = [flat(t[0]).reshape(by_block) for t in terms]
        olds = [flat(w).reshape(by_block) for w in weights]
        own_m, own_v = ([flat(one).reshape(layers, COLOURS, rows, LANES) for one in ones] for ones in (m, v))
        x, zs, sums = communicate(side, grads, olds, own_m, own_v, kept)
        ys = [[lax.ppermute(z, "dp", ring(k)) for k, z in enumerate(chunk)] for chunk in zs]

        new_m, new_v = [], []
        for one_m, one_v, g in zip(m, v, sums, strict=True):
            g = unflat(g.reshape(layers, COLOURS * rows, LANES), *one_m.shape[1:]).astype(jnp.float32)
            a, b = moments(one_m, one_v, g)
            new_m.append(a)
            new_v.append(b)

        def group(ref, lead, k, first):
            return ref.at[lead, first, :, k] if direction(k)[1] == 0 else ref.at[lead, :, first, k]

        def first_of(k, by):
            way, axis = direction(k)
            return lax.rem(place(side)[axis] + way * by + 4 * side, side)

        whole = []
        for i, w in enumerate(weights):
            c = i - kept // layers

            def placed(ins, out, i=i, c=c):
                pairs = []
                for layer in range(layers):
                    for k in range(COLOURS):
                        for back in range(side if c < 0 else hops):
                            first = first_of(k, -back)
                            src = group(ins[0], i * layers + layer, k, first) if c < 0 or back < hops - 1 else ins[1 + k].at[layer]
                            pairs.append((src, group(out, layer, k, first)))
                return pairs

            def last(ins, out):
                return [(ins[k].at[layer], group(out, layer, k, first_of(k, -hops))) for layer in range(layers) for k in range(COLOURS)]

            new = copies(side, placed, [x, *(zs[c] if c >= 0 else [])], by_block, rows)
            if c >= 0:
                new = copies(side, last, ys[c], by_block, rows, onto=new)
            whole.append(unflat(new.reshape(layers, n * COLOURS * rows, LANES), *w.shape[1:]))
        return (*whole, *new_m, *new_v)

    all_of, cut = P(None, None, None), P(None, "dp", None)
    return jax.shard_map(
        step,
        mesh=mesh,
        in_specs=(P(("rep", "dp"), None, None, None),) * 3 + (all_of,) * 3 + (cut,) * 6,
        out_specs=(P("rep", None, None),) * 3 + (P("rep", "dp", None),) * 6,
        check_vma=False,
    )
```

```python
import functools
import math

import jax
import jax.numpy as jnp
from jax import lax
from jax.experimental import pallas as pl
from jax.experimental.pallas import tpu as pltpu
from jax.sharding import PartitionSpec as P

MESH = pl.DeviceIdType.MESH
LANES, SUBLANES = 128, 8
COLOURS = 4
CHUNK = 128


def flat(a):
    *lead, rows, columns = a.shape
    a = a.reshape(*lead, rows // SUBLANES, SUBLANES, columns // LANES, LANES)
    return jnp.swapaxes(a, -3, -2).reshape(*lead, rows * columns // LANES, LANES)


def unflat(a, rows, columns):
    *lead, _, _ = a.shape
    a = a.reshape(*lead, rows // SUBLANES, columns // LANES, SUBLANES, LANES)
    return jnp.swapaxes(a, -3, -2).reshape(*lead, rows, columns)


pinned = pltpu.with_memory_space_constraint


def moments(m, v, g):
    return 0.9 * m + 0.1 * g, 0.95 * v + 0.05 * g * g


def new_weight(w, m, v):
    step = m * lax.rsqrt(v + 1e-8) + 0.1 * w
    return (w - 0.02 * step).astype(jnp.bfloat16)


def direction(k):
    return (1 if k % 2 == 0 else -1), k // 2


def place(side):
    me = lax.axis_index("dp")
    return lax.div(me, side), lax.rem(me, side)


def at(k, first, second):
    return (first, second) if direction(k)[1] == 0 else (second, first)


def comm_kernel(side, layers, units, parts, *refs):
    weights = units // layers
    grads, olds, ms, vs = (refs[i * weights : (i + 1) * weights] for i in range(4))
    refs = refs[4 * weights :]
    x_ref, refs = refs[0], refs[1:]
    kept = units - sum(parts)
    zs, refs = refs[: len(parts) * COLOURS], refs[len(parts) * COLOURS :]
    gs, refs = refs[:weights], refs[weights:]
    (land1, land2, got, own, out1, in2, out2, old_v, m_v, v_v, out_w, out_g, send_sem, recv_sem, load_sem, store_sem) = refs
    rows = got.shape[2]
    last = side - 1
    xy = place(side)

    def turn(k, axis, by):
        way, first = direction(k)
        c = xy[first if axis == 0 else 1 - first]
        return lax.rem(c + way * by + 4 * side, side)

    def neighbour(k, axis):
        a, b = turn(k, 0, 1 if axis == 0 else 0), turn(k, 1, 1 if axis == 1 else 0)
        px, py = at(k, a, b)
        return {"dp": px * side + py}

    pl.when(lax.rem(lax.axis_index("rep"), 2) == 1)(lambda: pl.delay(DELAY))
    barrier = pltpu.get_barrier_semaphore()
    for k in range(COLOURS):
        pl.semaphore_signal(barrier, inc=1, device_id=neighbour(k, 0), device_id_type=MESH)
    pl.semaphore_wait(barrier, COLOURS)

    def of_weight(u, f):
        for w in range(weights):
            pl.when(lax.div(u, layers) == w)(functools.partial(f, w, lax.rem(u, layers)))

    def group(ref, lead, k, first):
        if direction(k)[1] == 0:
            return ref.at[lead, first, :, k]
        return ref.at[lead, :, first, k]

    def block(ref, lead, k, first, second):
        px, py = at(k, first, second)
        return ref.at[lead, px, py, k]

    def remote(stage, u, k, src, dst, axis):
        return pltpu.make_async_remote_copy(
            src_ref=src,
            dst_ref=dst,
            send_sem=send_sem.at[stage, lax.rem(u, 2), k],
            recv_sem=recv_sem.at[stage, u, k],
            device_id=neighbour(k, axis),
            device_id_type=MESH,
        )

    n1, n2 = last, last
    FIRST, SECOND, STEP = 0, n1, n1 + n2
    GATHER2, GATHER1 = STEP, STEP + n2
    stages = GATHER1 + n1

    def dst_of(stage, u, k):
        if stage < SECOND:
            return land1.at[u, k, stage - FIRST]
        if stage < STEP:
            return land2.at[u, k, stage - SECOND]
        raise AssertionError

    def wait_recv(stage, u, k):
        if stage < STEP:
            dst = dst_of(stage, u, k)
        elif stage < GATHER1:
            dst = block(x_ref, u, k, turn(k, 0, 0), turn(k, 1, -(stage - GATHER2) - 1))
        else:
            dst = group(x_ref, u, k, turn(k, 0, -(stage - GATHER1) - 1))
        remote(stage, u, k, dst, dst, 0).wait_recv()

    def wait_send(stage, u, k):
        small = SECOND <= stage < GATHER1
        ref = land2.at[0, k, 0] if small else land1.at[0, k, 0]
        remote(stage, u, k, ref, ref, 0).wait_send()

    def free(stage, u, k):
        pl.when(u >= 2)(lambda: wait_send(stage, u, k))

    def load(k, i, src, dst):
        return pltpu.make_async_copy(src, dst, load_sem.at[i, k])

    def stage_first(s, u):
        ks = range(COLOURS)
        if s == 0:
            def start(k, w, layer):
                remote(FIRST, u, k, group(grads[w], layer, k, turn(k, 0, -1)), land1.at[u, k, 0], 0).start()

            for k in ks:
                free(FIRST, u, k)
            def start_all(w, layer):
                for k in ks:
                    start(k, w, layer)
            of_weight(u, start_all)
            return

        def load_own(w, layer):
            for k in ks:
                load(k, 0, group(grads[w], layer, k, turn(k, 0, -1 - s)), own.at[k]).start()

        of_weight(u, load_own)
        for k in ks:
            wait_recv(FIRST + s - 1, u, k)
            load(k, 1, land1.at[u, k, s - 1], got.at[k]).start()
        slot = lax.rem(u, 2)
        for k in ks:
            free(FIRST + s, u, k)
            load(k, 0, land1.at[u, k, s - 1], own.at[k]).wait()
            load(k, 1, land1.at[u, k, s - 1], got.at[k]).wait()
            out = out1.at[s - 1, slot, k]
            per = rows // CHUNK

            def add(c, _):
                j, r = lax.div(c, per), pl.multiple_of(lax.rem(c, per) * CHUNK, CHUNK)
                total = got[k, j, pl.ds(r, CHUNK)].astype(jnp.float32) + own[k, j, pl.ds(r, CHUNK)].astype(jnp.float32)
                out[j, pl.ds(r, CHUNK)] = total.astype(jnp.bfloat16)
                return 0

            lax.fori_loop(0, side * per, add, 0)
            remote(FIRST + s, u, k, out, land1.at[u, k, s], 0).start()

    def load_second(s, u):
        ks = range(COLOURS)

        def load_own(w, layer):
            for k in ks:
                load(k, 0, block(grads[w], layer, k, turn(k, 0, 0), turn(k, 1, -1 - s)), in2.at[0, k]).start()

        of_weight(u, load_own)
        for k in ks:
            wait_recv(SECOND + s - 1, u, k)
            load(k, 1, land1.at[u, k, n1 - 1, turn(k, 1, -1 - s)], in2.at[1, k]).start()
            if s > 0:
                load(k, 2, land2.at[u, k, s - 1], in2.at[2, k]).start()

    def wait_second(s, k):
        for i in range(3 if s > 0 else 2):
            load(k, i, land2.at[0, k, 0], in2.at[i, k]).wait()

    def sum_second(s, k, r):
        total = in2[1, k, pl.ds(r, CHUNK)].astype(jnp.float32) + in2[0, k, pl.ds(r, CHUNK)].astype(jnp.float32)
        if s > 0:
            total += in2[2, k, pl.ds(r, CHUNK)].astype(jnp.float32)
        return total.astype(jnp.bfloat16)

    def stage_second(s, u):
        load_second(s, u)
        slot = lax.rem(u, 2)
        for k in range(COLOURS):
            free(SECOND + s, u, k)
            wait_second(s, k)
            out = out2.at[s, slot, k]

            def add(c, _):
                r = pl.multiple_of(c * CHUNK, CHUNK)
                out[pl.ds(r, CHUNK)] = sum_second(s, k, r)
                return 0

            lax.fori_loop(0, rows // CHUNK, add, 0)
            remote(SECOND + s, u, k, out, land2.at[u, k, s], 1).start()

    def store_w(k, u, slot):
        return pltpu.make_async_copy(out_w.at[slot, k], block(x_ref, u, k, turn(k, 0, 0), turn(k, 1, 0)), store_sem.at[0, slot, k])

    def store_g(k, slot, w, layer):
        return pltpu.make_async_copy(out_g.at[slot, k], gs[w].at[layer, k], store_sem.at[1, slot, k])

    def stage_step(u):
        ks = range(COLOURS)

        def load_state(w, layer):
            for k in ks:
                load(k, 3, block(olds[w], layer, k, turn(k, 0, 0), turn(k, 1, 0)), old_v.at[k]).start()
                load(k, 4, ms[w].at[layer, k], m_v.at[k]).start()
                load(k, 5, vs[w].at[layer, k], v_v.at[k]).start()

        of_weight(u, load_state)
        load_second(n2, u)
        slot = lax.rem(u, 2)
        for k in ks:
            free(GATHER2, u, k)

            pl.when(u >= 2)(lambda: store_g(k, slot, 0, 0).wait())

            wait_second(n2, k)
            load(k, 3, old_v.at[k], old_v.at[k]).wait()
            load(k, 4, m_v.at[k], m_v.at[k]).wait()
            load(k, 5, v_v.at[k], v_v.at[k]).wait()

            def adamw(c, _):
                r = pl.multiple_of(c * CHUNK, CHUNK)
                here = pl.ds(r, CHUNK)
                g = sum_second(n2, k, r)
                m, v = moments(m_v[k, here], v_v[k, here], g.astype(jnp.float32))
                out_w[slot, k, here] = new_weight(old_v[k, here].astype(jnp.float32), m, v)
                out_g[slot, k, here] = g
                return 0

            lax.fori_loop(0, rows // CHUNK, adamw, 0)
            remote(GATHER2, u, k, out_w.at[slot, k], block(x_ref, u, k, turn(k, 0, 0), turn(k, 1, 0)), 1).start()
            store_w(k, u, slot).start()

        def store_all(w, layer):
            for k in ks:
                store_g(k, slot, w, layer).start()

        of_weight(u, store_all)

    def stage_gather2(s, u):
        for k in range(COLOURS):
            if s == 1:
                store_w(k, u, lax.rem(u, 2)).wait()
            wait_recv(GATHER2 + s - 1, u, k)
            free(GATHER2 + s, u, k)
            it = block(x_ref, u, k, turn(k, 0, 0), turn(k, 1, -s))
            remote(GATHER2 + s, u, k, it, it, 1).start()

    def stage_gather1(s, u):
        for k in range(COLOURS):
            wait_recv(GATHER1 + s - 1, u, k)
            free(GATHER1 + s, u, k)
            it = group(x_ref, u, k, turn(k, 0, -s))
            if s == n1 - 2:
                pl.when(u < kept)(lambda: remote(GATHER1 + s, u, k, it, it, 0).start())
                for p, count in enumerate(parts):
                    z, begin = zs[p * COLOURS + k], kept + sum(parts[:p])
                    pl.when((u >= begin) & (u < begin + count))(
                        lambda: remote(GATHER1 + s, u, k, it, z.at[u - begin], 0).start()
                    )
            else:
                remote(GATHER1 + s, u, k, it, it, 0).start()

    def body(i, _):
        for s in range(stages):
            u = i - s
            count = kept if s == stages - 1 else units
            run = (
                functools.partial(stage_first, s, u)
                if s < SECOND
                else functools.partial(stage_second, s - SECOND, u)
                if s < STEP
                else functools.partial(stage_step, u)
                if s == GATHER2
                else functools.partial(stage_gather2, s - GATHER2, u)
                if s < GATHER1
                else functools.partial(stage_gather1, s - GATHER1, u)
            )
            pl.when((u >= 0) & (u < count))(run)
        return 0

    lax.fori_loop(0, stages - 1 + (units if kept == units else max(units - 1, kept)), body, 0)

    def drain(u, _):
        for k in range(COLOURS):
            pl.when(u >= kept)(lambda: wait_recv(stages - 2, u, k))
            pl.when(u < kept)(lambda: wait_recv(stages - 1, u, k))
        return 0

    lax.fori_loop(0, units, drain, 0)
    for s in range(stages):
        count = kept if s == stages - 1 else units
        for u in range(max(count - 2, 0), count):
            for k in range(COLOURS):
                wait_send(s, u, k)
    for u in range(max(units - 2, 0), units):
        for k in range(COLOURS):
            store_g(k, u % 2, 0, 0).wait()


def communicate(side, grads, olds, ms, vs, parts):
    layers = grads[0].shape[0]
    weights = len(grads)
    units = weights * layers
    rows = grads[0].shape[-2]
    hops = side - 1
    hbm = pl.BlockSpec(memory_space=pltpu.HBM)
    bf16, f32 = jnp.bfloat16, jnp.float32
    shape = pltpu.HBM
    outs = [
        shape((units, *grads[0].shape[1:]), bf16),
        *[shape((count, side, rows, LANES), bf16) for count in parts for _ in range(COLOURS)],
        *[shape((layers, COLOURS, rows, LANES), bf16)] * weights,
        shape((units, COLOURS, hops, side, rows, LANES), bf16),
        shape((units, COLOURS, hops, rows, LANES), bf16),
    ]
    stages = 4 * hops
    scratch = [
        pltpu.VMEM((COLOURS, side, rows, LANES), bf16),
        pltpu.VMEM((COLOURS, side, rows, LANES), bf16),
        pltpu.VMEM((hops - 1, 2, COLOURS, side, rows, LANES), bf16),
        pltpu.VMEM((3, COLOURS, rows, LANES), bf16),
        pltpu.VMEM((hops, 2, COLOURS, rows, LANES), bf16),
        pltpu.VMEM((COLOURS, rows, LANES), bf16),
        pltpu.VMEM((COLOURS, rows, LANES), f32),
        pltpu.VMEM((COLOURS, rows, LANES), f32),
        pltpu.VMEM((2, COLOURS, rows, LANES), bf16),
        pltpu.VMEM((2, COLOURS, rows, LANES), bf16),
        pltpu.SemaphoreType.DMA((stages, 2, COLOURS)),
        pltpu.SemaphoreType.DMA((stages, units, COLOURS)),
        pltpu.SemaphoreType.DMA((6, COLOURS)),
        pltpu.SemaphoreType.DMA((2, 2, COLOURS)),
    ]
    got = pl.pallas_call(
        functools.partial(comm_kernel, side, layers, units, parts),
        out_shape=outs,
        in_specs=[hbm] * (4 * weights),
        out_specs=[hbm] * len(outs),
        scratch_shapes=scratch,
        compiler_params=pltpu.CompilerParams(collective_id=0, has_side_effects=True, vmem_limit_bytes=60 << 20),
        name="sum_step_gather",
    )(*(pinned(a, pltpu.HBM) for a in (*grads, *olds, *ms, *vs)))
    x, got = got[0], got[1:]
    zs, got = got[: len(parts) * COLOURS], got[len(parts) * COLOURS :]
    return x, [zs[i * COLOURS : (i + 1) * COLOURS] for i in range(len(parts))], got[:weights]


SLOTS = 16


def copy_kernel(jobs, n_in, *refs):
    ins, (out, buf, in_sem, out_sem, straight_sem) = refs[:n_in], refs[-5:]
    pairs = jobs(ins, out)
    staged = [pair for pair in pairs if pair[2]]
    straight = [pltpu.make_async_copy(src, dst, straight_sem.at[i]) for i, (src, dst, _) in enumerate(p for p in pairs if not p[2])]

    def into(i):
        return pltpu.make_async_copy(staged[i][0], buf.at[i % SLOTS], in_sem.at[i % SLOTS])

    def outof(i):
        return pltpu.make_async_copy(buf.at[i % SLOTS], staged[i][1], out_sem.at[i % SLOTS])

    ahead = SLOTS // 2
    for copy in straight:
        copy.start()
    for i in range(len(staged) + ahead):
        if i < len(staged):
            if i >= SLOTS:
                outof(i - SLOTS).wait()
            into(i).start()
        if ahead <= i:
            into(i - ahead).wait()
            outof(i - ahead).start()
    for i in range(max(len(staged) - SLOTS, 0), len(staged)):
        outof(i).wait()
    for copy in straight:
        copy.wait()


def copies(jobs, ins, space, shape, moved, onto=None):
    hbm = pl.BlockSpec(memory_space=pltpu.HBM)
    side, rows = shape[1], shape[-2]
    given = [pinned(a, space) for a in ins] + ([] if onto is None else [pinned(onto, pltpu.HBM)])
    return pl.pallas_call(
        functools.partial(copy_kernel, jobs, len(ins)),
        out_shape=pltpu.HBM(shape, jnp.bfloat16),
        in_specs=[pl.BlockSpec(memory_space=space)] * len(ins) + [hbm] * (onto is not None),
        out_specs=hbm,
        scratch_shapes=[
            pltpu.VMEM((SLOTS if onto is None else 1, side, rows, LANES), jnp.bfloat16),
            pltpu.SemaphoreType.DMA((SLOTS,)),
            pltpu.SemaphoreType.DMA((SLOTS,)),
            pltpu.SemaphoreType.DMA((SLOTS,)),
        ],
        input_output_aliases={} if onto is None else {len(ins): 0},
        compiler_params=pltpu.CompilerParams(vmem_limit_bytes=(16 if onto is None else 8) << 20),
        cost_estimate=pl.CostEstimate(flops=4 * moved, bytes_accessed=4 * moved, transcendentals=0),
        name="place" if onto is None else "place_last",
    )(*given)


PARTS = (4, 2)
DELAY = 16000


def solution(mesh):
    n = mesh.shape["dp"]
    side = math.isqrt(n)
    hops = side - 1

    def ring(k):
        way, axis = direction(k)
        pairs = []
        for i in range(n):
            c = [i // side, i % side]
            c[axis] = (c[axis] + way) % side
            pairs.append((i, c[0] * side + c[1]))
        return pairs

    def group(ref, lead, k, back):
        way, axis = direction(k)
        first = lax.rem(place(side)[axis] - way * back + 4 * side, side)
        return ref.at[lead, first, :, k] if axis == 0 else ref.at[lead, :, first, k]

    def step(*arrays):
        terms, weights, m, v = (arrays[i : i + 3] for i in (0, 3, 6, 9))
        layers = m[0].shape[0]
        units = layers * len(m)
        rows = m[0].shape[1] * m[0].shape[2] // LANES // COLOURS
        by_block = (layers, side, side, COLOURS, rows, LANES)
        grads = [flat(t[0]).reshape(by_block) for t in terms]
        olds = [flat(w).reshape(by_block) for w in weights]
        own_m, own_v = ([flat(one).reshape(layers, COLOURS, rows, LANES) for one in ones] for ones in (m, v))
        x, zs, sums = communicate(side, grads, olds, own_m, own_v, PARTS)
        ys = [[lax.ppermute(z, "dp", ring(k)) for k, z in enumerate(part)] for part in zs]

        new_m, new_v = [], []
        for one_m, one_v, g in zip(m, v, sums, strict=True):
            g = unflat(g.reshape(layers, COLOURS * rows, LANES), *one_m.shape[1:]).astype(jnp.float32)
            a, b = moments(one_m, one_v, g)
            new_m.append(a)
            new_v.append(b)

        begins = [units - sum(PARTS[p:]) for p in range(len(PARTS))]

        def part_of(unit):
            return next((p for p, (begin, count) in enumerate(zip(begins, PARTS)) if begin <= unit < begin + count), None)

        colours = range(COLOURS)
        piece = side * rows * LANES
        whole = []
        for i in range(len(weights)):
            parts = [part_of(i * layers + layer) for layer in range(layers)]
            used = sorted({p for p in parts if p is not None})

            def placed(ins, out, i=i, parts=parts, used=used):
                pairs = []
                for layer, p in enumerate(parts):
                    unit = i * layers + layer
                    for k in colours:
                        for back in range(side if p is None else hops):
                            from_x = p is None or back < hops - 1
                            src = group(ins[0], unit, k, back) if from_x else ins[1 + used.index(p) * COLOURS + k].at[unit - begins[p]]
                            pairs.append((src, group(out, layer, k, back), True))
                return pairs

            ins = [x, *(z for p in used for z in zs[p])]
            whole.append(copies(placed, ins, pltpu.HBM, by_block, layers * n * COLOURS * rows * LANES))

        for p, begin in enumerate(begins):
            if p > 0:
                ys[p], whole = lax.optimization_barrier((ys[p], whole))
            for i in range(len(weights)):
                mine = [layer for layer in range(layers) if part_of(i * layers + layer) == p]
                if not mine:
                    continue

                def last(ins, out, i=i, mine=mine, begin=begin):
                    return [(ins[k].at[i * layers + layer - begin], group(out, layer, k, hops), False) for layer in mine for k in colours]

                whole[i] = copies(last, ys[p], pltpu.VMEM, by_block, len(mine) * COLOURS * piece, onto=whole[i])
        whole = [unflat(one.reshape(layers, n * COLOURS * rows, LANES), *w.shape[1:]) for one, w in zip(whole, weights, strict=True)]
        return (*whole, *new_m, *new_v)

    all_of, cut = P(None, None, None), P(None, "dp", None)
    return jax.shard_map(
        step,
        mesh=mesh,
        in_specs=(P(("rep", "dp"), None, None, None),) * 3 + (all_of,) * 3 + (cut,) * 6,
        out_specs=(P("rep", None, None),) * 3 + (P("rep", "dp", None),) * 6,
        check_vma=False,
    )
```

```python
import functools
import math

import jax
import jax.numpy as jnp
from jax import lax
from jax.experimental import pallas as pl
from jax.experimental.pallas import tpu as pltpu
from jax.sharding import PartitionSpec as P

MESH = pl.DeviceIdType.MESH
LANES, SUBLANES = 128, 8
COLOURS = 4
CHUNK = 128
STAGGER_NS = 12000


def flat(a):
    *lead, rows, columns = a.shape
    a = a.reshape(*lead, rows // SUBLANES, SUBLANES, columns // LANES, LANES)
    return jnp.swapaxes(a, -3, -2).reshape(*lead, rows * columns // LANES, LANES)


def unflat(a, rows, columns):
    *lead, _, _ = a.shape
    a = a.reshape(*lead, rows // SUBLANES, columns // LANES, SUBLANES, LANES)
    return jnp.swapaxes(a, -3, -2).reshape(*lead, rows, columns)


pinned = pltpu.with_memory_space_constraint


def moments(m, v, g):
    return 0.9 * m + 0.1 * g, 0.95 * v + 0.05 * g * g


def new_weight(w, m, v):
    step = m * lax.rsqrt(v + 1e-8) + 0.1 * w
    return (w - 0.02 * step).astype(jnp.bfloat16)


def direction(k):
    return (1 if k % 2 == 0 else -1), k // 2


def place(side):
    me = lax.axis_index("dp")
    return lax.div(me, side), lax.rem(me, side)


def at(k, first, second):
    return (first, second) if direction(k)[1] == 0 else (second, first)


def comm_kernel(side, layers, units, parts, *refs):
    weights = units // layers
    grads, olds, ms, vs = (refs[i * weights : (i + 1) * weights] for i in range(4))
    refs = refs[4 * weights :]
    x_ref, refs = refs[0], refs[1:]
    kept = units - sum(parts)
    zs, refs = refs[: len(parts) * COLOURS], refs[len(parts) * COLOURS :]
    gs, refs = refs[:weights], refs[weights:]
    (land1, land2, got, own, out1, in2, out2, old_v, m_v, v_v, out_w, out_g, send_sem, recv_sem, load_sem, store_sem) = refs
    rows = got.shape[2]
    last = side - 1
    xy = place(side)

    def turn(k, axis, by):
        way, first = direction(k)
        c = xy[first if axis == 0 else 1 - first]
        return lax.rem(c + way * by + 4 * side, side)

    def neighbour(k, axis):
        a, b = turn(k, 0, 1 if axis == 0 else 0), turn(k, 1, 1 if axis == 1 else 0)
        px, py = at(k, a, b)
        return {"dp": px * side + py}

    pl.when(lax.rem(lax.axis_index("rep"), 2) == 0)(lambda: pl.delay(STAGGER_NS))
    barrier = pltpu.get_barrier_semaphore()
    for k in range(COLOURS):
        pl.semaphore_signal(barrier, inc=1, device_id=neighbour(k, 0), device_id_type=MESH)
    pl.semaphore_wait(barrier, COLOURS)

    def of_weight(u, f):
        for w in range(weights):
            pl.when(lax.div(u, layers) == w)(functools.partial(f, w, lax.rem(u, layers)))

    def group(ref, lead, k, first):
        if direction(k)[1] == 0:
            return ref.at[lead, first, :, k]
        return ref.at[lead, :, first, k]

    def block(ref, lead, k, first, second):
        px, py = at(k, first, second)
        return ref.at[lead, px, py, k]

    def remote(stage, u, k, src, dst, axis):
        return pltpu.make_async_remote_copy(
            src_ref=src,
            dst_ref=dst,
            send_sem=send_sem.at[stage, lax.rem(u, 2), k],
            recv_sem=recv_sem.at[stage, u, k],
            device_id=neighbour(k, axis),
            device_id_type=MESH,
        )

    n1, n2 = last, last
    FIRST, SECOND, STEP = 0, n1, n1 + n2
    GATHER2, GATHER1 = STEP, STEP + n2
    stages = GATHER1 + n1

    def dst_of(stage, u, k):
        if stage < SECOND:
            return land1.at[u, k, stage - FIRST]
        if stage < STEP:
            return land2.at[u, k, stage - SECOND]
        raise AssertionError

    def wait_recv(stage, u, k):
        if stage < STEP:
            dst = dst_of(stage, u, k)
        elif stage < GATHER1:
            dst = block(x_ref, u, k, turn(k, 0, 0), turn(k, 1, -(stage - GATHER2) - 1))
        else:
            dst = group(x_ref, u, k, turn(k, 0, -(stage - GATHER1) - 1))
        remote(stage, u, k, dst, dst, 0).wait_recv()

    def wait_send(stage, u, k):
        small = SECOND <= stage < GATHER1
        ref = land2.at[0, k, 0] if small else land1.at[0, k, 0]
        remote(stage, u, k, ref, ref, 0).wait_send()

    def free(stage, u, k):
        pl.when(u >= 2)(lambda: wait_send(stage, u, k))

    def load(k, i, src, dst):
        return pltpu.make_async_copy(src, dst, load_sem.at[i, k])

    def stage_first(s, u):
        ks = range(COLOURS)
        if s == 0:
            def start(k, w, layer):
                remote(FIRST, u, k, group(grads[w], layer, k, turn(k, 0, -1)), land1.at[u, k, 0], 0).start()

            for k in ks:
                free(FIRST, u, k)
            def start_all(w, layer):
                for k in ks:
                    start(k, w, layer)
            of_weight(u, start_all)
            return

        def load_own(w, layer):
            for k in ks:
                load(k, 0, group(grads[w], layer, k, turn(k, 0, -1 - s)), own.at[k]).start()

        of_weight(u, load_own)
        for k in ks:
            wait_recv(FIRST + s - 1, u, k)
            load(k, 1, land1.at[u, k, s - 1], got.at[k]).start()
        slot = lax.rem(u, 2)
        for k in ks:
            free(FIRST + s, u, k)
            load(k, 0, land1.at[u, k, s - 1], own.at[k]).wait()
            load(k, 1, land1.at[u, k, s - 1], got.at[k]).wait()
            out = out1.at[s - 1, slot, k]
            per = rows // CHUNK

            def add(c, _):
                j, r = lax.div(c, per), pl.multiple_of(lax.rem(c, per) * CHUNK, CHUNK)
                total = got[k, j, pl.ds(r, CHUNK)].astype(jnp.float32) + own[k, j, pl.ds(r, CHUNK)].astype(jnp.float32)
                out[j, pl.ds(r, CHUNK)] = total.astype(jnp.bfloat16)
                return 0

            lax.fori_loop(0, side * per, add, 0)
            remote(FIRST + s, u, k, out, land1.at[u, k, s], 0).start()

    def load_second(s, u):
        ks = range(COLOURS)

        def load_own(w, layer):
            for k in ks:
                load(k, 0, block(grads[w], layer, k, turn(k, 0, 0), turn(k, 1, -1 - s)), in2.at[0, k]).start()

        of_weight(u, load_own)
        for k in ks:
            wait_recv(SECOND + s - 1, u, k)
            load(k, 1, land1.at[u, k, n1 - 1, turn(k, 1, -1 - s)], in2.at[1, k]).start()
            if s > 0:
                load(k, 2, land2.at[u, k, s - 1], in2.at[2, k]).start()

    def wait_second(s, k):
        for i in range(3 if s > 0 else 2):
            load(k, i, land2.at[0, k, 0], in2.at[i, k]).wait()

    def sum_second(s, k, r):
        total = in2[1, k, pl.ds(r, CHUNK)].astype(jnp.float32) + in2[0, k, pl.ds(r, CHUNK)].astype(jnp.float32)
        if s > 0:
            total += in2[2, k, pl.ds(r, CHUNK)].astype(jnp.float32)
        return total.astype(jnp.bfloat16)

    def stage_second(s, u):
        load_second(s, u)
        slot = lax.rem(u, 2)
        for k in range(COLOURS):
            free(SECOND + s, u, k)
            wait_second(s, k)
            out = out2.at[s, slot, k]

            def add(c, _):
                r = pl.multiple_of(c * CHUNK, CHUNK)
                out[pl.ds(r, CHUNK)] = sum_second(s, k, r)
                return 0

            lax.fori_loop(0, rows // CHUNK, add, 0)
            remote(SECOND + s, u, k, out, land2.at[u, k, s], 1).start()

    def store_w(k, u, slot):
        return pltpu.make_async_copy(out_w.at[slot, k], block(x_ref, u, k, turn(k, 0, 0), turn(k, 1, 0)), store_sem.at[0, slot, k])

    def store_g(k, slot, w, layer):
        return pltpu.make_async_copy(out_g.at[slot, k], gs[w].at[layer, k], store_sem.at[1, slot, k])

    def stage_step(u):
        ks = range(COLOURS)

        def load_state(w, layer):
            for k in ks:
                load(k, 3, block(olds[w], layer, k, turn(k, 0, 0), turn(k, 1, 0)), old_v.at[k]).start()
                load(k, 4, ms[w].at[layer, k], m_v.at[k]).start()
                load(k, 5, vs[w].at[layer, k], v_v.at[k]).start()

        of_weight(u, load_state)
        load_second(n2, u)
        slot = lax.rem(u, 2)
        for k in ks:
            free(GATHER2, u, k)

            pl.when(u >= 2)(lambda: store_g(k, slot, 0, 0).wait())

            wait_second(n2, k)
            load(k, 3, old_v.at[k], old_v.at[k]).wait()
            load(k, 4, m_v.at[k], m_v.at[k]).wait()
            load(k, 5, v_v.at[k], v_v.at[k]).wait()

            def adamw(c, _):
                r = pl.multiple_of(c * CHUNK, CHUNK)
                here = pl.ds(r, CHUNK)
                g = sum_second(n2, k, r)
                m, v = moments(m_v[k, here], v_v[k, here], g.astype(jnp.float32))
                out_w[slot, k, here] = new_weight(old_v[k, here].astype(jnp.float32), m, v)
                out_g[slot, k, here] = g
                return 0

            lax.fori_loop(0, rows // CHUNK, adamw, 0)
            remote(GATHER2, u, k, out_w.at[slot, k], block(x_ref, u, k, turn(k, 0, 0), turn(k, 1, 0)), 1).start()
            store_w(k, u, slot).start()

        def store_all(w, layer):
            for k in ks:
                store_g(k, slot, w, layer).start()

        of_weight(u, store_all)

    def stage_gather2(s, u):
        for k in range(COLOURS):
            if s == 1:
                store_w(k, u, lax.rem(u, 2)).wait()
            wait_recv(GATHER2 + s - 1, u, k)
            free(GATHER2 + s, u, k)
            it = block(x_ref, u, k, turn(k, 0, 0), turn(k, 1, -s))
            remote(GATHER2 + s, u, k, it, it, 1).start()

    def stage_gather1(s, u):
        for k in range(COLOURS):
            wait_recv(GATHER1 + s - 1, u, k)
            free(GATHER1 + s, u, k)
            it = group(x_ref, u, k, turn(k, 0, -s))
            if s == n1 - 2:
                pl.when(u < kept)(lambda: remote(GATHER1 + s, u, k, it, it, 0).start())
                for p, count in enumerate(parts):
                    z, begin = zs[p * COLOURS + k], kept + sum(parts[:p])
                    pl.when((u >= begin) & (u < begin + count))(
                        lambda: remote(GATHER1 + s, u, k, it, z.at[u - begin], 0).start()
                    )
            else:
                remote(GATHER1 + s, u, k, it, it, 0).start()

    def body(i, _):
        for s in range(stages):
            u = i - s
            count = kept if s == stages - 1 else units
            run = (
                functools.partial(stage_first, s, u)
                if s < SECOND
                else functools.partial(stage_second, s - SECOND, u)
                if s < STEP
                else functools.partial(stage_step, u)
                if s == GATHER2
                else functools.partial(stage_gather2, s - GATHER2, u)
                if s < GATHER1
                else functools.partial(stage_gather1, s - GATHER1, u)
            )
            pl.when((u >= 0) & (u < count))(run)
        return 0

    lax.fori_loop(0, stages - 1 + (units if kept == units else max(units - 1, kept)), body, 0)

    def drain(u, _):
        for k in range(COLOURS):
            pl.when(u >= kept)(lambda: wait_recv(stages - 2, u, k))
            pl.when(u < kept)(lambda: wait_recv(stages - 1, u, k))
        return 0

    lax.fori_loop(0, units, drain, 0)
    for s in range(stages):
        count = kept if s == stages - 1 else units
        for u in range(max(count - 2, 0), count):
            for k in range(COLOURS):
                wait_send(s, u, k)
    for u in range(max(units - 2, 0), units):
        for k in range(COLOURS):
            store_g(k, u % 2, 0, 0).wait()


def communicate(side, grads, olds, ms, vs, parts):
    layers = grads[0].shape[0]
    weights = len(grads)
    units = weights * layers
    rows = grads[0].shape[-2]
    hops = side - 1
    hbm = pl.BlockSpec(memory_space=pltpu.HBM)
    bf16, f32 = jnp.bfloat16, jnp.float32
    shape = pltpu.HBM
    outs = [
        shape((units, *grads[0].shape[1:]), bf16),
        *[shape((count, side, rows, LANES), bf16) for count in parts for _ in range(COLOURS)],
        *[shape((layers, COLOURS, rows, LANES), bf16)] * weights,
        shape((units, COLOURS, hops, side, rows, LANES), bf16),
        shape((units, COLOURS, hops, rows, LANES), bf16),
    ]
    stages = 4 * hops
    scratch = [
        pltpu.VMEM((COLOURS, side, rows, LANES), bf16),
        pltpu.VMEM((COLOURS, side, rows, LANES), bf16),
        pltpu.VMEM((hops - 1, 2, COLOURS, side, rows, LANES), bf16),
        pltpu.VMEM((3, COLOURS, rows, LANES), bf16),
        pltpu.VMEM((hops, 2, COLOURS, rows, LANES), bf16),
        pltpu.VMEM((COLOURS, rows, LANES), bf16),
        pltpu.VMEM((COLOURS, rows, LANES), f32),
        pltpu.VMEM((COLOURS, rows, LANES), f32),
        pltpu.VMEM((2, COLOURS, rows, LANES), bf16),
        pltpu.VMEM((2, COLOURS, rows, LANES), bf16),
        pltpu.SemaphoreType.DMA((stages, 2, COLOURS)),
        pltpu.SemaphoreType.DMA((stages, units, COLOURS)),
        pltpu.SemaphoreType.DMA((6, COLOURS)),
        pltpu.SemaphoreType.DMA((2, 2, COLOURS)),
    ]
    got = pl.pallas_call(
        functools.partial(comm_kernel, side, layers, units, parts),
        out_shape=outs,
        in_specs=[hbm] * (4 * weights),
        out_specs=[hbm] * len(outs),
        scratch_shapes=scratch,
        compiler_params=pltpu.CompilerParams(collective_id=0, has_side_effects=True, vmem_limit_bytes=60 << 20),
        name="sum_step_gather",
    )(*(pinned(a, pltpu.HBM) for a in (*grads, *olds, *ms, *vs)))
    x, got = got[0], got[1:]
    zs, got = got[: len(parts) * COLOURS], got[len(parts) * COLOURS :]
    return x, [zs[i * COLOURS : (i + 1) * COLOURS] for i in range(len(parts))], got[:weights]


SLOTS = 16


def copy_kernel(jobs, n_in, *refs):
    ins, (out, buf, in_sem, out_sem, straight_sem) = refs[:n_in], refs[-5:]
    pairs = jobs(ins, out)
    staged = [pair for pair in pairs if pair[2]]
    straight = [pltpu.make_async_copy(src, dst, straight_sem.at[i]) for i, (src, dst, _) in enumerate(p for p in pairs if not p[2])]

    def into(i):
        return pltpu.make_async_copy(staged[i][0], buf.at[i % SLOTS], in_sem.at[i % SLOTS])

    def outof(i):
        return pltpu.make_async_copy(buf.at[i % SLOTS], staged[i][1], out_sem.at[i % SLOTS])

    ahead = SLOTS // 2
    for copy in straight:
        copy.start()
    for i in range(len(staged) + ahead):
        if i < len(staged):
            if i >= SLOTS:
                outof(i - SLOTS).wait()
            into(i).start()
        if ahead <= i:
            into(i - ahead).wait()
            outof(i - ahead).start()
    for i in range(max(len(staged) - SLOTS, 0), len(staged)):
        outof(i).wait()
    for copy in straight:
        copy.wait()


def copies(jobs, ins, space, shape, moved, onto=None):
    hbm = pl.BlockSpec(memory_space=pltpu.HBM)
    side, rows = shape[1], shape[-2]
    given = [pinned(a, space) for a in ins] + ([] if onto is None else [pinned(onto, pltpu.HBM)])
    return pl.pallas_call(
        functools.partial(copy_kernel, jobs, len(ins)),
        out_shape=pltpu.HBM(shape, jnp.bfloat16),
        in_specs=[pl.BlockSpec(memory_space=space)] * len(ins) + [hbm] * (onto is not None),
        out_specs=hbm,
        scratch_shapes=[
            pltpu.VMEM((SLOTS if onto is None else 1, side, rows, LANES), jnp.bfloat16),
            pltpu.SemaphoreType.DMA((SLOTS,)),
            pltpu.SemaphoreType.DMA((SLOTS,)),
            pltpu.SemaphoreType.DMA((SLOTS,)),
        ],
        input_output_aliases={} if onto is None else {len(ins): 0},
        compiler_params=pltpu.CompilerParams(vmem_limit_bytes=(16 if onto is None else 8) << 20),
        cost_estimate=pl.CostEstimate(flops=4 * moved, bytes_accessed=4 * moved, transcendentals=0),
        name="place" if onto is None else "place_last",
    )(*given)


def solution(mesh):
    n = mesh.shape["dp"]
    side = math.isqrt(n)
    hops = side - 1

    def ring(k):
        way, axis = direction(k)
        pairs = []
        for i in range(n):
            c = [i // side, i % side]
            c[axis] = (c[axis] + way) % side
            pairs.append((i, c[0] * side + c[1]))
        return pairs

    def group(ref, lead, k, back):
        way, axis = direction(k)
        first = lax.rem(place(side)[axis] - way * back + 4 * side, side)
        return ref.at[lead, first, :, k] if axis == 0 else ref.at[lead, :, first, k]

    def step(*arrays):
        terms, weights, m, v = (arrays[i : i + 3] for i in (0, 3, 6, 9))
        layers = m[0].shape[0]
        units = layers * len(m)
        rows = m[0].shape[1] * m[0].shape[2] // LANES // COLOURS
        by_block = (layers, side, side, COLOURS, rows, LANES)
        grads = [flat(t[0]).reshape(by_block) for t in terms]
        olds = [flat(w).reshape(by_block) for w in weights]
        own_m, own_v = ([flat(one).reshape(layers, COLOURS, rows, LANES) for one in ones] for ones in (m, v))
        parts = (layers,) * (len(weights) - 1) + (1,) * layers
        x, zs, sums = communicate(side, grads, olds, own_m, own_v, parts)
        ys = [[lax.ppermute(z, "dp", ring(k)) for k, z in enumerate(part)] for part in zs]

        new_m, new_v = [], []
        for one_m, one_v, g in zip(m, v, sums, strict=True):
            g = unflat(g.reshape(layers, COLOURS * rows, LANES), *one_m.shape[1:]).astype(jnp.float32)
            a, b = moments(one_m, one_v, g)
            new_m.append(a)
            new_v.append(b)

        begins = [units - sum(parts[p:]) for p in range(len(parts))]

        def part_of(unit):
            return next((p for p, (begin, count) in enumerate(zip(begins, parts)) if begin <= unit < begin + count), None)

        colours = range(COLOURS)
        piece = side * rows * LANES
        whole = []
        for i in range(len(weights)):
            of_layer = [part_of(i * layers + layer) for layer in range(layers)]
            used = sorted({p for p in of_layer if p is not None})

            def placed(ins, out, i=i, of_layer=of_layer, used=used):
                pairs = []
                for layer, p in enumerate(of_layer):
                    unit = i * layers + layer
                    for k in colours:
                        for back in range(side if p is None else hops):
                            from_x = p is None or back < hops - 1
                            src = group(ins[0], unit, k, back) if from_x else ins[1 + used.index(p) * COLOURS + k].at[unit - begins[p]]
                            pairs.append((src, group(out, layer, k, back), True))
                return pairs

            ins = [x, *(z for p in used for z in zs[p])]
            whole.append(copies(placed, ins, pltpu.HBM, by_block, layers * n * COLOURS * rows * LANES))

        for p, begin in enumerate(begins):
            if p > 0:
                ys[p], whole = lax.optimization_barrier((ys[p], whole))
            for i in range(len(weights)):
                mine = [layer for layer in range(layers) if part_of(i * layers + layer) == p]
                if not mine:
                    continue

                def last(ins, out, i=i, mine=mine, begin=begin):
                    return [(ins[k].at[i * layers + layer - begin], group(out, layer, k, hops), False) for layer in mine for k in colours]

                whole[i] = copies(last, ys[p], pltpu.VMEM, by_block, len(mine) * COLOURS * piece, onto=whole[i])
        whole = [unflat(one.reshape(layers, n * COLOURS * rows, LANES), *w.shape[1:]) for one, w in zip(whole, weights, strict=True)]
        return (*whole, *new_m, *new_v)

    all_of, cut = P(None, None, None), P(None, "dp", None)
    return jax.shard_map(
        step,
        mesh=mesh,
        in_specs=(P(("rep", "dp"), None, None, None),) * 3 + (all_of,) * 3 + (cut,) * 6,
        out_specs=(P("rep", None, None),) * 3 + (P("rep", "dp", None),) * 6,
        check_vma=False,
    )
```

```python
import functools
import math

import jax
import jax.numpy as jnp
from jax import lax
from jax.experimental import pallas as pl
from jax.experimental.pallas import tpu as pltpu
from jax.sharding import PartitionSpec as P

MESH = pl.DeviceIdType.MESH
LANES, SUBLANES = 128, 8
COLOURS = 4
CHUNK = 128
STAGGER_NS = 12000


def flat(a):
    *lead, rows, columns = a.shape
    a = a.reshape(*lead, rows // SUBLANES, SUBLANES, columns // LANES, LANES)
    return jnp.swapaxes(a, -3, -2).reshape(*lead, rows * columns // LANES, LANES)


def unflat(a, rows, columns):
    *lead, _, _ = a.shape
    a = a.reshape(*lead, rows // SUBLANES, columns // LANES, SUBLANES, LANES)
    return jnp.swapaxes(a, -3, -2).reshape(*lead, rows, columns)


pinned = pltpu.with_memory_space_constraint


def moments(m, v, g):
    return 0.9 * m + 0.1 * g, 0.95 * v + 0.05 * g * g


def new_weight(w, m, v):
    step = m * lax.rsqrt(v + 1e-8) + 0.1 * w
    return (w - 0.02 * step).astype(jnp.bfloat16)


def direction(k):
    return (1 if k % 2 == 0 else -1), k // 2


def place(side):
    me = lax.axis_index("dp")
    return lax.div(me, side), lax.rem(me, side)


def at(k, first, second):
    return (first, second) if direction(k)[1] == 0 else (second, first)


def comm_kernel(side, layers, units, parts, *refs):
    weights = units // layers
    grads, olds, ms, vs = (refs[i * weights : (i + 1) * weights] for i in range(4))
    refs = refs[4 * weights :]
    x_ref, refs = refs[0], refs[1:]
    zs, refs = refs[: len(parts) * COLOURS], refs[len(parts) * COLOURS :]
    gs, refs = refs[:weights], refs[weights:]
    (land1, land2, got, own1, out1, in2, own2, out2, old_v, m_v, v_v, out_w, out_g, *sems) = refs
    send_sem, recv_sem, load_sem, own_sem, store_sem = sems
    rows = got.shape[2]
    last = side - 1
    xy = place(side)

    def turn(k, axis, by):
        way, first = direction(k)
        c = xy[first if axis == 0 else 1 - first]
        return lax.rem(c + way * by + 4 * side, side)

    def neighbour(k, axis):
        a, b = turn(k, 0, 1 if axis == 0 else 0), turn(k, 1, 1 if axis == 1 else 0)
        px, py = at(k, a, b)
        return {"dp": px * side + py}

    pl.when(lax.rem(lax.axis_index("rep"), 2) == 0)(lambda: pl.delay(STAGGER_NS))
    barrier = pltpu.get_barrier_semaphore()
    for k in range(COLOURS):
        pl.semaphore_signal(barrier, inc=1, device_id=neighbour(k, 0), device_id_type=MESH)
    pl.semaphore_wait(barrier, COLOURS)

    def of_weight(u, f):
        for w in range(weights):
            pl.when(lax.div(u, layers) == w)(functools.partial(f, w, lax.rem(u, layers)))

    def group(ref, lead, k, first):
        if direction(k)[1] == 0:
            return ref.at[lead, first, :, k]
        return ref.at[lead, :, first, k]

    def block(ref, lead, k, first, second):
        px, py = at(k, first, second)
        return ref.at[lead, px, py, k]

    def remote(stage, u, k, src, dst, axis):
        return pltpu.make_async_remote_copy(
            src_ref=src,
            dst_ref=dst,
            send_sem=send_sem.at[stage, lax.rem(u, 2), k],
            recv_sem=recv_sem.at[stage, u, k],
            device_id=neighbour(k, axis),
            device_id_type=MESH,
        )

    n1, n2 = last, last
    FIRST, SECOND, STEP = 0, n1, n1 + n2
    GATHER2, GATHER1 = STEP, STEP + n2
    stages = GATHER1 + n1 - 1

    def wait_recv(stage, u, k):
        if stage < SECOND:
            dst = land1.at[u, k, stage - FIRST]
        elif stage < STEP:
            dst = land2.at[u, k, stage - SECOND]
        elif stage < GATHER1:
            dst = block(x_ref, u, k, turn(k, 0, 0), turn(k, 1, -(stage - GATHER2) - 1))
        else:
            dst = group(x_ref, u, k, turn(k, 0, -(stage - GATHER1) - 1))
        remote(stage, u, k, dst, dst, 0).wait_recv()

    def wait_send(stage, u, k):
        small = SECOND <= stage < GATHER1
        ref = land2.at[0, k, 0] if small else land1.at[0, k, 0]
        remote(stage, u, k, ref, ref, 0).wait_send()

    def free(stage, u, k):
        pl.when(u >= 2)(lambda: wait_send(stage, u, k))

    def load(k, i, src, dst):
        return pltpu.make_async_copy(src, dst, load_sem.at[i, k])

    def own_of(stage, u, k, w, layer):
        if stage < SECOND:
            src, dst = group(grads[w], layer, k, turn(k, 0, -1 - (stage - FIRST))), own1.at[stage - FIRST - 1, k]
        else:
            src, dst = block(grads[w], layer, k, turn(k, 0, 0), turn(k, 1, -1 - (stage - SECOND))), own2.at[stage - SECOND, k]
        return pltpu.make_async_copy(src, dst, own_sem.at[stage, k])

    def state_of(k, w, layer):
        return (
            load(k, 2, block(olds[w], layer, k, turn(k, 0, 0), turn(k, 1, 0)), old_v.at[k]),
            load(k, 3, ms[w].at[layer, k], m_v.at[k]),
            load(k, 4, vs[w].at[layer, k], v_v.at[k]),
        )

    def prefetch(stage, u):
        def start(w, layer):
            for k in range(COLOURS):
                own_of(stage, u, k, w, layer).start()
                if stage == STEP:
                    for one in state_of(k, w, layer):
                        one.start()

        of_weight(u, start)

    def stage_first(s, u):
        ks = range(COLOURS)
        if s == 0:

            def start(w, layer):
                for k in ks:
                    remote(FIRST, u, k, group(grads[w], layer, k, turn(k, 0, -1)), land1.at[u, k, 0], 0).start()

            for k in ks:
                free(FIRST, u, k)
            of_weight(u, start)
            return

        for k in ks:
            wait_recv(FIRST + s - 1, u, k)
            load(k, 0, land1.at[u, k, s - 1], got.at[k]).start()
        slot = lax.rem(u, 2)
        for k in ks:
            free(FIRST + s, u, k)
            own_of(FIRST + s, u, k, 0, 0).wait()
            load(k, 0, land1.at[u, k, s - 1], got.at[k]).wait()
            out = out1.at[s - 1, slot, k]
            per = rows // CHUNK

            def add(c, _):
                j, r = lax.div(c, per), pl.multiple_of(lax.rem(c, per) * CHUNK, CHUNK)
                total = got[k, j, pl.ds(r, CHUNK)].astype(jnp.float32) + own1[s - 1, k, j, pl.ds(r, CHUNK)].astype(jnp.float32)
                out[j, pl.ds(r, CHUNK)] = total.astype(jnp.bfloat16)
                return 0

            lax.fori_loop(0, side * per, add, 0)
            remote(FIRST + s, u, k, out, land1.at[u, k, s], 0).start()

    def load_second(s, u):
        for k in range(COLOURS):
            wait_recv(SECOND + s - 1, u, k)
            load(k, 0, land1.at[u, k, n1 - 1, turn(k, 1, -1 - s)], in2.at[0, k]).start()
            if s > 0:
                load(k, 1, land2.at[u, k, s - 1], in2.at[1, k]).start()

    def wait_second(s, u, k):
        own_of(SECOND + s, u, k, 0, 0).wait()
        for i in range(2 if s > 0 else 1):
            load(k, i, land2.at[0, k, 0], in2.at[i, k]).wait()

    def sum_second(s, k, r):
        total = in2[0, k, pl.ds(r, CHUNK)].astype(jnp.float32) + own2[s, k, pl.ds(r, CHUNK)].astype(jnp.float32)
        if s > 0:
            total += in2[1, k, pl.ds(r, CHUNK)].astype(jnp.float32)
        return total.astype(jnp.bfloat16)

    def stage_second(s, u):
        load_second(s, u)
        slot = lax.rem(u, 2)
        for k in range(COLOURS):
            free(SECOND + s, u, k)
            wait_second(s, u, k)
            out = out2.at[s, slot, k]

            def add(c, _):
                r = pl.multiple_of(c * CHUNK, CHUNK)
                out[pl.ds(r, CHUNK)] = sum_second(s, k, r)
                return 0

            lax.fori_loop(0, rows // CHUNK, add, 0)
            remote(SECOND + s, u, k, out, land2.at[u, k, s], 1).start()

    def store_w(k, u, slot):
        return pltpu.make_async_copy(out_w.at[slot, k], block(x_ref, u, k, turn(k, 0, 0), turn(k, 1, 0)), store_sem.at[0, slot, k])

    def store_g(k, slot, w, layer):
        return pltpu.make_async_copy(out_g.at[slot, k], gs[w].at[layer, k], store_sem.at[1, slot, k])

    def stage_step(u):
        ks = range(COLOURS)
        load_second(n2, u)
        slot = lax.rem(u, 2)
        for k in ks:
            free(GATHER2, u, k)
            pl.when(u >= 2)(lambda: store_g(k, slot, 0, 0).wait())

            wait_second(n2, u, k)
            for one in state_of(k, 0, 0):
                one.wait()

            def adamw(c, _):
                r = pl.multiple_of(c * CHUNK, CHUNK)
                here = pl.ds(r, CHUNK)
                g = sum_second(n2, k, r)
                m, v = moments(m_v[k, here], v_v[k, here], g.astype(jnp.float32))
                out_w[slot, k, here] = new_weight(old_v[k, here].astype(jnp.float32), m, v)
                out_g[slot, k, here] = g
                return 0

            lax.fori_loop(0, rows // CHUNK, adamw, 0)
            remote(GATHER2, u, k, out_w.at[slot, k], block(x_ref, u, k, turn(k, 0, 0), turn(k, 1, 0)), 1).start()
            store_w(k, u, slot).start()

        def store_all(w, layer):
            for k in ks:
                store_g(k, slot, w, layer).start()

        of_weight(u, store_all)

    def stage_gather2(s, u):
        for k in range(COLOURS):
            if s == 1:
                store_w(k, u, lax.rem(u, 2)).wait()
            wait_recv(GATHER2 + s - 1, u, k)
            free(GATHER2 + s, u, k)
            it = block(x_ref, u, k, turn(k, 0, 0), turn(k, 1, -s))
            remote(GATHER2 + s, u, k, it, it, 1).start()

    def stage_gather1(s, u):
        for k in range(COLOURS):
            wait_recv(GATHER1 + s - 1, u, k)
            free(GATHER1 + s, u, k)
            it = group(x_ref, u, k, turn(k, 0, -s))
            if s < n1 - 2:
                remote(GATHER1 + s, u, k, it, it, 0).start()
                continue
            for p, count in enumerate(parts):
                z, begin = zs[p * COLOURS + k], sum(parts[:p])
                pl.when((u >= begin) & (u < begin + count))(lambda: remote(GATHER1 + s, u, k, it, z.at[u - begin], 0).start())

    def body(i, _):
        for s in range(FIRST + 1, STEP + 1):
            u = i - s
            pl.when((u >= 0) & (u < units))(functools.partial(prefetch, s, u))
        for s in range(stages):
            u = i - s
            run = (
                functools.partial(stage_first, s, u)
                if s < SECOND
                else functools.partial(stage_second, s - SECOND, u)
                if s < STEP
                else functools.partial(stage_step, u)
                if s == GATHER2
                else functools.partial(stage_gather2, s - GATHER2, u)
                if s < GATHER1
                else functools.partial(stage_gather1, s - GATHER1, u)
            )
            pl.when((u >= 0) & (u < units))(run)
        return 0

    lax.fori_loop(0, stages - 1 + units, body, 0)

    def drain(u, _):
        for k in range(COLOURS):
            wait_recv(stages - 1, u, k)
        return 0

    lax.fori_loop(0, units, drain, 0)
    for s in range(stages):
        for u in range(max(units - 2, 0), units):
            for k in range(COLOURS):
                wait_send(s, u, k)
    for u in range(max(units - 2, 0), units):
        for k in range(COLOURS):
            store_g(k, u % 2, 0, 0).wait()


def communicate(side, grads, olds, ms, vs, parts):
    layers = grads[0].shape[0]
    weights = len(grads)
    units = weights * layers
    rows = grads[0].shape[-2]
    hops = side - 1
    hbm = pl.BlockSpec(memory_space=pltpu.HBM)
    bf16, f32 = jnp.bfloat16, jnp.float32
    shape = pltpu.HBM
    outs = [
        shape((units, *grads[0].shape[1:]), bf16),
        *[shape((count, side, rows, LANES), bf16) for count in parts for _ in range(COLOURS)],
        *[shape((layers, COLOURS, rows, LANES), bf16)] * weights,
        shape((units, COLOURS, hops, side, rows, LANES), bf16),
        shape((units, COLOURS, hops, rows, LANES), bf16),
    ]
    stages = 4 * hops - 1
    scratch = [
        pltpu.VMEM((COLOURS, side, rows, LANES), bf16),
        pltpu.VMEM((hops - 1, COLOURS, side, rows, LANES), bf16),
        pltpu.VMEM((hops - 1, 2, COLOURS, side, rows, LANES), bf16),
        pltpu.VMEM((2, COLOURS, rows, LANES), bf16),
        pltpu.VMEM((hops + 1, COLOURS, rows, LANES), bf16),
        pltpu.VMEM((hops, 2, COLOURS, rows, LANES), bf16),
        pltpu.VMEM((COLOURS, rows, LANES), bf16),
        pltpu.VMEM((COLOURS, rows, LANES), f32),
        pltpu.VMEM((COLOURS, rows, LANES), f32),
        pltpu.VMEM((2, COLOURS, rows, LANES), bf16),
        pltpu.VMEM((2, COLOURS, rows, LANES), bf16),
        pltpu.SemaphoreType.DMA((stages, 2, COLOURS)),
        pltpu.SemaphoreType.DMA((stages, units, COLOURS)),
        pltpu.SemaphoreType.DMA((5, COLOURS)),
        pltpu.SemaphoreType.DMA((stages, COLOURS)),
        pltpu.SemaphoreType.DMA((2, 2, COLOURS)),
    ]
    got = pl.pallas_call(
        functools.partial(comm_kernel, side, layers, units, parts),
        out_shape=outs,
        in_specs=[hbm] * (4 * weights),
        out_specs=[hbm] * len(outs),
        scratch_shapes=scratch,
        compiler_params=pltpu.CompilerParams(collective_id=0, has_side_effects=True, vmem_limit_bytes=60 << 20),
        name="sum_step_gather",
    )(*(pinned(a, pltpu.HBM) for a in (*grads, *olds, *ms, *vs)))
    x, got = got[0], got[1:]
    zs, got = got[: len(parts) * COLOURS], got[len(parts) * COLOURS :]
    return x, [zs[i * COLOURS : (i + 1) * COLOURS] for i in range(len(parts))], got[:weights]


SLOTS = 8


def copy_kernel(jobs, n_in, *refs):
    ins, (out, buf, in_sem, out_sem, straight_sem) = refs[:n_in], refs[-5:]
    pairs = jobs(ins, out)
    staged = [pair for pair in pairs if pair[2]]
    straight = [pltpu.make_async_copy(src, dst, straight_sem.at[i]) for i, (src, dst, _) in enumerate(p for p in pairs if not p[2])]

    def slot(i):
        return buf.at[i % SLOTS, pl.ds(0, staged[i][0].shape[0])]

    def into(i):
        return pltpu.make_async_copy(staged[i][0], slot(i), in_sem.at[i % SLOTS])

    def outof(i):
        return pltpu.make_async_copy(slot(i), staged[i][1], out_sem.at[i % SLOTS])

    ahead = SLOTS // 2
    for copy in straight:
        copy.start()
    for i in range(len(staged) + ahead):
        if i < len(staged):
            if i >= SLOTS:
                outof(i - SLOTS).wait()
            into(i).start()
        if ahead <= i:
            into(i - ahead).wait()
            outof(i - ahead).start()
    for i in range(max(len(staged) - SLOTS, 0), len(staged)):
        outof(i).wait()
    for copy in straight:
        copy.wait()


def copies(jobs, ins, space, shape, moved, onto=None):
    hbm = pl.BlockSpec(memory_space=pltpu.HBM)
    side, rows = shape[1], shape[-2]
    given = [pinned(a, space) for a in ins] + ([] if onto is None else [pinned(onto, pltpu.HBM)])
    return pl.pallas_call(
        functools.partial(copy_kernel, jobs, len(ins)),
        out_shape=pltpu.HBM(shape, jnp.bfloat16),
        in_specs=[pl.BlockSpec(memory_space=space)] * len(ins) + [hbm] * (onto is not None),
        out_specs=hbm,
        scratch_shapes=[
            pltpu.VMEM((SLOTS if onto is None else 1, shape[0], side, rows, LANES), jnp.bfloat16),
            pltpu.SemaphoreType.DMA((SLOTS,)),
            pltpu.SemaphoreType.DMA((SLOTS,)),
            pltpu.SemaphoreType.DMA((SLOTS,)),
        ],
        input_output_aliases={} if onto is None else {len(ins): 0},
        compiler_params=pltpu.CompilerParams(vmem_limit_bytes=(16 if onto is None else 8) << 20),
        cost_estimate=pl.CostEstimate(flops=4 * moved, bytes_accessed=4 * moved, transcendentals=0),
        name="place" if onto is None else "place_last",
    )(*given)


def solution(mesh):
    n = mesh.shape["dp"]
    side = math.isqrt(n)
    hops = side - 1

    def ring(k):
        way, axis = direction(k)
        pairs = []
        for i in range(n):
            c = [i // side, i % side]
            c[axis] = (c[axis] + way) % side
            pairs.append((i, c[0] * side + c[1]))
        return pairs

    def group(ref, lead, k, back):
        way, axis = direction(k)
        first = lax.rem(place(side)[axis] - way * back + 4 * side, side)
        return ref.at[lead, first, :, k] if axis == 0 else ref.at[lead, :, first, k]

    def step(*arrays):
        terms, weights, m, v = (arrays[i : i + 3] for i in (0, 3, 6, 9))
        layers = m[0].shape[0]
        rows = m[0].shape[1] * m[0].shape[2] // LANES // COLOURS
        by_block = (layers, side, side, COLOURS, rows, LANES)
        grads = [flat(t[0]).reshape(by_block) for t in terms]
        olds = [flat(w).reshape(by_block) for w in weights]
        own_m, own_v = ([flat(one).reshape(layers, COLOURS, rows, LANES) for one in ones] for ones in (m, v))
        parts = (layers,) * (len(weights) - 1) + (1,) * layers
        x, zs, sums = communicate(side, grads, olds, own_m, own_v, parts)
        ys = [[lax.ppermute(z, "dp", ring(k)) for k, z in enumerate(part)] for part in zs]

        new_m, new_v = [], []
        for one_m, one_v, g in zip(m, v, sums, strict=True):
            g = unflat(g.reshape(layers, COLOURS * rows, LANES), *one_m.shape[1:]).astype(jnp.float32)
            a, b = moments(one_m, one_v, g)
            new_m.append(a)
            new_v.append(b)

        begins = [sum(parts[:p]) for p in range(len(parts))]
        part_of = [p for p, count in enumerate(parts) for _ in range(count)]

        colours = range(COLOURS)
        piece = side * rows * LANES
        whole = []
        for i in range(len(weights)):
            of_layer = part_of[i * layers : (i + 1) * layers]
            used = sorted(set(of_layer))

            def placed(ins, out, i=i, of_layer=of_layer, used=used):
                pairs = []
                for k in colours:
                    for back in range(hops - 1):
                        here = group(out, pl.ds(0, layers), k, back)
                        pairs.append((group(ins[0], pl.ds(i * layers, layers), k, back), here, True))
                    for p in used:
                        first, count = of_layer.index(p), of_layer.count(p)
                        z = ins[1 + used.index(p) * COLOURS + k].at[pl.ds(i * layers + first - begins[p], count)]
                        pairs.append((z, group(out, pl.ds(first, count), k, hops - 1), True))
                return pairs

            ins = [x, *(z for p in used for z in zs[p])]
            whole.append(copies(placed, ins, pltpu.HBM, by_block, layers * n * COLOURS * rows * LANES))

        for p, begin in enumerate(begins):
            if p > 0:
                ys[p], whole = lax.optimization_barrier((ys[p], whole))
            for i in range(len(weights)):
                mine = [layer for layer in range(layers) if part_of[i * layers + layer] == p]
                if not mine:
                    continue

                def last(ins, out, i=i, mine=mine, begin=begin):
                    here = pl.ds(mine[0], len(mine))
                    return [(ins[k].at[pl.ds(i * layers + mine[0] - begin, len(mine))], group(out, here, k, hops), False) for k in colours]

                whole[i] = copies(last, ys[p], pltpu.VMEM, by_block, len(mine) * COLOURS * piece, onto=whole[i])
        whole = [unflat(one.reshape(layers, n * COLOURS * rows, LANES), *w.shape[1:]) for one, w in zip(whole, weights, strict=True)]
        return (*whole, *new_m, *new_v)

    all_of, cut = P(None, None, None), P(None, "dp", None)
    return jax.shard_map(
        step,
        mesh=mesh,
        in_specs=(P(("rep", "dp"), None, None, None),) * 3 + (all_of,) * 3 + (cut,) * 6,
        out_specs=(P("rep", None, None),) * 3 + (P("rep", "dp", None),) * 6,
        check_vma=False,
    )
```

```python
import functools
import math

import jax
import jax.numpy as jnp
from jax import lax
from jax.experimental import pallas as pl
from jax.experimental.pallas import tpu as pltpu
from jax.sharding import PartitionSpec as P

MESH = pl.DeviceIdType.MESH
LANES, SUBLANES = 128, 8
COLOURS = 4
CHUNK = 128
STAGGER_NS = 12000
LATE = 256


def flat(a):
    *lead, rows, columns = a.shape
    a = a.reshape(*lead, rows // SUBLANES, SUBLANES, columns // LANES, LANES)
    return jnp.swapaxes(a, -3, -2).reshape(*lead, rows * columns // LANES, LANES)


def unflat(a, rows, columns):
    *lead, _, _ = a.shape
    a = a.reshape(*lead, rows // SUBLANES, columns // LANES, SUBLANES, LANES)
    return jnp.swapaxes(a, -3, -2).reshape(*lead, rows, columns)


pinned = pltpu.with_memory_space_constraint


def moments(m, v, g):
    return 0.9 * m + 0.1 * g, 0.95 * v + 0.05 * g * g


def new_weight(w, m, v):
    step = m * lax.rsqrt(v + 1e-8) + 0.1 * w
    return (w - 0.02 * step).astype(jnp.bfloat16)


def direction(k):
    return (1 if k % 2 == 0 else -1), k // 2


def place(side):
    me = lax.axis_index("dp")
    return lax.div(me, side), lax.rem(me, side)


def at(k, first, second):
    return (first, second) if direction(k)[1] == 0 else (second, first)


def comm_kernel(side, layers, units, *refs):
    weights = units // layers
    grads, olds, ms, vs = (refs[i * weights : (i + 1) * weights] for i in range(4))
    refs = refs[4 * weights :]
    x_ref, refs = refs[0], refs[1:]
    parts = weights + 1
    zs, refs = refs[: parts * COLOURS], refs[parts * COLOURS :]
    gs, refs = refs[:weights], refs[weights:]
    (land1, land2, got, own1, out1, in2, own2, out2, old_v, m_v, v_v, out_w, out_g, *sems) = refs
    send_sem, recv_sem, load_sem, own_sem, store_sem, late_sem = sems
    rows = got.shape[2]
    last = side - 1
    xy = place(side)

    def turn(k, axis, by):
        way, first = direction(k)
        c = xy[first if axis == 0 else 1 - first]
        return lax.rem(c + way * by + 4 * side, side)

    def neighbour(k, axis):
        a, b = turn(k, 0, 1 if axis == 0 else 0), turn(k, 1, 1 if axis == 1 else 0)
        px, py = at(k, a, b)
        return {"dp": px * side + py}

    pl.when(lax.rem(lax.axis_index("rep"), 2) == 0)(lambda: pl.delay(STAGGER_NS))
    barrier = pltpu.get_barrier_semaphore()
    for k in range(COLOURS):
        pl.semaphore_signal(barrier, inc=1, device_id=neighbour(k, 0), device_id_type=MESH)
    pl.semaphore_wait(barrier, COLOURS)

    def of_weight(u, f):
        for w in range(weights):
            pl.when(lax.div(u, layers) == w)(functools.partial(f, w, lax.rem(u, layers)))

    def group(ref, lead, k, first):
        if direction(k)[1] == 0:
            return ref.at[lead, first, :, k]
        return ref.at[lead, :, first, k]

    def block(ref, lead, k, first, second):
        px, py = at(k, first, second)
        return ref.at[lead, px, py, k]

    def remote(stage, u, k, src, dst, axis):
        return pltpu.make_async_remote_copy(
            src_ref=src,
            dst_ref=dst,
            send_sem=send_sem.at[stage, lax.rem(u, 2), k],
            recv_sem=recv_sem.at[stage, u, k],
            device_id=neighbour(k, axis),
            device_id_type=MESH,
        )

    n1, n2 = last, last
    FIRST, SECOND, STEP = 0, n1, n1 + n2
    GATHER2, GATHER1 = STEP, STEP + n2
    stages = GATHER1 + n1 - 1

    def wait_recv(stage, u, k):
        if stage < SECOND:
            dst = land1.at[u, k, stage - FIRST]
        elif stage < STEP:
            dst = land2.at[u, k, stage - SECOND]
        elif stage < GATHER1:
            dst = block(x_ref, u, k, turn(k, 0, 0), turn(k, 1, -(stage - GATHER2) - 1))
        else:
            dst = group(x_ref, u, k, turn(k, 0, -(stage - GATHER1) - 1))
        remote(stage, u, k, dst, dst, 0).wait_recv()

    def wait_send(stage, u, k):
        small = SECOND <= stage < GATHER1
        ref = land2.at[0, k, 0] if small else land1.at[0, k, 0]
        remote(stage, u, k, ref, ref, 0).wait_send()

    def free(stage, u, k):
        pl.when(u >= 2)(lambda: wait_send(stage, u, k))

    def load(k, i, src, dst):
        return pltpu.make_async_copy(src, dst, load_sem.at[i, k])

    def own_of(stage, u, k, w, layer):
        if stage < SECOND:
            src, dst = group(grads[w], layer, k, turn(k, 0, -1 - (stage - FIRST))), own1.at[stage - FIRST - 1, k]
        else:
            src, dst = block(grads[w], layer, k, turn(k, 0, 0), turn(k, 1, -1 - (stage - SECOND))), own2.at[stage - SECOND, k]
        return pltpu.make_async_copy(src, dst, own_sem.at[stage, k])

    def state_of(k, w, layer):
        return (
            load(k, 2, block(olds[w], layer, k, turn(k, 0, 0), turn(k, 1, 0)), old_v.at[k]),
            load(k, 3, ms[w].at[layer, k], m_v.at[k]),
            load(k, 4, vs[w].at[layer, k], v_v.at[k]),
        )

    def prefetch(stage, u):
        def start(w, layer):
            for k in range(COLOURS):
                own_of(stage, u, k, w, layer).start()
                if stage == STEP:
                    for one in state_of(k, w, layer):
                        one.start()

        of_weight(u, start)

    def stage_first(s, u):
        ks = range(COLOURS)
        if s == 0:

            def start(w, layer):
                for k in ks:
                    remote(FIRST, u, k, group(grads[w], layer, k, turn(k, 0, -1)), land1.at[u, k, 0], 0).start()

            for k in ks:
                free(FIRST, u, k)
            of_weight(u, start)
            return

        for k in ks:
            wait_recv(FIRST + s - 1, u, k)
            load(k, 0, land1.at[u, k, s - 1], got.at[k]).start()
        slot = lax.rem(u, 2)
        for k in ks:
            free(FIRST + s, u, k)
            own_of(FIRST + s, u, k, 0, 0).wait()
            load(k, 0, land1.at[u, k, s - 1], got.at[k]).wait()
            out = out1.at[s - 1, slot, k]
            per = rows // CHUNK

            def add(c, _):
                j, r = lax.div(c, per), pl.multiple_of(lax.rem(c, per) * CHUNK, CHUNK)
                total = got[k, j, pl.ds(r, CHUNK)].astype(jnp.float32) + own1[s - 1, k, j, pl.ds(r, CHUNK)].astype(jnp.float32)
                out[j, pl.ds(r, CHUNK)] = total.astype(jnp.bfloat16)
                return 0

            lax.fori_loop(0, side * per, add, 0)
            remote(FIRST + s, u, k, out, land1.at[u, k, s], 0).start()

    def load_second(s, u):
        for k in range(COLOURS):
            wait_recv(SECOND + s - 1, u, k)
            load(k, 0, land1.at[u, k, n1 - 1, turn(k, 1, -1 - s)], in2.at[0, k]).start()
            if s > 0:
                load(k, 1, land2.at[u, k, s - 1], in2.at[1, k]).start()

    def wait_second(s, u, k):
        own_of(SECOND + s, u, k, 0, 0).wait()
        for i in range(2 if s > 0 else 1):
            load(k, i, land2.at[0, k, 0], in2.at[i, k]).wait()

    def sum_second(s, k, r):
        total = in2[0, k, pl.ds(r, CHUNK)].astype(jnp.float32) + own2[s, k, pl.ds(r, CHUNK)].astype(jnp.float32)
        if s > 0:
            total += in2[1, k, pl.ds(r, CHUNK)].astype(jnp.float32)
        return total.astype(jnp.bfloat16)

    def stage_second(s, u):
        load_second(s, u)
        slot = lax.rem(u, 2)
        for k in range(COLOURS):
            free(SECOND + s, u, k)
            wait_second(s, u, k)
            out = out2.at[s, slot, k]

            def add(c, _):
                r = pl.multiple_of(c * CHUNK, CHUNK)
                out[pl.ds(r, CHUNK)] = sum_second(s, k, r)
                return 0

            lax.fori_loop(0, rows // CHUNK, add, 0)
            remote(SECOND + s, u, k, out, land2.at[u, k, s], 1).start()

    def store_w(k, u, slot):
        return pltpu.make_async_copy(out_w.at[slot, k], block(x_ref, u, k, turn(k, 0, 0), turn(k, 1, 0)), store_sem.at[0, slot, k])

    def store_g(k, slot, w, layer):
        return pltpu.make_async_copy(out_g.at[slot, k], gs[w].at[layer, k], store_sem.at[1, slot, k])

    def stage_step(u):
        ks = range(COLOURS)
        load_second(n2, u)
        slot = lax.rem(u, 2)
        for k in ks:
            free(GATHER2, u, k)
            pl.when(u >= 2)(lambda: store_g(k, slot, 0, 0).wait())

            wait_second(n2, u, k)
            for one in state_of(k, 0, 0):
                one.wait()

            def adamw(c, _):
                r = pl.multiple_of(c * CHUNK, CHUNK)
                here = pl.ds(r, CHUNK)
                g = sum_second(n2, k, r)
                m, v = moments(m_v[k, here], v_v[k, here], g.astype(jnp.float32))
                out_w[slot, k, here] = new_weight(old_v[k, here].astype(jnp.float32), m, v)
                out_g[slot, k, here] = g
                return 0

            lax.fori_loop(0, rows // CHUNK, adamw, 0)
            remote(GATHER2, u, k, out_w.at[slot, k], block(x_ref, u, k, turn(k, 0, 0), turn(k, 1, 0)), 1).start()
            store_w(k, u, slot).start()

        def store_all(w, layer):
            for k in ks:
                store_g(k, slot, w, layer).start()

        of_weight(u, store_all)

    def stage_gather2(s, u):
        for k in range(COLOURS):
            if s == 1:
                store_w(k, u, lax.rem(u, 2)).wait()
            wait_recv(GATHER2 + s - 1, u, k)
            free(GATHER2 + s, u, k)
            it = block(x_ref, u, k, turn(k, 0, 0), turn(k, 1, -s))
            remote(GATHER2 + s, u, k, it, it, 1).start()

    def last_unit(k, it):
        early = rows - LATE
        z, late = zs[(weights - 1) * COLOURS + k], zs[weights * COLOURS + k]
        return (
            remote(stages - 1, units - 1, k, it.at[:, pl.ds(0, early)], z.at[:, pl.ds((layers - 1) * rows, early)], 0),
            pltpu.make_async_remote_copy(
                src_ref=it.at[:, pl.ds(early, LATE)],
                dst_ref=late,
                send_sem=late_sem.at[0, k],
                recv_sem=late_sem.at[1, k],
                device_id=neighbour(k, 0),
                device_id_type=MESH,
            ),
        )

    def stage_gather1(s, u):
        for k in range(COLOURS):
            wait_recv(GATHER1 + s - 1, u, k)
            free(GATHER1 + s, u, k)
            it = group(x_ref, u, k, turn(k, 0, -s))
            if s < n1 - 2:
                remote(GATHER1 + s, u, k, it, it, 0).start()
                continue
            for p in range(weights):
                z, layer = zs[p * COLOURS + k], u - p * layers
                mine = (layer >= 0) & (layer < (layers if p < weights - 1 else layers - 1))
                pl.when(mine)(lambda: remote(GATHER1 + s, u, k, it, z.at[:, pl.ds(layer * rows, rows)], 0).start())

            @pl.when(u == units - 1)
            def _():
                for copy in last_unit(k, it):
                    copy.start()

    def body(i, _):
        for s in range(FIRST + 1, STEP + 1):
            u = i - s
            pl.when((u >= 0) & (u < units))(functools.partial(prefetch, s, u))
        for s in range(stages):
            u = i - s
            run = (
                functools.partial(stage_first, s, u)
                if s < SECOND
                else functools.partial(stage_second, s - SECOND, u)
                if s < STEP
                else functools.partial(stage_step, u)
                if s == GATHER2
                else functools.partial(stage_gather2, s - GATHER2, u)
                if s < GATHER1
                else functools.partial(stage_gather1, s - GATHER1, u)
            )
            pl.when((u >= 0) & (u < units))(run)
        return 0

    lax.fori_loop(0, stages - 1 + units, body, 0)

    def drain(u, _):
        for k in range(COLOURS):
            wait_recv(stages - 1, u, k)
        return 0

    lax.fori_loop(0, units - 1, drain, 0)
    for s in range(stages):
        for u in range(max(units - 2, 0), units - (s == stages - 1)):
            for k in range(COLOURS):
                wait_send(s, u, k)
    for k in range(COLOURS):
        for copy in last_unit(k, land1.at[0, k, 0]):
            copy.wait_recv()
            copy.wait_send()
    for u in range(max(units - 2, 0), units):
        for k in range(COLOURS):
            store_g(k, u % 2, 0, 0).wait()


def part_rows(weights, layers, rows):
    return (layers * rows,) * (weights - 1) + (layers * rows - LATE, LATE)


def communicate(side, grads, olds, ms, vs):
    layers = grads[0].shape[0]
    weights = len(grads)
    units = weights * layers
    rows = grads[0].shape[-2]
    hops = side - 1
    hbm = pl.BlockSpec(memory_space=pltpu.HBM)
    bf16, f32 = jnp.bfloat16, jnp.float32
    shape = pltpu.HBM
    outs = [
        shape((units, *grads[0].shape[1:]), bf16),
        *[shape((side, count, LANES), bf16) for count in part_rows(weights, layers, rows) for _ in range(COLOURS)],
        *[shape((layers, COLOURS, rows, LANES), bf16)] * weights,
        shape((units, COLOURS, hops, side, rows, LANES), bf16),
        shape((units, COLOURS, hops, rows, LANES), bf16),
    ]
    stages = 4 * hops - 1
    scratch = [
        pltpu.VMEM((COLOURS, side, rows, LANES), bf16),
        pltpu.VMEM((hops - 1, COLOURS, side, rows, LANES), bf16),
        pltpu.VMEM((hops - 1, 2, COLOURS, side, rows, LANES), bf16),
        pltpu.VMEM((2, COLOURS, rows, LANES), bf16),
        pltpu.VMEM((hops + 1, COLOURS, rows, LANES), bf16),
        pltpu.VMEM((hops, 2, COLOURS, rows, LANES), bf16),
        pltpu.VMEM((COLOURS, rows, LANES), bf16),
        pltpu.VMEM((COLOURS, rows, LANES), f32),
        pltpu.VMEM((COLOURS, rows, LANES), f32),
        pltpu.VMEM((2, COLOURS, rows, LANES), bf16),
        pltpu.VMEM((2, COLOURS, rows, LANES), bf16),
        pltpu.SemaphoreType.DMA((stages, 2, COLOURS)),
        pltpu.SemaphoreType.DMA((stages, units, COLOURS)),
        pltpu.SemaphoreType.DMA((5, COLOURS)),
        pltpu.SemaphoreType.DMA((stages, COLOURS)),
        pltpu.SemaphoreType.DMA((2, 2, COLOURS)),
        pltpu.SemaphoreType.DMA((2, COLOURS)),
    ]
    got = pl.pallas_call(
        functools.partial(comm_kernel, side, layers, units),
        out_shape=outs,
        in_specs=[hbm] * (4 * weights),
        out_specs=[hbm] * len(outs),
        scratch_shapes=scratch,
        compiler_params=pltpu.CompilerParams(collective_id=0, has_side_effects=True, vmem_limit_bytes=60 << 20),
        name="sum_step_gather",
    )(*(pinned(a, pltpu.HBM) for a in (*grads, *olds, *ms, *vs)))
    x, got = got[0], got[1:]
    zs, got = got[: (weights + 1) * COLOURS], got[(weights + 1) * COLOURS :]
    return x, [zs[i * COLOURS : (i + 1) * COLOURS] for i in range(weights + 1)], got[:weights]


SLOTS = 8


def copy_kernel(jobs, n_in, *refs):
    ins, (out, buf, in_sem, out_sem, straight_sem) = refs[:n_in], refs[-5:]
    pairs = jobs(ins, out)
    staged = [pair for pair in pairs if pair[2]]
    straight = [pltpu.make_async_copy(src, dst, straight_sem.at[i]) for i, (src, dst, _) in enumerate(p for p in pairs if not p[2])]

    def slot(i):
        shape = staged[i][0].shape
        return buf.at[i % SLOTS] if len(shape) == len(buf.shape) - 1 else buf.at[i % SLOTS, 0, :, pl.ds(0, shape[1])]

    def into(i):
        return pltpu.make_async_copy(staged[i][0], slot(i), in_sem.at[i % SLOTS])

    def outof(i):
        return pltpu.make_async_copy(slot(i), staged[i][1], out_sem.at[i % SLOTS])

    ahead = SLOTS // 2
    for copy in straight:
        copy.start()
    for i in range(len(staged) + ahead):
        if i < len(staged):
            if i >= SLOTS:
                outof(i - SLOTS).wait()
            into(i).start()
        if ahead <= i:
            into(i - ahead).wait()
            outof(i - ahead).start()
    for i in range(max(len(staged) - SLOTS, 0), len(staged)):
        outof(i).wait()
    for copy in straight:
        copy.wait()


def copies(jobs, ins, space, shape, moved, onto=None):
    hbm = pl.BlockSpec(memory_space=pltpu.HBM)
    side, rows = shape[1], shape[-2]
    given = [pinned(a, space) for a in ins] + ([] if onto is None else [pinned(onto, pltpu.HBM)])
    return pl.pallas_call(
        functools.partial(copy_kernel, jobs, len(ins)),
        out_shape=pltpu.HBM(shape, jnp.bfloat16),
        in_specs=[pl.BlockSpec(memory_space=space)] * len(ins) + [hbm] * (onto is not None),
        out_specs=hbm,
        scratch_shapes=[
            pltpu.VMEM((SLOTS if onto is None else 1, shape[0], side, rows, LANES), jnp.bfloat16),
            pltpu.SemaphoreType.DMA((SLOTS,)),
            pltpu.SemaphoreType.DMA((SLOTS,)),
            pltpu.SemaphoreType.DMA((SLOTS,)),
        ],
        input_output_aliases={} if onto is None else {len(ins): 0},
        compiler_params=pltpu.CompilerParams(vmem_limit_bytes=(16 if onto is None else 8) << 20),
        cost_estimate=pl.CostEstimate(flops=4 * moved, bytes_accessed=4 * moved, transcendentals=0),
        name="place" if onto is None else "place_last",
    )(*given)


def solution(mesh):
    n = mesh.shape["dp"]
    side = math.isqrt(n)
    hops = side - 1

    def ring(k):
        way, axis = direction(k)
        pairs = []
        for i in range(n):
            c = [i // side, i % side]
            c[axis] = (c[axis] + way) % side
            pairs.append((i, c[0] * side + c[1]))
        return pairs

    def group(ref, lead, k, back):
        way, axis = direction(k)
        first = lax.rem(place(side)[axis] - way * back + 4 * side, side)
        return ref.at[lead, first, :, k] if axis == 0 else ref.at[lead, :, first, k]

    def step(*arrays):
        terms, weights, m, v = (arrays[i : i + 3] for i in (0, 3, 6, 9))
        layers = m[0].shape[0]
        rows = m[0].shape[1] * m[0].shape[2] // LANES // COLOURS
        by_block = (layers, side, side, COLOURS, rows, LANES)
        grads = [flat(t[0]).reshape(by_block) for t in terms]
        olds = [flat(w).reshape(by_block) for w in weights]
        own_m, own_v = ([flat(one).reshape(layers, COLOURS, rows, LANES) for one in ones] for ones in (m, v))
        x, zs, sums = communicate(side, grads, olds, own_m, own_v)
        ys = [[lax.ppermute(z, "dp", ring(k)) for k, z in enumerate(part)] for part in zs]

        new_m, new_v = [], []
        for one_m, one_v, g in zip(m, v, sums, strict=True):
            g = unflat(g.reshape(layers, COLOURS * rows, LANES), *one_m.shape[1:]).astype(jnp.float32)
            a, b = moments(one_m, one_v, g)
            new_m.append(a)
            new_v.append(b)

        end = len(weights) - 1

        def pieces(p, part, out, k, back):
            pairs = []
            for layer in range(layers):
                here = group(out, layer, k, back)
                cut = rows - LATE if p >= end and layer == layers - 1 else rows
                if p <= end:
                    pairs.append((part.at[:, pl.ds(layer * rows, cut)], here.at[:, pl.ds(0, cut)]))
                elif cut < rows:
                    pairs.append((part, here.at[:, pl.ds(cut, LATE)]))
            return pairs

        whole = []
        for i in range(len(weights)):
            used = (i, i + 1) if i == end else (i,)

            def placed(ins, out, i=i, used=used):
                pairs = []
                for k in range(COLOURS):
                    for back in range(hops - 1):
                        here = group(out, pl.ds(0, layers), k, back)
                        pairs.append((group(ins[0], pl.ds(i * layers, layers), k, back), here, True))
                    for j, p in enumerate(used):
                        pairs += [(*pair, True) for pair in pieces(p, ins[1 + j * COLOURS + k], out, k, hops - 1)]
                return pairs

            ins = [x, *(z for p in used for z in zs[p])]
            whole.append(copies(placed, ins, pltpu.HBM, by_block, layers * n * COLOURS * rows * LANES))

        for p, count in enumerate(part_rows(len(weights), layers, rows)):
            if p > 0:
                ys[p], whole = lax.optimization_barrier((ys[p], whole))

            def last(ins, out, p=p):
                return [(*pair, False) for k in range(COLOURS) for pair in pieces(p, ins[k], out, k, hops)]

            i = min(p, end)
            whole[i] = copies(last, ys[p], pltpu.VMEM, by_block, COLOURS * side * count * LANES, onto=whole[i])
        whole = [unflat(one.reshape(layers, n * COLOURS * rows, LANES), *w.shape[1:]) for one, w in zip(whole, weights, strict=True)]
        return (*whole, *new_m, *new_v)

    all_of, cut = P(None, None, None), P(None, "dp", None)
    return jax.shard_map(
        step,
        mesh=mesh,
        in_specs=(P(("rep", "dp"), None, None, None),) * 3 + (all_of,) * 3 + (cut,) * 6,
        out_specs=(P("rep", None, None),) * 3 + (P("rep", "dp", None),) * 6,
        check_vma=False,
    )
```

```python
import functools
import math

import jax
import jax.numpy as jnp
from jax import lax
from jax.experimental import pallas as pl
from jax.experimental.pallas import tpu as pltpu
from jax.sharding import PartitionSpec as P

MESH = pl.DeviceIdType.MESH
LANES, SUBLANES = 128, 8
COLOURS = 4
CHUNK = 128
STAGGER_NS = 12000
LATE = 256


def flat(a):
    *lead, rows, columns = a.shape
    a = a.reshape(*lead, rows // SUBLANES, SUBLANES, columns // LANES, LANES)
    return jnp.swapaxes(a, -3, -2).reshape(*lead, rows * columns // LANES, LANES)


def unflat(a, rows, columns):
    *lead, _, _ = a.shape
    a = a.reshape(*lead, rows // SUBLANES, columns // LANES, SUBLANES, LANES)
    return jnp.swapaxes(a, -3, -2).reshape(*lead, rows, columns)


pinned = pltpu.with_memory_space_constraint


def moments(m, v, g):
    return 0.9 * m + 0.1 * g, 0.95 * v + 0.05 * g * g


def new_weight(w, m, v):
    step = m * lax.rsqrt(v + 1e-8) + 0.1 * w
    return (w - 0.02 * step).astype(jnp.bfloat16)


def direction(k):
    return (1 if k % 2 == 0 else -1), k // 2


def place(side):
    me = lax.axis_index("dp")
    return lax.div(me, side), lax.rem(me, side)


def at(k, first, second):
    return (first, second) if direction(k)[1] == 0 else (second, first)


def comm_kernel(side, layers, units, *refs):
    weights = units // layers
    grads, olds, ms, vs = (refs[i * weights : (i + 1) * weights] for i in range(4))
    refs = refs[4 * weights :]
    x_ref, refs = refs[0], refs[1:]
    parts = weights + 1
    zs, refs = refs[: parts * COLOURS], refs[parts * COLOURS :]
    gs, refs = refs[:weights], refs[weights:]
    (land1, land2, got, own1, out1, in2, own2, out2, old_v, m_v, v_v, out_w, out_g, *sems) = refs
    send_sem, recv_sem, load_sem, own_sem, sum_sem, store_sem, late_sem = sems
    rows = got.shape[2]
    last = side - 1
    xy = place(side)

    def turn(k, axis, by):
        way, first = direction(k)
        c = xy[first if axis == 0 else 1 - first]
        return lax.rem(c + way * by + 4 * side, side)

    def neighbour(k, axis):
        a, b = turn(k, 0, 1 if axis == 0 else 0), turn(k, 1, 1 if axis == 1 else 0)
        px, py = at(k, a, b)
        return {"dp": px * side + py}

    pl.when(lax.rem(lax.axis_index("rep"), 2) == 0)(lambda: pl.delay(STAGGER_NS))
    barrier = pltpu.get_barrier_semaphore()
    for k in range(COLOURS):
        pl.semaphore_signal(barrier, inc=1, device_id=neighbour(k, 0), device_id_type=MESH)
    pl.semaphore_wait(barrier, COLOURS)

    def of_weight(u, f):
        for w in range(weights):
            pl.when(lax.div(u, layers) == w)(functools.partial(f, w, lax.rem(u, layers)))

    def group(ref, lead, k, first):
        if direction(k)[1] == 0:
            return ref.at[lead, first, :, k]
        return ref.at[lead, :, first, k]

    def block(ref, lead, k, first, second):
        px, py = at(k, first, second)
        return ref.at[lead, px, py, k]

    def remote(stage, u, k, src, dst, axis):
        return pltpu.make_async_remote_copy(
            src_ref=src,
            dst_ref=dst,
            send_sem=send_sem.at[stage, lax.rem(u, 2), k],
            recv_sem=recv_sem.at[stage, u, k],
            device_id=neighbour(k, axis),
            device_id_type=MESH,
        )

    n1, n2 = last, last
    FIRST, SECOND, STEP = 0, n1, n1 + n2
    GATHER2, GATHER1 = STEP, STEP + n2
    stages = GATHER1 + n1 - 1

    def wait_recv(stage, u, k):
        if stage < SECOND:
            dst = land1.at[u, k, stage - FIRST]
        elif stage < STEP:
            dst = land2.at[u, k, stage - SECOND]
        elif stage < GATHER1:
            dst = block(x_ref, u, k, turn(k, 0, 0), turn(k, 1, -(stage - GATHER2) - 1))
        else:
            dst = group(x_ref, u, k, turn(k, 0, -(stage - GATHER1) - 1))
        remote(stage, u, k, dst, dst, 0).wait_recv()

    def wait_send(stage, u, k):
        small = SECOND <= stage < GATHER1
        ref = land2.at[0, k, 0] if small else land1.at[0, k, 0]
        remote(stage, u, k, ref, ref, 0).wait_send()

    def free(stage, u, k):
        pl.when(u >= 2)(lambda: wait_send(stage, u, k))

    def load(k, i, src, dst):
        return pltpu.make_async_copy(src, dst, load_sem.at[i, k])

    def own_of(stage, u, k, w, layer):
        if stage < SECOND:
            src, dst = group(grads[w], layer, k, turn(k, 0, -1 - (stage - FIRST))), own1.at[stage - FIRST - 1, k]
        else:
            src, dst = block(grads[w], layer, k, turn(k, 0, 0), turn(k, 1, -1 - (stage - SECOND))), own2.at[stage - SECOND, k]
        return pltpu.make_async_copy(src, dst, own_sem.at[stage, k])

    def sum_of(stage, u, k):
        s = stage - SECOND
        return pltpu.make_async_copy(land1.at[u, k, n1 - 1, turn(k, 1, -1 - s)], in2.at[s, k], sum_sem.at[s, k])

    def state_of(k, w, layer):
        return (
            load(k, 1, block(olds[w], layer, k, turn(k, 0, 0), turn(k, 1, 0)), old_v.at[k]),
            load(k, 2, ms[w].at[layer, k], m_v.at[k]),
            load(k, 3, vs[w].at[layer, k], v_v.at[k]),
        )

    def prefetch(stage, u):
        def start(w, layer):
            for k in range(COLOURS):
                own_of(stage, u, k, w, layer).start()
                if stage == STEP:
                    for one in state_of(k, w, layer):
                        one.start()

        of_weight(u, start)
        if stage > SECOND:
            for k in range(COLOURS):
                sum_of(stage, u, k).start()

    def stage_first(s, u):
        ks = range(COLOURS)
        if s == 0:

            def start(w, layer):
                for k in ks:
                    remote(FIRST, u, k, group(grads[w], layer, k, turn(k, 0, -1)), land1.at[u, k, 0], 0).start()

            for k in ks:
                free(FIRST, u, k)
            of_weight(u, start)
            return

        for k in ks:
            wait_recv(FIRST + s - 1, u, k)
            load(k, 0, land1.at[u, k, s - 1], got.at[k]).start()
        slot = lax.rem(u, 2)
        for k in ks:
            free(FIRST + s, u, k)
            own_of(FIRST + s, u, k, 0, 0).wait()
            load(k, 0, land1.at[u, k, s - 1], got.at[k]).wait()
            out = out1.at[s - 1, slot, k]
            per = rows // CHUNK

            def add(c, _):
                j, r = lax.div(c, per), pl.multiple_of(lax.rem(c, per) * CHUNK, CHUNK)
                total = got[k, j, pl.ds(r, CHUNK)].astype(jnp.float32) + own1[s - 1, k, j, pl.ds(r, CHUNK)].astype(jnp.float32)
                out[j, pl.ds(r, CHUNK)] = total.astype(jnp.bfloat16)
                return 0

            lax.fori_loop(0, side * per, add, 0)
            remote(FIRST + s, u, k, out, land1.at[u, k, s], 0).start()

    def load_second(s, u):
        for k in range(COLOURS):
            wait_recv(SECOND + s - 1, u, k)
            if s == 0:
                sum_of(SECOND, u, k).start()

    def wait_second(s, u, k):
        own_of(SECOND + s, u, k, 0, 0).wait()
        sum_of(SECOND + s, u, k).wait()

    def sum_second(s, u, k, r):
        total = in2[s, k, pl.ds(r, CHUNK)].astype(jnp.float32) + own2[s, k, pl.ds(r, CHUNK)].astype(jnp.float32)
        if s > 0:
            total += land2[u, k, s - 1, pl.ds(r, CHUNK)].astype(jnp.float32)
        return total.astype(jnp.bfloat16)

    def stage_second(s, u):
        load_second(s, u)
        slot = lax.rem(u, 2)
        for k in range(COLOURS):
            free(SECOND + s, u, k)
            wait_second(s, u, k)
            out = out2.at[s, slot, k]

            def add(c, _):
                r = pl.multiple_of(c * CHUNK, CHUNK)
                out[pl.ds(r, CHUNK)] = sum_second(s, u, k, r)
                return 0

            lax.fori_loop(0, rows // CHUNK, add, 0)
            remote(SECOND + s, u, k, out, land2.at[u, k, s], 1).start()

    def store_w(k, u, slot):
        return pltpu.make_async_copy(out_w.at[slot, k], block(x_ref, u, k, turn(k, 0, 0), turn(k, 1, 0)), store_sem.at[0, slot, k])

    def store_g(k, slot, w, layer):
        return pltpu.make_async_copy(out_g.at[slot, k], gs[w].at[layer, k], store_sem.at[1, slot, k])

    def stage_step(u):
        ks = range(COLOURS)
        load_second(n2, u)
        slot = lax.rem(u, 2)
        for k in ks:
            free(GATHER2, u, k)
            pl.when(u >= 2)(lambda: store_g(k, slot, 0, 0).wait())

            wait_second(n2, u, k)
            for one in state_of(k, 0, 0):
                one.wait()

            def adamw(c, _):
                r = pl.multiple_of(c * CHUNK, CHUNK)
                here = pl.ds(r, CHUNK)
                g = sum_second(n2, u, k, r)
                m, v = moments(m_v[k, here], v_v[k, here], g.astype(jnp.float32))
                out_w[slot, k, here] = new_weight(old_v[k, here].astype(jnp.float32), m, v)
                out_g[slot, k, here] = g
                return 0

            lax.fori_loop(0, rows // CHUNK, adamw, 0)
            remote(GATHER2, u, k, out_w.at[slot, k], block(x_ref, u, k, turn(k, 0, 0), turn(k, 1, 0)), 1).start()
            store_w(k, u, slot).start()

        def store_all(w, layer):
            for k in ks:
                store_g(k, slot, w, layer).start()

        of_weight(u, store_all)

    def stage_gather2(s, u):
        for k in range(COLOURS):
            if s == 1:
                store_w(k, u, lax.rem(u, 2)).wait()
            wait_recv(GATHER2 + s - 1, u, k)
            free(GATHER2 + s, u, k)
            it = block(x_ref, u, k, turn(k, 0, 0), turn(k, 1, -s))
            remote(GATHER2 + s, u, k, it, it, 1).start()

    def last_unit(k, it):
        early = rows - LATE
        z, late = zs[(weights - 1) * COLOURS + k], zs[weights * COLOURS + k]
        return (
            remote(stages - 1, units - 1, k, it.at[:, pl.ds(0, early)], z.at[:, pl.ds((layers - 1) * rows, early)], 0),
            pltpu.make_async_remote_copy(
                src_ref=it.at[:, pl.ds(early, LATE)],
                dst_ref=late,
                send_sem=late_sem.at[0, k],
                recv_sem=late_sem.at[1, k],
                device_id=neighbour(k, 0),
                device_id_type=MESH,
            ),
        )

    def stage_gather1(s, u):
        for k in range(COLOURS):
            wait_recv(GATHER1 + s - 1, u, k)
            free(GATHER1 + s, u, k)
            it = group(x_ref, u, k, turn(k, 0, -s))
            if s < n1 - 2:
                remote(GATHER1 + s, u, k, it, it, 0).start()
                continue
            for p in range(weights):
                z, layer = zs[p * COLOURS + k], u - p * layers
                mine = (layer >= 0) & (layer < (layers if p < weights - 1 else layers - 1))
                pl.when(mine)(lambda: remote(GATHER1 + s, u, k, it, z.at[:, pl.ds(layer * rows, rows)], 0).start())

            @pl.when(u == units - 1)
            def _():
                for copy in last_unit(k, it):
                    copy.start()

    def body(i, _):
        for s in range(FIRST + 1, STEP + 1):
            u = i - s
            pl.when((u >= 0) & (u < units))(functools.partial(prefetch, s, u))
        for s in range(stages):
            u = i - s
            run = (
                functools.partial(stage_first, s, u)
                if s < SECOND
                else functools.partial(stage_second, s - SECOND, u)
                if s < STEP
                else functools.partial(stage_step, u)
                if s == GATHER2
                else functools.partial(stage_gather2, s - GATHER2, u)
                if s < GATHER1
                else functools.partial(stage_gather1, s - GATHER1, u)
            )
            pl.when((u >= 0) & (u < units))(run)
        return 0

    lax.fori_loop(0, stages - 1 + units, body, 0)

    def drain(u, _):
        for k in range(COLOURS):
            wait_recv(stages - 1, u, k)
        return 0

    lax.fori_loop(0, units - 1, drain, 0)
    for s in range(stages):
        for u in range(max(units - 2, 0), units - (s == stages - 1)):
            for k in range(COLOURS):
                wait_send(s, u, k)
    for k in range(COLOURS):
        for copy in last_unit(k, land1.at[0, k, 0]):
            copy.wait_recv()
            copy.wait_send()
    for u in range(max(units - 2, 0), units):
        for k in range(COLOURS):
            store_g(k, u % 2, 0, 0).wait()


def part_rows(weights, layers, rows):
    return (layers * rows,) * (weights - 1) + (layers * rows - LATE, LATE)


def communicate(side, grads, olds, ms, vs):
    layers = grads[0].shape[0]
    weights = len(grads)
    units = weights * layers
    rows = grads[0].shape[-2]
    hops = side - 1
    hbm = pl.BlockSpec(memory_space=pltpu.HBM)
    bf16, f32 = jnp.bfloat16, jnp.float32
    shape = pltpu.HBM
    outs = [
        shape((units, *grads[0].shape[1:]), bf16),
        *[shape((side, count, LANES), bf16) for count in part_rows(weights, layers, rows) for _ in range(COLOURS)],
        *[shape((layers, COLOURS, rows, LANES), bf16)] * weights,
        shape((units, COLOURS, hops, side, rows, LANES), bf16),
    ]
    stages = 4 * hops - 1
    scratch = [
        pltpu.VMEM((units, COLOURS, hops, rows, LANES), bf16),
        pltpu.VMEM((COLOURS, side, rows, LANES), bf16),
        pltpu.VMEM((hops - 1, COLOURS, side, rows, LANES), bf16),
        pltpu.VMEM((hops - 1, 2, COLOURS, side, rows, LANES), bf16),
        pltpu.VMEM((hops + 1, COLOURS, rows, LANES), bf16),
        pltpu.VMEM((hops + 1, COLOURS, rows, LANES), bf16),
        pltpu.VMEM((hops, 2, COLOURS, rows, LANES), bf16),
        pltpu.VMEM((COLOURS, rows, LANES), bf16),
        pltpu.VMEM((COLOURS, rows, LANES), f32),
        pltpu.VMEM((COLOURS, rows, LANES), f32),
        pltpu.VMEM((2, COLOURS, rows, LANES), bf16),
        pltpu.VMEM((2, COLOURS, rows, LANES), bf16),
        pltpu.SemaphoreType.DMA((stages, 2, COLOURS)),
        pltpu.SemaphoreType.DMA((stages, units, COLOURS)),
        pltpu.SemaphoreType.DMA((4, COLOURS)),
        pltpu.SemaphoreType.DMA((stages, COLOURS)),
        pltpu.SemaphoreType.DMA((hops + 1, COLOURS)),
        pltpu.SemaphoreType.DMA((2, 2, COLOURS)),
        pltpu.SemaphoreType.DMA((2, COLOURS)),
    ]
    got = pl.pallas_call(
        functools.partial(comm_kernel, side, layers, units),
        out_shape=outs,
        in_specs=[hbm] * (4 * weights),
        out_specs=[hbm] * len(outs),
        scratch_shapes=scratch,
        compiler_params=pltpu.CompilerParams(collective_id=0, has_side_effects=True, vmem_limit_bytes=60 << 20),
        name="sum_step_gather",
    )(*(pinned(a, pltpu.HBM) for a in (*grads, *olds, *ms, *vs)))
    x, got = got[0], got[1:]
    zs, got = got[: (weights + 1) * COLOURS], got[(weights + 1) * COLOURS :]
    return x, [zs[i * COLOURS : (i + 1) * COLOURS] for i in range(weights + 1)], got[:weights]


SLOTS = 8


def copy_kernel(jobs, n_in, *refs):
    ins, (out, buf, in_sem, out_sem, straight_sem) = refs[:n_in], refs[-5:]
    pairs = jobs(ins, out)
    staged = [pair for pair in pairs if pair[2]]
    straight = [pltpu.make_async_copy(src, dst, straight_sem.at[i]) for i, (src, dst, _) in enumerate(p for p in pairs if not p[2])]

    def slot(i):
        shape = staged[i][0].shape
        return buf.at[i % SLOTS] if len(shape) == len(buf.shape) - 1 else buf.at[i % SLOTS, 0, :, pl.ds(0, shape[1])]

    def into(i):
        return pltpu.make_async_copy(staged[i][0], slot(i), in_sem.at[i % SLOTS])

    def outof(i):
        return pltpu.make_async_copy(slot(i), staged[i][1], out_sem.at[i % SLOTS])

    ahead = SLOTS // 2
    for copy in straight:
        copy.start()
    for i in range(len(staged) + ahead):
        if i < len(staged):
            if i >= SLOTS:
                outof(i - SLOTS).wait()
            into(i).start()
        if ahead <= i:
            into(i - ahead).wait()
            outof(i - ahead).start()
    for i in range(max(len(staged) - SLOTS, 0), len(staged)):
        outof(i).wait()
    for copy in straight:
        copy.wait()


def copies(jobs, ins, space, shape, moved, onto=None):
    hbm = pl.BlockSpec(memory_space=pltpu.HBM)
    side, rows = shape[1], shape[-2]
    given = [pinned(a, space) for a in ins] + ([] if onto is None else [pinned(onto, pltpu.HBM)])
    return pl.pallas_call(
        functools.partial(copy_kernel, jobs, len(ins)),
        out_shape=pltpu.HBM(shape, jnp.bfloat16),
        in_specs=[pl.BlockSpec(memory_space=space)] * len(ins) + [hbm] * (onto is not None),
        out_specs=hbm,
        scratch_shapes=[
            pltpu.VMEM((SLOTS if onto is None else 1, shape[0], side, rows, LANES), jnp.bfloat16),
            pltpu.SemaphoreType.DMA((SLOTS,)),
            pltpu.SemaphoreType.DMA((SLOTS,)),
            pltpu.SemaphoreType.DMA((SLOTS,)),
        ],
        input_output_aliases={} if onto is None else {len(ins): 0},
        compiler_params=pltpu.CompilerParams(vmem_limit_bytes=(16 if onto is None else 8) << 20),
        cost_estimate=pl.CostEstimate(flops=4 * moved, bytes_accessed=4 * moved, transcendentals=0),
        name="place" if onto is None else "place_last",
    )(*given)


def solution(mesh):
    n = mesh.shape["dp"]
    side = math.isqrt(n)
    hops = side - 1

    def ring(k):
        way, axis = direction(k)
        pairs = []
        for i in range(n):
            c = [i // side, i % side]
            c[axis] = (c[axis] + way) % side
            pairs.append((i, c[0] * side + c[1]))
        return pairs

    def group(ref, lead, k, back):
        way, axis = direction(k)
        first = lax.rem(place(side)[axis] - way * back + 4 * side, side)
        return ref.at[lead, first, :, k] if axis == 0 else ref.at[lead, :, first, k]

    def step(*arrays):
        terms, weights, m, v = (arrays[i : i + 3] for i in (0, 3, 6, 9))
        layers = m[0].shape[0]
        rows = m[0].shape[1] * m[0].shape[2] // LANES // COLOURS
        by_block = (layers, side, side, COLOURS, rows, LANES)
        grads = [flat(t[0]).reshape(by_block) for t in terms]
        olds = [flat(w).reshape(by_block) for w in weights]
        own_m, own_v = ([flat(one).reshape(layers, COLOURS, rows, LANES) for one in ones] for ones in (m, v))
        x, zs, sums = communicate(side, grads, olds, own_m, own_v)
        ys = [[lax.ppermute(z, "dp", ring(k)) for k, z in enumerate(part)] for part in zs]

        new_m, new_v = [], []
        for one_m, one_v, g in zip(m, v, sums, strict=True):
            g = unflat(g.reshape(layers, COLOURS * rows, LANES), *one_m.shape[1:]).astype(jnp.float32)
            a, b = moments(one_m, one_v, g)
            new_m.append(a)
            new_v.append(b)

        end = len(weights) - 1

        def pieces(p, part, out, k, back):
            pairs = []
            for layer in range(layers):
                here = group(out, layer, k, back)
                cut = rows - LATE if p >= end and layer == layers - 1 else rows
                if p <= end:
                    pairs.append((part.at[:, pl.ds(layer * rows, cut)], here.at[:, pl.ds(0, cut)]))
                elif cut < rows:
                    pairs.append((part, here.at[:, pl.ds(cut, LATE)]))
            return pairs

        whole = []
        for i in range(len(weights)):
            used = (i, i + 1) if i == end else (i,)

            def placed(ins, out, i=i, used=used):
                pairs = []
                for k in range(COLOURS):
                    for back in range(hops - 1):
                        here = group(out, pl.ds(0, layers), k, back)
                        pairs.append((group(ins[0], pl.ds(i * layers, layers), k, back), here, True))
                    for j, p in enumerate(used):
                        pairs += [(*pair, True) for pair in pieces(p, ins[1 + j * COLOURS + k], out, k, hops - 1)]
                return pairs

            ins = [x, *(z for p in used for z in zs[p])]
            whole.append(copies(placed, ins, pltpu.HBM, by_block, layers * n * COLOURS * rows * LANES))

        for p, count in enumerate(part_rows(len(weights), layers, rows)):
            if p > 0:
                ys[p], whole = lax.optimization_barrier((ys[p], whole))

            def last(ins, out, p=p):
                return [(*pair, False) for k in range(COLOURS) for pair in pieces(p, ins[k], out, k, hops)]

            i = min(p, end)
            whole[i] = copies(last, ys[p], pltpu.VMEM, by_block, COLOURS * side * count * LANES, onto=whole[i])
        whole = [unflat(one.reshape(layers, n * COLOURS * rows, LANES), *w.shape[1:]) for one, w in zip(whole, weights, strict=True)]
        return (*whole, *new_m, *new_v)

    all_of, cut = P(None, None, None), P(None, "dp", None)
    return jax.shard_map(
        step,
        mesh=mesh,
        in_specs=(P(("rep", "dp"), None, None, None),) * 3 + (all_of,) * 3 + (cut,) * 6,
        out_specs=(P("rep", None, None),) * 3 + (P("rep", "dp", None),) * 6,
        check_vma=False,
    )
```

```python
import functools
import math

import jax
import jax.numpy as jnp
from jax import lax
from jax.experimental import pallas as pl
from jax.experimental.pallas import tpu as pltpu
from jax.sharding import PartitionSpec as P

MESH = pl.DeviceIdType.MESH
LANES, SUBLANES = 128, 8
COLOURS = 4
CHUNK = 128
STAGGER_NS = 12000
LATE = 256


def flat(a):
    *lead, rows, columns = a.shape
    a = a.reshape(*lead, rows // SUBLANES, SUBLANES, columns // LANES, LANES)
    return jnp.swapaxes(a, -3, -2).reshape(*lead, rows * columns // LANES, LANES)


def unflat(a, rows, columns):
    *lead, _, _ = a.shape
    a = a.reshape(*lead, rows // SUBLANES, columns // LANES, SUBLANES, LANES)
    return jnp.swapaxes(a, -3, -2).reshape(*lead, rows, columns)


pinned = pltpu.with_memory_space_constraint


def moments(m, v, g):
    return 0.9 * m + 0.1 * g, 0.95 * v + 0.05 * g * g


def new_weight(w, m, v):
    step = m * lax.rsqrt(v + 1e-8) + 0.1 * w
    return (w - 0.02 * step).astype(jnp.bfloat16)


def direction(k):
    return (1 if k % 2 == 0 else -1), k // 2


def place(side):
    me = lax.axis_index("dp")
    return lax.div(me, side), lax.rem(me, side)


def at(k, first, second):
    return (first, second) if direction(k)[1] == 0 else (second, first)


def comm_kernel(side, layers, units, *refs):
    weights = units // layers
    grads, olds, ms, vs = (refs[i * weights : (i + 1) * weights] for i in range(4))
    refs = refs[4 * weights :]
    x_ref, refs = refs[0], refs[1:]
    parts = weights + 1
    zs, refs = refs[: parts * COLOURS], refs[parts * COLOURS :]
    gs, refs = refs[:weights], refs[weights:]
    (land1, land2, got, own1, out1, in2, own2, out2, old_v, m_v, v_v, out_w, out_g, *sems) = refs
    send_sem, recv_sem, load_sem, own_sem, sum_sem, store_sem, late_sem, ready_sem = sems
    rows = got.shape[2]
    last = side - 1
    xy = place(side)

    def turn(k, axis, by):
        way, first = direction(k)
        c = xy[first if axis == 0 else 1 - first]
        return lax.rem(c + way * by + 4 * side, side)

    def neighbour(k, axis):
        a, b = turn(k, 0, 1 if axis == 0 else 0), turn(k, 1, 1 if axis == 1 else 0)
        px, py = at(k, a, b)
        return {"dp": px * side + py}

    pl.when(lax.rem(lax.axis_index("rep"), 2) == 0)(lambda: pl.delay(STAGGER_NS))
    def of_weight(u, f):
        for w in range(weights):
            pl.when(lax.div(u, layers) == w)(functools.partial(f, w, lax.rem(u, layers)))

    def group(ref, lead, k, first):
        if direction(k)[1] == 0:
            return ref.at[lead, first, :, k]
        return ref.at[lead, :, first, k]

    def block(ref, lead, k, first, second):
        px, py = at(k, first, second)
        return ref.at[lead, px, py, k]

    def remote(stage, u, k, src, dst, axis):
        return pltpu.make_async_remote_copy(
            src_ref=src,
            dst_ref=dst,
            send_sem=send_sem.at[stage, lax.rem(u, 2), k],
            recv_sem=recv_sem.at[stage, u, k],
            device_id=neighbour(k, axis),
            device_id_type=MESH,
        )

    n1, n2 = last, last
    FIRST, SECOND, STEP = 0, n1, n1 + n2
    GATHER2, GATHER1 = STEP, STEP + n2
    stages = GATHER1 + n1 - 1

    def wait_recv(stage, u, k):
        if stage < SECOND:
            dst = land1.at[u, k, stage - FIRST]
        elif stage < STEP:
            dst = land2.at[u, k, stage - SECOND]
        elif stage < GATHER1:
            dst = block(x_ref, u, k, turn(k, 0, 0), turn(k, 1, -(stage - GATHER2) - 1))
        else:
            dst = group(x_ref, u, k, turn(k, 0, -(stage - GATHER1) - 1))
        remote(stage, u, k, dst, dst, 0).wait_recv()

    def wait_send(stage, u, k):
        small = SECOND <= stage < GATHER1
        ref = land2.at[0, k, 0] if small else land1.at[0, k, 0]
        remote(stage, u, k, ref, ref, 0).wait_send()

    def free(stage, u, k):
        pl.when(u >= 2)(lambda: wait_send(stage, u, k))

    def load(k, i, src, dst):
        return pltpu.make_async_copy(src, dst, load_sem.at[i, k])

    def own_of(stage, u, k, w, layer):
        if stage < SECOND:
            src, dst = group(grads[w], layer, k, turn(k, 0, -1 - (stage - FIRST))), own1.at[stage - FIRST - 1, k]
        else:
            src, dst = block(grads[w], layer, k, turn(k, 0, 0), turn(k, 1, -1 - (stage - SECOND))), own2.at[stage - SECOND, k]
        return pltpu.make_async_copy(src, dst, own_sem.at[stage, k])

    def sum_of(stage, u, k):
        s = stage - SECOND
        return pltpu.make_async_copy(land1.at[u, k, n1 - 1, turn(k, 1, -1 - s)], in2.at[s, k], sum_sem.at[s, k])

    def state_of(k, w, layer):
        return (
            load(k, 1, block(olds[w], layer, k, turn(k, 0, 0), turn(k, 1, 0)), old_v.at[k]),
            load(k, 2, ms[w].at[layer, k], m_v.at[k]),
            load(k, 3, vs[w].at[layer, k], v_v.at[k]),
        )

    def prefetch(stage, u):
        def start(w, layer):
            for k in range(COLOURS):
                own_of(stage, u, k, w, layer).start()
                if stage == STEP:
                    for one in state_of(k, w, layer):
                        one.start()

        of_weight(u, start)
        if stage > SECOND:
            for k in range(COLOURS):
                sum_of(stage, u, k).start()

    def stage_first(s, u):
        ks = range(COLOURS)
        if s == 0:

            def start(w, layer):
                for k in ks:
                    remote(FIRST, u, k, group(grads[w], layer, k, turn(k, 0, -1)), land1.at[u, k, 0], 0).start()

            for k in ks:
                free(FIRST, u, k)
            pl.when(u > 0)(lambda: of_weight(u, start))
            return

        for k in ks:
            wait_recv(FIRST + s - 1, u, k)
            load(k, 0, land1.at[u, k, s - 1], got.at[k]).start()
        slot = lax.rem(u, 2)
        for k in ks:
            free(FIRST + s, u, k)
            own_of(FIRST + s, u, k, 0, 0).wait()
            load(k, 0, land1.at[u, k, s - 1], got.at[k]).wait()
            out = out1.at[s - 1, slot, k]
            per = rows // CHUNK

            def add(c, _):
                j, r = lax.div(c, per), pl.multiple_of(lax.rem(c, per) * CHUNK, CHUNK)
                total = got[k, j, pl.ds(r, CHUNK)].astype(jnp.float32) + own1[s - 1, k, j, pl.ds(r, CHUNK)].astype(jnp.float32)
                out[j, pl.ds(r, CHUNK)] = total.astype(jnp.bfloat16)
                return 0

            lax.fori_loop(0, side * per, add, 0)
            remote(FIRST + s, u, k, out, land1.at[u, k, s], 0).start()

    def load_second(s, u):
        for k in range(COLOURS):
            wait_recv(SECOND + s - 1, u, k)
            if s == 0:
                sum_of(SECOND, u, k).start()

    def wait_second(s, u, k):
        own_of(SECOND + s, u, k, 0, 0).wait()
        sum_of(SECOND + s, u, k).wait()

    def sum_second(s, u, k, r):
        total = in2[s, k, pl.ds(r, CHUNK)].astype(jnp.float32) + own2[s, k, pl.ds(r, CHUNK)].astype(jnp.float32)
        if s > 0:
            total += land2[u, k, s - 1, pl.ds(r, CHUNK)].astype(jnp.float32)
        return total.astype(jnp.bfloat16)

    def stage_second(s, u):
        load_second(s, u)
        slot = lax.rem(u, 2)
        for k in range(COLOURS):
            free(SECOND + s, u, k)
            wait_second(s, u, k)
            out = out2.at[s, slot, k]

            def add(c, _):
                r = pl.multiple_of(c * CHUNK, CHUNK)
                out[pl.ds(r, CHUNK)] = sum_second(s, u, k, r)
                return 0

            lax.fori_loop(0, rows // CHUNK, add, 0)
            remote(SECOND + s, u, k, out, land2.at[u, k, s], 1).start()

    def store_w(k, u, slot):
        return pltpu.make_async_copy(out_w.at[slot, k], block(x_ref, u, k, turn(k, 0, 0), turn(k, 1, 0)), store_sem.at[0, slot, k])

    def store_g(k, slot, w, layer):
        return pltpu.make_async_copy(out_g.at[slot, k], gs[w].at[layer, k], store_sem.at[1, slot, k])

    def stage_step(u):
        ks = range(COLOURS)
        load_second(n2, u)
        slot = lax.rem(u, 2)
        for k in ks:
            free(GATHER2, u, k)
            pl.when(u >= 2)(lambda: store_g(k, slot, 0, 0).wait())

            wait_second(n2, u, k)
            for one in state_of(k, 0, 0):
                one.wait()

            def adamw(c, _):
                r = pl.multiple_of(c * CHUNK, CHUNK)
                here = pl.ds(r, CHUNK)
                g = sum_second(n2, u, k, r)
                m, v = moments(m_v[k, here], v_v[k, here], g.astype(jnp.float32))
                out_w[slot, k, here] = new_weight(old_v[k, here].astype(jnp.float32), m, v)
                out_g[slot, k, here] = g
                return 0

            lax.fori_loop(0, rows // CHUNK, adamw, 0)
            remote(GATHER2, u, k, out_w.at[slot, k], block(x_ref, u, k, turn(k, 0, 0), turn(k, 1, 0)), 1).start()
            store_w(k, u, slot).start()

        def store_all(w, layer):
            for k in ks:
                store_g(k, slot, w, layer).start()

        of_weight(u, store_all)

    def stage_gather2(s, u):
        for k in range(COLOURS):
            if s == 1:
                store_w(k, u, lax.rem(u, 2)).wait()
            wait_recv(GATHER2 + s - 1, u, k)
            free(GATHER2 + s, u, k)
            it = block(x_ref, u, k, turn(k, 0, 0), turn(k, 1, -s))
            remote(GATHER2 + s, u, k, it, it, 1).start()

    def last_unit(k, it):
        early = rows - LATE
        z, late = zs[(weights - 1) * COLOURS + k], zs[weights * COLOURS + k]
        return (
            remote(stages - 1, units - 1, k, it.at[:, pl.ds(0, early)], z.at[:, pl.ds((layers - 1) * rows, early)], 0),
            pltpu.make_async_remote_copy(
                src_ref=it.at[:, pl.ds(early, LATE)],
                dst_ref=late,
                send_sem=late_sem.at[0, k],
                recv_sem=late_sem.at[1, k],
                device_id=neighbour(k, 0),
                device_id_type=MESH,
            ),
        )

    def stage_gather1(s, u):
        for k in range(COLOURS):
            wait_recv(GATHER1 + s - 1, u, k)
            free(GATHER1 + s, u, k)
            it = group(x_ref, u, k, turn(k, 0, -s))
            if s < n1 - 2:
                remote(GATHER1 + s, u, k, it, it, 0).start()
                continue
            for p in range(weights):
                z, layer = zs[p * COLOURS + k], u - p * layers
                mine = (layer >= 0) & (layer < (layers if p < weights - 1 else layers - 1))
                pl.when(mine)(lambda: remote(GATHER1 + s, u, k, it, z.at[:, pl.ds(layer * rows, rows)], 0).start())

            @pl.when(u == units - 1)
            def _():
                for copy in last_unit(k, it):
                    copy.start()

    def body(i, _):
        for s in range(FIRST + 1, STEP + 1):
            u = i - s
            pl.when((u >= 0) & (u < units))(functools.partial(prefetch, s, u))
        for s in range(stages):
            u = i - s
            run = (
                functools.partial(stage_first, s, u)
                if s < SECOND
                else functools.partial(stage_second, s - SECOND, u)
                if s < STEP
                else functools.partial(stage_step, u)
                if s == GATHER2
                else functools.partial(stage_gather2, s - GATHER2, u)
                if s < GATHER1
                else functools.partial(stage_gather1, s - GATHER1, u)
            )
            pl.when((u >= 0) & (u < units))(run)
        return 0

    ahead, behind = (0, 2), (1, 3)
    barrier = pltpu.get_barrier_semaphore()
    for k in behind:
        pl.semaphore_signal(barrier, inc=1, device_id=neighbour(k, 0), device_id_type=MESH)
    pl.semaphore_wait(barrier, len(behind))
    for k in ahead:
        pl.semaphore_signal(ready_sem.at[direction(k)[1]], inc=1, device_id=neighbour(k, 0), device_id_type=MESH)
    for k in (*ahead, *behind):
        if k in behind:
            pl.semaphore_wait(ready_sem.at[direction(k)[1]], 1)
        remote(FIRST, 0, k, group(grads[0], 0, k, turn(k, 0, -1)), land1.at[0, k, 0], 0).start()

    lax.fori_loop(0, stages - 1 + units, body, 0)

    def drain(u, _):
        for k in range(COLOURS):
            wait_recv(stages - 1, u, k)
        return 0

    lax.fori_loop(0, units - 1, drain, 0)
    for s in range(stages):
        for u in range(max(units - 2, 0), units - (s == stages - 1)):
            for k in range(COLOURS):
                wait_send(s, u, k)
    for k in range(COLOURS):
        for copy in last_unit(k, land1.at[0, k, 0]):
            copy.wait_recv()
            copy.wait_send()
    for u in range(max(units - 2, 0), units):
        for k in range(COLOURS):
            store_g(k, u % 2, 0, 0).wait()


def part_rows(weights, layers, rows):
    return (layers * rows,) * (weights - 1) + (layers * rows - LATE, LATE)


def communicate(side, grads, olds, ms, vs):
    layers = grads[0].shape[0]
    weights = len(grads)
    units = weights * layers
    rows = grads[0].shape[-2]
    hops = side - 1
    hbm = pl.BlockSpec(memory_space=pltpu.HBM)
    bf16, f32 = jnp.bfloat16, jnp.float32
    shape = pltpu.HBM
    outs = [
        shape((units, *grads[0].shape[1:]), bf16),
        *[shape((side, count, LANES), bf16) for count in part_rows(weights, layers, rows) for _ in range(COLOURS)],
        *[shape((layers, COLOURS, rows, LANES), bf16)] * weights,
        shape((units, COLOURS, hops, side, rows, LANES), bf16),
    ]
    stages = 4 * hops - 1
    scratch = [
        pltpu.VMEM((units, COLOURS, hops, rows, LANES), bf16),
        pltpu.VMEM((COLOURS, side, rows, LANES), bf16),
        pltpu.VMEM((hops - 1, COLOURS, side, rows, LANES), bf16),
        pltpu.VMEM((hops - 1, 2, COLOURS, side, rows, LANES), bf16),
        pltpu.VMEM((hops + 1, COLOURS, rows, LANES), bf16),
        pltpu.VMEM((hops + 1, COLOURS, rows, LANES), bf16),
        pltpu.VMEM((hops, 2, COLOURS, rows, LANES), bf16),
        pltpu.VMEM((COLOURS, rows, LANES), bf16),
        pltpu.VMEM((COLOURS, rows, LANES), f32),
        pltpu.VMEM((COLOURS, rows, LANES), f32),
        pltpu.VMEM((2, COLOURS, rows, LANES), bf16),
        pltpu.VMEM((2, COLOURS, rows, LANES), bf16),
        pltpu.SemaphoreType.DMA((stages, 2, COLOURS)),
        pltpu.SemaphoreType.DMA((stages, units, COLOURS)),
        pltpu.SemaphoreType.DMA((4, COLOURS)),
        pltpu.SemaphoreType.DMA((stages, COLOURS)),
        pltpu.SemaphoreType.DMA((hops + 1, COLOURS)),
        pltpu.SemaphoreType.DMA((2, 2, COLOURS)),
        pltpu.SemaphoreType.DMA((2, COLOURS)),
        pltpu.SemaphoreType.REGULAR((2,)),
    ]
    got = pl.pallas_call(
        functools.partial(comm_kernel, side, layers, units),
        out_shape=outs,
        in_specs=[hbm] * (4 * weights),
        out_specs=[hbm] * len(outs),
        scratch_shapes=scratch,
        compiler_params=pltpu.CompilerParams(collective_id=0, has_side_effects=True, vmem_limit_bytes=60 << 20),
        name="sum_step_gather",
    )(*(pinned(a, pltpu.HBM) for a in (*grads, *olds, *ms, *vs)))
    x, got = got[0], got[1:]
    zs, got = got[: (weights + 1) * COLOURS], got[(weights + 1) * COLOURS :]
    return x, [zs[i * COLOURS : (i + 1) * COLOURS] for i in range(weights + 1)], got[:weights]


SLOTS = 8


def copy_kernel(jobs, n_in, *refs):
    ins, (out, buf, in_sem, out_sem, straight_sem) = refs[:n_in], refs[-5:]
    pairs = jobs(ins, out)
    staged = [pair for pair in pairs if pair[2]]
    straight = [pltpu.make_async_copy(src, dst, straight_sem.at[i]) for i, (src, dst, _) in enumerate(p for p in pairs if not p[2])]

    def slot(i):
        shape = staged[i][0].shape
        return buf.at[i % SLOTS] if len(shape) == len(buf.shape) - 1 else buf.at[i % SLOTS, 0, :, pl.ds(0, shape[1])]

    def into(i):
        return pltpu.make_async_copy(staged[i][0], slot(i), in_sem.at[i % SLOTS])

    def outof(i):
        return pltpu.make_async_copy(slot(i), staged[i][1], out_sem.at[i % SLOTS])

    ahead = SLOTS // 2
    for copy in straight:
        copy.start()
    for i in range(len(staged) + ahead):
        if i < len(staged):
            if i >= SLOTS:
                outof(i - SLOTS).wait()
            into(i).start()
        if ahead <= i:
            into(i - ahead).wait()
            outof(i - ahead).start()
    for i in range(max(len(staged) - SLOTS, 0), len(staged)):
        outof(i).wait()
    for copy in straight:
        copy.wait()


def copies(jobs, ins, space, shape, moved, onto=None):
    hbm = pl.BlockSpec(memory_space=pltpu.HBM)
    side, rows = shape[1], shape[-2]
    given = [pinned(a, space) for a in ins] + ([] if onto is None else [pinned(onto, pltpu.HBM)])
    return pl.pallas_call(
        functools.partial(copy_kernel, jobs, len(ins)),
        out_shape=pltpu.HBM(shape, jnp.bfloat16),
        in_specs=[pl.BlockSpec(memory_space=space)] * len(ins) + [hbm] * (onto is not None),
        out_specs=hbm,
        scratch_shapes=[
            pltpu.VMEM((SLOTS if onto is None else 1, shape[0], side, rows, LANES), jnp.bfloat16),
            pltpu.SemaphoreType.DMA((SLOTS,)),
            pltpu.SemaphoreType.DMA((SLOTS,)),
            pltpu.SemaphoreType.DMA((SLOTS,)),
        ],
        input_output_aliases={} if onto is None else {len(ins): 0},
        compiler_params=pltpu.CompilerParams(vmem_limit_bytes=(16 if onto is None else 8) << 20),
        cost_estimate=pl.CostEstimate(flops=4 * moved, bytes_accessed=4 * moved, transcendentals=0),
        name="place" if onto is None else "place_last",
    )(*given)


def solution(mesh):
    n = mesh.shape["dp"]
    side = math.isqrt(n)
    hops = side - 1

    def ring(k):
        way, axis = direction(k)
        pairs = []
        for i in range(n):
            c = [i // side, i % side]
            c[axis] = (c[axis] + way) % side
            pairs.append((i, c[0] * side + c[1]))
        return pairs

    def group(ref, lead, k, back):
        way, axis = direction(k)
        first = lax.rem(place(side)[axis] - way * back + 4 * side, side)
        return ref.at[lead, first, :, k] if axis == 0 else ref.at[lead, :, first, k]

    def step(*arrays):
        terms, weights, m, v = (arrays[i : i + 3] for i in (0, 3, 6, 9))
        layers = m[0].shape[0]
        rows = m[0].shape[1] * m[0].shape[2] // LANES // COLOURS
        by_block = (layers, side, side, COLOURS, rows, LANES)
        grads = [flat(t[0]).reshape(by_block) for t in terms]
        olds = [flat(w).reshape(by_block) for w in weights]
        own_m, own_v = ([flat(one).reshape(layers, COLOURS, rows, LANES) for one in ones] for ones in (m, v))
        x, zs, sums = communicate(side, grads, olds, own_m, own_v)
        ys = [[lax.ppermute(z, "dp", ring(k)) for k, z in enumerate(part)] for part in zs]

        new_m, new_v = [], []
        for one_m, one_v, g in zip(m, v, sums, strict=True):
            g = unflat(g.reshape(layers, COLOURS * rows, LANES), *one_m.shape[1:]).astype(jnp.float32)
            a, b = moments(one_m, one_v, g)
            new_m.append(a)
            new_v.append(b)

        end = len(weights) - 1

        def pieces(p, part, out, k, back):
            pairs = []
            for layer in range(layers):
                here = group(out, layer, k, back)
                cut = rows - LATE if p >= end and layer == layers - 1 else rows
                if p <= end:
                    pairs.append((part.at[:, pl.ds(layer * rows, cut)], here.at[:, pl.ds(0, cut)]))
                elif cut < rows:
                    pairs.append((part, here.at[:, pl.ds(cut, LATE)]))
            return pairs

        whole = []
        for i in range(len(weights)):
            used = (i, i + 1) if i == end else (i,)

            def placed(ins, out, i=i, used=used):
                pairs = []
                for k in range(COLOURS):
                    for back in range(hops - 1):
                        here = group(out, pl.ds(0, layers), k, back)
                        pairs.append((group(ins[0], pl.ds(i * layers, layers), k, back), here, True))
                    for j, p in enumerate(used):
                        pairs += [(*pair, True) for pair in pieces(p, ins[1 + j * COLOURS + k], out, k, hops - 1)]
                return pairs

            ins = [x, *(z for p in used for z in zs[p])]
            whole.append(copies(placed, ins, pltpu.HBM, by_block, layers * n * COLOURS * rows * LANES))

        for p, count in enumerate(part_rows(len(weights), layers, rows)):
            if p > 0:
                ys[p], whole = lax.optimization_barrier((ys[p], whole))

            def last(ins, out, p=p):
                return [(*pair, False) for k in range(COLOURS) for pair in pieces(p, ins[k], out, k, hops)]

            i = min(p, end)
            whole[i] = copies(last, ys[p], pltpu.VMEM, by_block, COLOURS * side * count * LANES, onto=whole[i])
        whole = [unflat(one.reshape(layers, n * COLOURS * rows, LANES), *w.shape[1:]) for one, w in zip(whole, weights, strict=True)]
        return (*whole, *new_m, *new_v)

    all_of, cut = P(None, None, None), P(None, "dp", None)
    return jax.shard_map(
        step,
        mesh=mesh,
        in_specs=(P(("rep", "dp"), None, None, None),) * 3 + (all_of,) * 3 + (cut,) * 6,
        out_specs=(P("rep", None, None),) * 3 + (P("rep", "dp", None),) * 6,
        check_vma=False,
    )
```

```python
import functools
import math

import jax
import jax.numpy as jnp
from jax import lax
from jax.experimental import pallas as pl
from jax.experimental.pallas import tpu as pltpu
from jax.sharding import PartitionSpec as P

MESH = pl.DeviceIdType.MESH
LANES, SUBLANES = 128, 8
COLOURS = 4
CHUNK = 128
STAGGER_NS = 12000
LATE = 256


def flat(a):
    *lead, rows, columns = a.shape
    a = a.reshape(*lead, rows // SUBLANES, SUBLANES, columns // LANES, LANES)
    return jnp.swapaxes(a, -3, -2).reshape(*lead, rows * columns // LANES, LANES)


def unflat(a, rows, columns):
    *lead, _, _ = a.shape
    a = a.reshape(*lead, rows // SUBLANES, columns // LANES, SUBLANES, LANES)
    return jnp.swapaxes(a, -3, -2).reshape(*lead, rows, columns)


pinned = pltpu.with_memory_space_constraint


def moments(m, v, g):
    return 0.9 * m + 0.1 * g, 0.95 * v + 0.05 * g * g


def new_weight(w, m, v):
    step = m * lax.rsqrt(v + 1e-8) + 0.1 * w
    return (w - 0.02 * step).astype(jnp.bfloat16)


def direction(k):
    return (1 if k % 2 == 0 else -1), k // 2


def place(side):
    me = lax.axis_index("dp")
    return lax.div(me, side), lax.rem(me, side)


def at(k, first, second):
    return (first, second) if direction(k)[1] == 0 else (second, first)


def comm_kernel(side, layers, units, *refs):
    weights = units // layers
    grads, olds, ms, vs = (refs[i * weights : (i + 1) * weights] for i in range(4))
    refs = refs[4 * weights :]
    x_ref, refs = refs[0], refs[1:]
    parts = weights + 1
    zs, refs = refs[: parts * COLOURS], refs[parts * COLOURS :]
    gs, refs = refs[:weights], refs[weights:]
    (land1, land2, got, own1, out1, in2, own2, out2, old_v, m_v, v_v, out_w, out_g, *sems) = refs
    send_sem, recv_sem, load_sem, own_sem, sum_sem, store_sem, late_sem, ready_sem = sems
    rows = got.shape[2]
    last = side - 1
    xy = place(side)

    def turn(k, axis, by):
        way, first = direction(k)
        c = xy[first if axis == 0 else 1 - first]
        return lax.rem(c + way * by + 4 * side, side)

    def neighbour(k, axis):
        a, b = turn(k, 0, 1 if axis == 0 else 0), turn(k, 1, 1 if axis == 1 else 0)
        px, py = at(k, a, b)
        return {"dp": px * side + py}

    pl.when(lax.rem(lax.axis_index("rep"), 2) == 0)(lambda: pl.delay(STAGGER_NS))
    def of_weight(u, f):
        for w in range(weights):
            pl.when(lax.div(u, layers) == w)(functools.partial(f, w, lax.rem(u, layers)))

    def group(ref, lead, k, first):
        if direction(k)[1] == 0:
            return ref.at[lead, first, :, k]
        return ref.at[lead, :, first, k]

    def block(ref, lead, k, first, second):
        px, py = at(k, first, second)
        return ref.at[lead, px, py, k]

    def remote(stage, u, k, src, dst, axis):
        return pltpu.make_async_remote_copy(
            src_ref=src,
            dst_ref=dst,
            send_sem=send_sem.at[stage, lax.rem(u, 2), k],
            recv_sem=recv_sem.at[stage, u, k],
            device_id=neighbour(k, axis),
            device_id_type=MESH,
        )

    n1, n2 = last, last
    FIRST, SECOND, STEP = 0, n1, n1 + n2
    GATHER2, GATHER1 = STEP, STEP + n2
    stages = GATHER1 + n1 - 1

    def wait_recv(stage, u, k):
        if stage < SECOND:
            dst = land1.at[u, stage - FIRST, k]
        elif stage < STEP:
            dst = land2.at[u, k, stage - SECOND]
        elif stage < GATHER1:
            dst = block(x_ref, u, k, turn(k, 0, 0), turn(k, 1, -(stage - GATHER2) - 1))
        else:
            dst = group(x_ref, u, k, turn(k, 0, -(stage - GATHER1) - 1))
        remote(stage, u, k, dst, dst, 0).wait_recv()

    def wait_send(stage, u, k):
        small = SECOND <= stage < GATHER1
        ref = land2.at[0, k, 0] if small else land1.at[0, 0, k]
        remote(stage, u, k, ref, ref, 0).wait_send()

    def free(stage, u, k):
        pl.when(u >= 2)(lambda: wait_send(stage, u, k))

    def load(k, i, src, dst):
        return pltpu.make_async_copy(src, dst, load_sem.at[i, k])

    def own_of(stage, u, k, w, layer):
        if stage < SECOND:
            src, dst = group(grads[w], layer, k, turn(k, 0, -1 - (stage - FIRST))), own1.at[stage - FIRST - 1, k]
        else:
            src, dst = block(grads[w], layer, k, turn(k, 0, 0), turn(k, 1, -1 - (stage - SECOND))), own2.at[stage - SECOND, k]
        return pltpu.make_async_copy(src, dst, own_sem.at[stage, k])

    def sum_of(stage, u, k):
        s = stage - SECOND
        return pltpu.make_async_copy(land1.at[u, n1 - 1, k, turn(k, 1, -1 - s)], in2.at[s, k], sum_sem.at[s, k])

    def state_of(k, w, layer):
        return (
            load(k, 1, block(olds[w], layer, k, turn(k, 0, 0), turn(k, 1, 0)), old_v.at[k]),
            load(k, 2, ms[w].at[layer, k], m_v.at[k]),
            load(k, 3, vs[w].at[layer, k], v_v.at[k]),
        )

    def prefetch(stage, u):
        def start(w, layer):
            for k in range(COLOURS):
                own_of(stage, u, k, w, layer).start()
                if stage == STEP:
                    for one in state_of(k, w, layer):
                        one.start()

        of_weight(u, start)
        if stage > SECOND:
            for k in range(COLOURS):
                sum_of(stage, u, k).start()

    def stage_first(s, u):
        ks = range(COLOURS)
        if s == 0:

            def start(w, layer):
                for k in ks:
                    remote(FIRST, u, k, group(grads[w], layer, k, turn(k, 0, -1)), land1.at[u, 0, k], 0).start()

            for k in ks:
                free(FIRST, u, k)
            pl.when(u > 0)(lambda: of_weight(u, start))
            return

        for k in ks:
            wait_recv(FIRST + s - 1, u, k)
        arrived = pltpu.make_async_copy(land1.at[u, s - 1], got, load_sem.at[0, 0])
        arrived.start()
        arrived.wait()
        slot = lax.rem(u, 2)
        for k in ks:
            free(FIRST + s, u, k)
            own_of(FIRST + s, u, k, 0, 0).wait()
            out = out1.at[s - 1, slot, k]
            per = rows // CHUNK

            def add(c, _):
                j, r = lax.div(c, per), pl.multiple_of(lax.rem(c, per) * CHUNK, CHUNK)
                total = got[k, j, pl.ds(r, CHUNK)].astype(jnp.float32) + own1[s - 1, k, j, pl.ds(r, CHUNK)].astype(jnp.float32)
                out[j, pl.ds(r, CHUNK)] = total.astype(jnp.bfloat16)
                return 0

            lax.fori_loop(0, side * per, add, 0)
            remote(FIRST + s, u, k, out, land1.at[u, s, k], 0).start()

    def load_second(s, u):
        for k in range(COLOURS):
            wait_recv(SECOND + s - 1, u, k)
            if s == 0:
                sum_of(SECOND, u, k).start()

    def wait_second(s, u, k):
        own_of(SECOND + s, u, k, 0, 0).wait()
        sum_of(SECOND + s, u, k).wait()

    def sum_second(s, u, k, r):
        total = in2[s, k, pl.ds(r, CHUNK)].astype(jnp.float32) + own2[s, k, pl.ds(r, CHUNK)].astype(jnp.float32)
        if s > 0:
            total += land2[u, k, s - 1, pl.ds(r, CHUNK)].astype(jnp.float32)
        return total.astype(jnp.bfloat16)

    def stage_second(s, u):
        load_second(s, u)
        slot = lax.rem(u, 2)
        for k in range(COLOURS):
            free(SECOND + s, u, k)
            wait_second(s, u, k)
            out = out2.at[s, slot, k]

            def add(c, _):
                r = pl.multiple_of(c * CHUNK, CHUNK)
                out[pl.ds(r, CHUNK)] = sum_second(s, u, k, r)
                return 0

            lax.fori_loop(0, rows // CHUNK, add, 0)
            remote(SECOND + s, u, k, out, land2.at[u, k, s], 1).start()

    def store_w(k, u, slot):
        return pltpu.make_async_copy(out_w.at[slot, k], block(x_ref, u, k, turn(k, 0, 0), turn(k, 1, 0)), store_sem.at[0, slot, k])

    def store_g(k, slot, w, layer):
        return pltpu.make_async_copy(out_g.at[slot, k], gs[w].at[layer, k], store_sem.at[1, slot, k])

    def stage_step(u):
        ks = range(COLOURS)
        load_second(n2, u)
        slot = lax.rem(u, 2)
        for k in ks:
            free(GATHER2, u, k)
            pl.when(u >= 2)(lambda: store_g(k, slot, 0, 0).wait())

            wait_second(n2, u, k)
            for one in state_of(k, 0, 0):
                one.wait()

            def adamw(c, _):
                r = pl.multiple_of(c * CHUNK, CHUNK)
                here = pl.ds(r, CHUNK)
                g = sum_second(n2, u, k, r)
                m, v = moments(m_v[k, here], v_v[k, here], g.astype(jnp.float32))
                out_w[slot, k, here] = new_weight(old_v[k, here].astype(jnp.float32), m, v)
                out_g[slot, k, here] = g
                return 0

            lax.fori_loop(0, rows // CHUNK, adamw, 0)
            remote(GATHER2, u, k, out_w.at[slot, k], block(x_ref, u, k, turn(k, 0, 0), turn(k, 1, 0)), 1).start()
            store_w(k, u, slot).start()

        def store_all(w, layer):
            for k in ks:
                store_g(k, slot, w, layer).start()

        of_weight(u, store_all)

    def stage_gather2(s, u):
        for k in range(COLOURS):
            if s == 1:
                store_w(k, u, lax.rem(u, 2)).wait()
            wait_recv(GATHER2 + s - 1, u, k)
            free(GATHER2 + s, u, k)
            it = block(x_ref, u, k, turn(k, 0, 0), turn(k, 1, -s))
            remote(GATHER2 + s, u, k, it, it, 1).start()

    def last_unit(k, it):
        early = rows - LATE
        z, late = zs[(weights - 1) * COLOURS + k], zs[weights * COLOURS + k]
        return (
            remote(stages - 1, units - 1, k, it.at[:, pl.ds(0, early)], z.at[:, pl.ds((layers - 1) * rows, early)], 0),
            pltpu.make_async_remote_copy(
                src_ref=it.at[:, pl.ds(early, LATE)],
                dst_ref=late,
                send_sem=late_sem.at[0, k],
                recv_sem=late_sem.at[1, k],
                device_id=neighbour(k, 0),
                device_id_type=MESH,
            ),
        )

    def stage_gather1(s, u):
        for k in range(COLOURS):
            wait_recv(GATHER1 + s - 1, u, k)
            free(GATHER1 + s, u, k)
            it = group(x_ref, u, k, turn(k, 0, -s))
            if s < n1 - 2:
                remote(GATHER1 + s, u, k, it, it, 0).start()
                continue
            for p in range(weights):
                z, layer = zs[p * COLOURS + k], u - p * layers
                mine = (layer >= 0) & (layer < (layers if p < weights - 1 else layers - 1))
                pl.when(mine)(lambda: remote(GATHER1 + s, u, k, it, z.at[:, pl.ds(layer * rows, rows)], 0).start())

            @pl.when(u == units - 1)
            def _():
                for copy in last_unit(k, it):
                    copy.start()

    def body(i, _):
        for s in range(FIRST + 1, STEP + 1):
            u = i - s
            pl.when((u >= 0) & (u < units))(functools.partial(prefetch, s, u))
        for s in range(stages):
            u = i - s
            run = (
                functools.partial(stage_first, s, u)
                if s < SECOND
                else functools.partial(stage_second, s - SECOND, u)
                if s < STEP
                else functools.partial(stage_step, u)
                if s == GATHER2
                else functools.partial(stage_gather2, s - GATHER2, u)
                if s < GATHER1
                else functools.partial(stage_gather1, s - GATHER1, u)
            )
            pl.when((u >= 0) & (u < units))(run)
        return 0

    ahead, behind = (0, 2), (1, 3)
    barrier = pltpu.get_barrier_semaphore()
    for k in behind:
        pl.semaphore_signal(barrier, inc=1, device_id=neighbour(k, 0), device_id_type=MESH)
    pl.semaphore_wait(barrier, len(behind))
    for k in ahead:
        pl.semaphore_signal(ready_sem.at[direction(k)[1]], inc=1, device_id=neighbour(k, 0), device_id_type=MESH)
    for k in (*ahead, *behind):
        if k in behind:
            pl.semaphore_wait(ready_sem.at[direction(k)[1]], 1)
        remote(FIRST, 0, k, group(grads[0], 0, k, turn(k, 0, -1)), land1.at[0, 0, k], 0).start()

    lax.fori_loop(0, stages - 1 + units, body, 0)

    def drain(u, _):
        for k in range(COLOURS):
            wait_recv(stages - 1, u, k)
        return 0

    lax.fori_loop(0, units - 1, drain, 0)
    for s in range(stages):
        for u in range(max(units - 2, 0), units - (s == stages - 1)):
            for k in range(COLOURS):
                wait_send(s, u, k)
    for k in range(COLOURS):
        for copy in last_unit(k, land1.at[0, 0, k]):
            copy.wait_recv()
            copy.wait_send()
    for u in range(max(units - 2, 0), units):
        for k in range(COLOURS):
            store_g(k, u % 2, 0, 0).wait()


def part_rows(weights, layers, rows):
    return (layers * rows,) * (weights - 1) + (layers * rows - LATE, LATE)


def communicate(side, grads, olds, ms, vs):
    layers = grads[0].shape[0]
    weights = len(grads)
    units = weights * layers
    rows = grads[0].shape[-2]
    hops = side - 1
    hbm = pl.BlockSpec(memory_space=pltpu.HBM)
    bf16, f32 = jnp.bfloat16, jnp.float32
    shape = pltpu.HBM
    outs = [
        shape((units, *grads[0].shape[1:]), bf16),
        *[shape((side, count, LANES), bf16) for count in part_rows(weights, layers, rows) for _ in range(COLOURS)],
        *[shape((layers, COLOURS, rows, LANES), bf16)] * weights,
        shape((units, hops, COLOURS, side, rows, LANES), bf16),
    ]
    stages = 4 * hops - 1
    scratch = [
        pltpu.VMEM((units, COLOURS, hops, rows, LANES), bf16),
        pltpu.VMEM((COLOURS, side, rows, LANES), bf16),
        pltpu.VMEM((hops - 1, COLOURS, side, rows, LANES), bf16),
        pltpu.VMEM((hops - 1, 2, COLOURS, side, rows, LANES), bf16),
        pltpu.VMEM((hops + 1, COLOURS, rows, LANES), bf16),
        pltpu.VMEM((hops + 1, COLOURS, rows, LANES), bf16),
        pltpu.VMEM((hops, 2, COLOURS, rows, LANES), bf16),
        pltpu.VMEM((COLOURS, rows, LANES), bf16),
        pltpu.VMEM((COLOURS, rows, LANES), f32),
        pltpu.VMEM((COLOURS, rows, LANES), f32),
        pltpu.VMEM((2, COLOURS, rows, LANES), bf16),
        pltpu.VMEM((2, COLOURS, rows, LANES), bf16),
        pltpu.SemaphoreType.DMA((stages, 2, COLOURS)),
        pltpu.SemaphoreType.DMA((stages, units, COLOURS)),
        pltpu.SemaphoreType.DMA((4, COLOURS)),
        pltpu.SemaphoreType.DMA((stages, COLOURS)),
        pltpu.SemaphoreType.DMA((hops + 1, COLOURS)),
        pltpu.SemaphoreType.DMA((2, 2, COLOURS)),
        pltpu.SemaphoreType.DMA((2, COLOURS)),
        pltpu.SemaphoreType.REGULAR((2,)),
    ]
    got = pl.pallas_call(
        functools.partial(comm_kernel, side, layers, units),
        out_shape=outs,
        in_specs=[hbm] * (4 * weights),
        out_specs=[hbm] * len(outs),
        scratch_shapes=scratch,
        compiler_params=pltpu.CompilerParams(collective_id=0, has_side_effects=True, vmem_limit_bytes=60 << 20),
        name="sum_step_gather",
    )(*(pinned(a, pltpu.HBM) for a in (*grads, *olds, *ms, *vs)))
    x, got = got[0], got[1:]
    zs, got = got[: (weights + 1) * COLOURS], got[(weights + 1) * COLOURS :]
    return x, [zs[i * COLOURS : (i + 1) * COLOURS] for i in range(weights + 1)], got[:weights]


SLOTS = 8


def copy_kernel(jobs, n_in, *refs):
    ins, (out, buf, in_sem, out_sem, straight_sem) = refs[:n_in], refs[-5:]
    pairs = jobs(ins, out)
    staged = [pair for pair in pairs if pair[2]]
    straight = [pltpu.make_async_copy(src, dst, straight_sem.at[i]) for i, (src, dst, _) in enumerate(p for p in pairs if not p[2])]

    def slot(i):
        shape = staged[i][0].shape
        return buf.at[i % SLOTS] if len(shape) == len(buf.shape) - 1 else buf.at[i % SLOTS, 0, :, pl.ds(0, shape[1])]

    def into(i):
        return pltpu.make_async_copy(staged[i][0], slot(i), in_sem.at[i % SLOTS])

    def outof(i):
        return pltpu.make_async_copy(slot(i), staged[i][1], out_sem.at[i % SLOTS])

    ahead = SLOTS - 3
    for copy in straight:
        copy.start()
    for i in range(len(staged) + ahead):
        if i < len(staged):
            if i >= SLOTS:
                outof(i - SLOTS).wait()
            into(i).start()
        if ahead <= i:
            into(i - ahead).wait()
            outof(i - ahead).start()
    for i in range(max(len(staged) - SLOTS, 0), len(staged)):
        outof(i).wait()
    for copy in straight:
        copy.wait()


def copies(jobs, ins, space, shape, moved, onto=None):
    hbm = pl.BlockSpec(memory_space=pltpu.HBM)
    side, rows = shape[1], shape[-2]
    given = [pinned(a, space) for a in ins] + ([] if onto is None else [pinned(onto, pltpu.HBM)])
    return pl.pallas_call(
        functools.partial(copy_kernel, jobs, len(ins)),
        out_shape=pltpu.HBM(shape, jnp.bfloat16),
        in_specs=[pl.BlockSpec(memory_space=space)] * len(ins) + [hbm] * (onto is not None),
        out_specs=hbm,
        scratch_shapes=[
            pltpu.VMEM((SLOTS if onto is None else 1, shape[0], side, rows, LANES), jnp.bfloat16),
            pltpu.SemaphoreType.DMA((SLOTS,)),
            pltpu.SemaphoreType.DMA((SLOTS,)),
            pltpu.SemaphoreType.DMA((SLOTS,)),
        ],
        input_output_aliases={} if onto is None else {len(ins): 0},
        compiler_params=pltpu.CompilerParams(vmem_limit_bytes=(16 if onto is None else 8) << 20),
        cost_estimate=pl.CostEstimate(flops=4 * moved, bytes_accessed=4 * moved, transcendentals=0),
        name="place" if onto is None else "place_last",
    )(*given)


def solution(mesh):
    n = mesh.shape["dp"]
    side = math.isqrt(n)
    hops = side - 1

    def ring(k):
        way, axis = direction(k)
        pairs = []
        for i in range(n):
            c = [i // side, i % side]
            c[axis] = (c[axis] + way) % side
            pairs.append((i, c[0] * side + c[1]))
        return pairs

    def group(ref, lead, k, back):
        way, axis = direction(k)
        first = lax.rem(place(side)[axis] - way * back + 4 * side, side)
        return ref.at[lead, first, :, k] if axis == 0 else ref.at[lead, :, first, k]

    def step(*arrays):
        terms, weights, m, v = (arrays[i : i + 3] for i in (0, 3, 6, 9))
        layers = m[0].shape[0]
        rows = m[0].shape[1] * m[0].shape[2] // LANES // COLOURS
        by_block = (layers, side, side, COLOURS, rows, LANES)
        grads = [flat(t[0]).reshape(by_block) for t in terms]
        olds = [flat(w).reshape(by_block) for w in weights]
        own_m, own_v = ([flat(one).reshape(layers, COLOURS, rows, LANES) for one in ones] for ones in (m, v))
        x, zs, sums = communicate(side, grads, olds, own_m, own_v)
        ys = [[lax.ppermute(z, "dp", ring(k)) for k, z in enumerate(part)] for part in zs]

        new_m, new_v = [], []
        for one_m, one_v, g in zip(m, v, sums, strict=True):
            g = unflat(g.reshape(layers, COLOURS * rows, LANES), *one_m.shape[1:]).astype(jnp.float32)
            a, b = moments(one_m, one_v, g)
            new_m.append(a)
            new_v.append(b)

        end = len(weights) - 1

        def pieces(p, part, out, k, back):
            pairs = []
            for layer in range(layers):
                here = group(out, layer, k, back)
                cut = rows - LATE if p >= end and layer == layers - 1 else rows
                if p <= end:
                    pairs.append((part.at[:, pl.ds(layer * rows, cut)], here.at[:, pl.ds(0, cut)]))
                elif cut < rows:
                    pairs.append((part, here.at[:, pl.ds(cut, LATE)]))
            return pairs

        whole = []
        for i in range(len(weights)):
            used = (i, i + 1) if i == end else (i,)

            def placed(ins, out, i=i, used=used):
                pairs = []
                for k in range(COLOURS):
                    for back in range(hops - 1):
                        here = group(out, pl.ds(0, layers), k, back)
                        pairs.append((group(ins[0], pl.ds(i * layers, layers), k, back), here, True))
                    for j, p in enumerate(used):
                        pairs += [(*pair, True) for pair in pieces(p, ins[1 + j * COLOURS + k], out, k, hops - 1)]
                return pairs

            ins = [x, *(z for p in used for z in zs[p])]
            whole.append(copies(placed, ins, pltpu.HBM, by_block, layers * n * COLOURS * rows * LANES))

        for p, count in enumerate(part_rows(len(weights), layers, rows)):
            if p > 0:
                ys[p], whole = lax.optimization_barrier((ys[p], whole))

            def last(ins, out, p=p):
                return [(*pair, False) for k in range(COLOURS) for pair in pieces(p, ins[k], out, k, hops)]

            i = min(p, end)
            whole[i] = copies(last, ys[p], pltpu.VMEM, by_block, COLOURS * side * count * LANES, onto=whole[i])
        whole = [unflat(one.reshape(layers, n * COLOURS * rows, LANES), *w.shape[1:]) for one, w in zip(whole, weights, strict=True)]
        return (*whole, *new_m, *new_v)

    all_of, cut = P(None, None, None), P(None, "dp", None)
    return jax.shard_map(
        step,
        mesh=mesh,
        in_specs=(P(("rep", "dp"), None, None, None),) * 3 + (all_of,) * 3 + (cut,) * 6,
        out_specs=(P("rep", None, None),) * 3 + (P("rep", "dp", None),) * 6,
        check_vma=False,
    )
```

```python
import functools
import math

import jax
import jax.numpy as jnp
from jax import lax
from jax.experimental import pallas as pl
from jax.experimental.pallas import tpu as pltpu
from jax.sharding import PartitionSpec as P

MESH = pl.DeviceIdType.MESH
LANES, SUBLANES = 128, 8
COLOURS = 4
CHUNK = 128
STAGGER_NS = 12000
LATE = 256


def flat(a):
    *lead, rows, columns = a.shape
    a = a.reshape(*lead, rows // SUBLANES, SUBLANES, columns // LANES, LANES)
    return jnp.swapaxes(a, -3, -2).reshape(*lead, rows * columns // LANES, LANES)


def unflat(a, rows, columns):
    *lead, _, _ = a.shape
    a = a.reshape(*lead, rows // SUBLANES, columns // LANES, SUBLANES, LANES)
    return jnp.swapaxes(a, -3, -2).reshape(*lead, rows, columns)


pinned = pltpu.with_memory_space_constraint


def moments(m, v, g):
    return 0.9 * m + 0.1 * g, 0.95 * v + 0.05 * g * g


def new_weight(w, m, v):
    step = m * lax.rsqrt(v + 1e-8) + 0.1 * w
    return (w - 0.02 * step).astype(jnp.bfloat16)


def direction(k):
    return (1 if k % 2 == 0 else -1), k // 2


def place(side):
    me = lax.axis_index("dp")
    return lax.div(me, side), lax.rem(me, side)


def at(k, first, second):
    return (first, second) if direction(k)[1] == 0 else (second, first)


def comm_kernel(side, layers, units, *refs):
    weights = units // layers
    grads, olds, ms, vs = (refs[i * weights : (i + 1) * weights] for i in range(4))
    refs = refs[4 * weights :]
    x_ref, refs = refs[0], refs[1:]
    parts = weights + 1
    zs, refs = refs[: parts * COLOURS], refs[parts * COLOURS :]
    gs, refs = refs[:weights], refs[weights:]
    (land1, land2, got, own1, out1, in2, own2, out2, old_v, m_v, v_v, out_w, out_g, *sems) = refs
    send_sem, recv_sem, load_sem, own_sem, sum_sem, store_sem, late_sem, ready_sem = sems
    rows = got.shape[2]
    last = side - 1
    xy = place(side)

    def turn(k, axis, by):
        way, first = direction(k)
        c = xy[first if axis == 0 else 1 - first]
        return lax.rem(c + way * by + 4 * side, side)

    def neighbour(k, axis):
        a, b = turn(k, 0, 1 if axis == 0 else 0), turn(k, 1, 1 if axis == 1 else 0)
        px, py = at(k, a, b)
        return {"dp": px * side + py}

    pl.when(lax.rem(lax.axis_index("rep"), 2) == 0)(lambda: pl.delay(STAGGER_NS))
    def of_weight(u, f):
        for w in range(weights):
            pl.when(lax.div(u, layers) == w)(functools.partial(f, w, lax.rem(u, layers)))

    def group(ref, lead, k, first):
        if direction(k)[1] == 0:
            return ref.at[lead, first, :, k]
        return ref.at[lead, :, first, k]

    def block(ref, lead, k, first, second):
        px, py = at(k, first, second)
        return ref.at[lead, px, py, k]

    def remote(stage, u, k, src, dst, axis):
        return pltpu.make_async_remote_copy(
            src_ref=src,
            dst_ref=dst,
            send_sem=send_sem.at[stage, lax.rem(u, 2), k],
            recv_sem=recv_sem.at[stage, u, k],
            device_id=neighbour(k, axis),
            device_id_type=MESH,
        )

    n1, n2 = last, last
    FIRST, SECOND, STEP = 0, n1, n1 + n2
    GATHER2, GATHER1 = STEP, STEP + n2
    stages = GATHER1 + n1 - 1

    def wait_recv(stage, u, k):
        if stage < SECOND:
            dst = land1.at[u, stage - FIRST, k]
        elif stage < STEP:
            dst = land2.at[u, k, stage - SECOND]
        elif stage < GATHER1:
            dst = block(x_ref, u, k, turn(k, 0, 0), turn(k, 1, -(stage - GATHER2) - 1))
        else:
            dst = group(x_ref, u, k, turn(k, 0, -(stage - GATHER1) - 1))
        remote(stage, u, k, dst, dst, 0).wait_recv()

    def wait_send(stage, u, k):
        small = SECOND <= stage < GATHER1
        ref = land2.at[0, k, 0] if small else land1.at[0, 0, k]
        remote(stage, u, k, ref, ref, 0).wait_send()

    def free(stage, u, k):
        pl.when(u >= 2)(lambda: wait_send(stage, u, k))

    def load(k, i, src, dst):
        return pltpu.make_async_copy(src, dst, load_sem.at[i, k])

    def own_of(stage, u, k, w, layer):
        if stage < SECOND:
            src, dst = group(grads[w], layer, k, turn(k, 0, -1 - (stage - FIRST))), own1.at[stage - FIRST - 1, k]
        else:
            src, dst = block(grads[w], layer, k, turn(k, 0, 0), turn(k, 1, -1 - (stage - SECOND))), own2.at[stage - SECOND, k]
        return pltpu.make_async_copy(src, dst, own_sem.at[stage, k])

    def sum_of(stage, u, k):
        s = stage - SECOND
        return pltpu.make_async_copy(land1.at[u, n1 - 1, k, turn(k, 1, -1 - s)], in2.at[s, k], sum_sem.at[s, k])

    def state_of(k, w, layer):
        return (
            load(k, 1, block(olds[w], layer, k, turn(k, 0, 0), turn(k, 1, 0)), old_v.at[k]),
            load(k, 2, ms[w].at[layer, k], m_v.at[k]),
            load(k, 3, vs[w].at[layer, k], v_v.at[k]),
        )

    def prefetch(stage, u):
        def start(w, layer):
            for k in range(COLOURS):
                own_of(stage, u, k, w, layer).start()
                if stage == STEP:
                    for one in state_of(k, w, layer):
                        one.start()

        of_weight(u, start)
        if stage > SECOND:
            for k in range(COLOURS):
                sum_of(stage, u, k).start()

    def stage_first(s, u):
        ks = range(COLOURS)
        if s == 0:

            def start(w, layer):
                for k in ks:
                    remote(FIRST, u, k, group(grads[w], layer, k, turn(k, 0, -1)), land1.at[u, 0, k], 0).start()

            for k in ks:
                free(FIRST, u, k)
            pl.when(u > 0)(lambda: of_weight(u, start))
            return

        for k in ks:
            wait_recv(FIRST + s - 1, u, k)
        arrived = pltpu.make_async_copy(land1.at[u, s - 1], got, load_sem.at[0, 0])
        arrived.start()
        arrived.wait()
        slot = lax.rem(u, 2)
        for k in ks:
            free(FIRST + s, u, k)
            own_of(FIRST + s, u, k, 0, 0).wait()
            out = out1.at[s - 1, slot, k]
            per = rows // CHUNK

            def add(c, _):
                j, r = lax.div(c, per), pl.multiple_of(lax.rem(c, per) * CHUNK, CHUNK)
                total = got[k, j, pl.ds(r, CHUNK)].astype(jnp.float32) + own1[s - 1, k, j, pl.ds(r, CHUNK)].astype(jnp.float32)
                out[j, pl.ds(r, CHUNK)] = total.astype(jnp.bfloat16)
                return 0

            lax.fori_loop(0, side * per, add, 0)
            remote(FIRST + s, u, k, out, land1.at[u, s, k], 0).start()

    def load_second(s, u):
        for k in range(COLOURS):
            wait_recv(SECOND + s - 1, u, k)
            if s == 0:
                sum_of(SECOND, u, k).start()

    def wait_second(s, u, k):
        own_of(SECOND + s, u, k, 0, 0).wait()
        sum_of(SECOND + s, u, k).wait()

    def sum_second(s, u, k, r):
        total = in2[s, k, pl.ds(r, CHUNK)].astype(jnp.float32) + own2[s, k, pl.ds(r, CHUNK)].astype(jnp.float32)
        if s > 0:
            total += land2[u, k, s - 1, pl.ds(r, CHUNK)].astype(jnp.float32)
        return total.astype(jnp.bfloat16)

    def stage_second(s, u):
        load_second(s, u)
        slot = lax.rem(u, 2)
        for k in range(COLOURS):
            free(SECOND + s, u, k)
            wait_second(s, u, k)
            out = out2.at[s, slot, k]

            def add(c, _):
                r = pl.multiple_of(c * CHUNK, CHUNK)
                out[pl.ds(r, CHUNK)] = sum_second(s, u, k, r)
                return 0

            lax.fori_loop(0, rows // CHUNK, add, 0)
            remote(SECOND + s, u, k, out, land2.at[u, k, s], 1).start()

    def store_w(k, u, slot):
        return pltpu.make_async_copy(out_w.at[slot, k], block(x_ref, u, k, turn(k, 0, 0), turn(k, 1, 0)), store_sem.at[0, slot, k])

    def store_g(k, slot, w, layer):
        return pltpu.make_async_copy(out_g.at[slot, k], gs[w].at[layer, k], store_sem.at[1, slot, k])

    def stage_step(u):
        ks = range(COLOURS)
        load_second(n2, u)
        slot = lax.rem(u, 2)
        for k in ks:
            free(GATHER2, u, k)
            pl.when(u >= 2)(lambda: store_g(k, slot, 0, 0).wait())

            wait_second(n2, u, k)
            for one in state_of(k, 0, 0):
                one.wait()

            def adamw(c, _):
                r = pl.multiple_of(c * CHUNK, CHUNK)
                here = pl.ds(r, CHUNK)
                g = sum_second(n2, u, k, r)
                m, v = moments(m_v[k, here], v_v[k, here], g.astype(jnp.float32))
                out_w[slot, k, here] = new_weight(old_v[k, here].astype(jnp.float32), m, v)
                out_g[slot, k, here] = g
                return 0

            lax.fori_loop(0, rows // CHUNK, adamw, 0)
            remote(GATHER2, u, k, out_w.at[slot, k], block(x_ref, u, k, turn(k, 0, 0), turn(k, 1, 0)), 1).start()
            store_w(k, u, slot).start()

        def store_all(w, layer):
            for k in ks:
                store_g(k, slot, w, layer).start()

        of_weight(u, store_all)

    def stage_gather2(s, u):
        for k in range(COLOURS):
            if s == 1:
                store_w(k, u, lax.rem(u, 2)).wait()
            wait_recv(GATHER2 + s - 1, u, k)
            free(GATHER2 + s, u, k)
            it = block(x_ref, u, k, turn(k, 0, 0), turn(k, 1, -s))
            remote(GATHER2 + s, u, k, it, it, 1).start()

    def last_unit(k, it):
        early = rows - LATE
        z, late = zs[(weights - 1) * COLOURS + k], zs[weights * COLOURS + k]
        return (
            remote(stages - 1, units - 1, k, it.at[:, pl.ds(0, early)], z.at[:, pl.ds((layers - 1) * rows, early)], 0),
            pltpu.make_async_remote_copy(
                src_ref=it.at[:, pl.ds(early, LATE)],
                dst_ref=late,
                send_sem=late_sem.at[0, k],
                recv_sem=late_sem.at[1, k],
                device_id=neighbour(k, 0),
                device_id_type=MESH,
            ),
        )

    def stage_gather1(s, u):
        for k in range(COLOURS):
            wait_recv(GATHER1 + s - 1, u, k)
            free(GATHER1 + s, u, k)
            it = group(x_ref, u, k, turn(k, 0, -s))
            if s < n1 - 2:
                remote(GATHER1 + s, u, k, it, it, 0).start()
                continue
            for p in range(weights):
                z, layer = zs[p * COLOURS + k], u - p * layers
                mine = (layer >= 0) & (layer < (layers if p < weights - 1 else layers - 1))
                pl.when(mine)(lambda: remote(GATHER1 + s, u, k, it, z.at[:, pl.ds(layer * rows, rows)], 0).start())

            @pl.when(u == units - 1)
            def _():
                for copy in last_unit(k, it):
                    copy.start()

    def body(i, _):
        for s in range(FIRST + 1, STEP + 1):
            u = i - s
            pl.when((u >= 0) & (u < units))(functools.partial(prefetch, s, u))
        for s in range(stages):
            u = i - s
            run = (
                functools.partial(stage_first, s, u)
                if s < SECOND
                else functools.partial(stage_second, s - SECOND, u)
                if s < STEP
                else functools.partial(stage_step, u)
                if s == GATHER2
                else functools.partial(stage_gather2, s - GATHER2, u)
                if s < GATHER1
                else functools.partial(stage_gather1, s - GATHER1, u)
            )
            pl.when((u >= 0) & (u < units))(run)
        return 0

    ahead, behind = (0, 2), (1, 3)
    barrier = pltpu.get_barrier_semaphore()
    for k in reversed(behind):
        pl.semaphore_signal(barrier, inc=1, device_id=neighbour(k, 0), device_id_type=MESH)
    pl.semaphore_wait(barrier, len(behind))
    for k in reversed(ahead):
        pl.semaphore_signal(ready_sem.at[direction(k)[1]], inc=1, device_id=neighbour(k, 0), device_id_type=MESH)
    for k in (*ahead, *behind):
        if k in behind:
            pl.semaphore_wait(ready_sem.at[direction(k)[1]], 1)
        remote(FIRST, 0, k, group(grads[0], 0, k, turn(k, 0, -1)), land1.at[0, 0, k], 0).start()

    lax.fori_loop(0, stages - 1 + units, body, 0)

    def drain(u, _):
        for k in range(COLOURS):
            wait_recv(stages - 1, u, k)
        return 0

    lax.fori_loop(0, units - 1, drain, 0)
    for s in range(stages):
        for u in range(max(units - 2, 0), units - (s == stages - 1)):
            for k in range(COLOURS):
                wait_send(s, u, k)
    for k in range(COLOURS):
        for copy in last_unit(k, land1.at[0, 0, k]):
            copy.wait_recv()
            copy.wait_send()
    for u in range(max(units - 2, 0), units):
        for k in range(COLOURS):
            store_g(k, u % 2, 0, 0).wait()


def part_rows(weights, layers, rows):
    return (layers * rows,) * (weights - 1) + (layers * rows - LATE, LATE)


def communicate(side, grads, olds, ms, vs):
    layers = grads[0].shape[0]
    weights = len(grads)
    units = weights * layers
    rows = grads[0].shape[-2]
    hops = side - 1
    hbm = pl.BlockSpec(memory_space=pltpu.HBM)
    bf16, f32 = jnp.bfloat16, jnp.float32
    shape = pltpu.HBM
    outs = [
        shape((units, *grads[0].shape[1:]), bf16),
        *[shape((side, count, LANES), bf16) for count in part_rows(weights, layers, rows) for _ in range(COLOURS)],
        *[shape((layers, COLOURS, rows, LANES), bf16)] * weights,
        shape((units, hops, COLOURS, side, rows, LANES), bf16),
    ]
    stages = 4 * hops - 1
    scratch = [
        pltpu.VMEM((units, COLOURS, hops, rows, LANES), bf16),
        pltpu.VMEM((COLOURS, side, rows, LANES), bf16),
        pltpu.VMEM((hops - 1, COLOURS, side, rows, LANES), bf16),
        pltpu.VMEM((hops - 1, 2, COLOURS, side, rows, LANES), bf16),
        pltpu.VMEM((hops + 1, COLOURS, rows, LANES), bf16),
        pltpu.VMEM((hops + 1, COLOURS, rows, LANES), bf16),
        pltpu.VMEM((hops, 2, COLOURS, rows, LANES), bf16),
        pltpu.VMEM((COLOURS, rows, LANES), bf16),
        pltpu.VMEM((COLOURS, rows, LANES), f32),
        pltpu.VMEM((COLOURS, rows, LANES), f32),
        pltpu.VMEM((2, COLOURS, rows, LANES), bf16),
        pltpu.VMEM((2, COLOURS, rows, LANES), bf16),
        pltpu.SemaphoreType.DMA((stages, 2, COLOURS)),
        pltpu.SemaphoreType.DMA((stages, units, COLOURS)),
        pltpu.SemaphoreType.DMA((4, COLOURS)),
        pltpu.SemaphoreType.DMA((stages, COLOURS)),
        pltpu.SemaphoreType.DMA((hops + 1, COLOURS)),
        pltpu.SemaphoreType.DMA((2, 2, COLOURS)),
        pltpu.SemaphoreType.DMA((2, COLOURS)),
        pltpu.SemaphoreType.REGULAR((2,)),
    ]
    got = pl.pallas_call(
        functools.partial(comm_kernel, side, layers, units),
        out_shape=outs,
        in_specs=[hbm] * (4 * weights),
        out_specs=[hbm] * len(outs),
        scratch_shapes=scratch,
        compiler_params=pltpu.CompilerParams(collective_id=0, has_side_effects=True, vmem_limit_bytes=60 << 20),
        name="sum_step_gather",
    )(*(pinned(a, pltpu.HBM) for a in (*grads, *olds, *ms, *vs)))
    x, got = got[0], got[1:]
    zs, got = got[: (weights + 1) * COLOURS], got[(weights + 1) * COLOURS :]
    return x, [zs[i * COLOURS : (i + 1) * COLOURS] for i in range(weights + 1)], got[:weights]


SLOTS = 8


def copy_kernel(jobs, n_in, *refs):
    ins, (out, buf, in_sem, out_sem, straight_sem) = refs[:n_in], refs[-5:]
    pairs = jobs(ins, out)
    staged = [pair for pair in pairs if pair[2]]
    straight = [pltpu.make_async_copy(src, dst, straight_sem.at[i]) for i, (src, dst, _) in enumerate(p for p in pairs if not p[2])]

    def slot(i):
        shape = staged[i][0].shape
        return buf.at[i % SLOTS] if len(shape) == len(buf.shape) - 1 else buf.at[i % SLOTS, 0, :, pl.ds(0, shape[1])]

    def into(i):
        return pltpu.make_async_copy(staged[i][0], slot(i), in_sem.at[i % SLOTS])

    def outof(i):
        return pltpu.make_async_copy(slot(i), staged[i][1], out_sem.at[i % SLOTS])

    ahead = SLOTS - 3
    for copy in straight:
        copy.start()
    for i in range(len(staged) + ahead):
        if i < len(staged):
            if i >= SLOTS:
                outof(i - SLOTS).wait()
            into(i).start()
        if ahead <= i:
            into(i - ahead).wait()
            outof(i - ahead).start()
    for i in range(max(len(staged) - SLOTS, 0), len(staged)):
        outof(i).wait()
    for copy in straight:
        copy.wait()


def copies(jobs, ins, space, shape, moved, onto=None):
    hbm = pl.BlockSpec(memory_space=pltpu.HBM)
    side, rows = shape[1], shape[-2]
    given = [pinned(a, space) for a in ins] + ([] if onto is None else [pinned(onto, pltpu.HBM)])
    return pl.pallas_call(
        functools.partial(copy_kernel, jobs, len(ins)),
        out_shape=pltpu.HBM(shape, jnp.bfloat16),
        in_specs=[pl.BlockSpec(memory_space=space)] * len(ins) + [hbm] * (onto is not None),
        out_specs=hbm,
        scratch_shapes=[
            pltpu.VMEM((SLOTS if onto is None else 1, shape[0], side, rows, LANES), jnp.bfloat16),
            pltpu.SemaphoreType.DMA((SLOTS,)),
            pltpu.SemaphoreType.DMA((SLOTS,)),
            pltpu.SemaphoreType.DMA((SLOTS,)),
        ],
        input_output_aliases={} if onto is None else {len(ins): 0},
        compiler_params=pltpu.CompilerParams(vmem_limit_bytes=(16 if onto is None else 8) << 20),
        cost_estimate=pl.CostEstimate(flops=4 * moved, bytes_accessed=4 * moved, transcendentals=0),
        name="place" if onto is None else "place_last",
    )(*given)


def solution(mesh):
    n = mesh.shape["dp"]
    side = math.isqrt(n)
    hops = side - 1

    def ring(k):
        way, axis = direction(k)
        pairs = []
        for i in range(n):
            c = [i // side, i % side]
            c[axis] = (c[axis] + way) % side
            pairs.append((i, c[0] * side + c[1]))
        return pairs

    def group(ref, lead, k, back):
        way, axis = direction(k)
        first = lax.rem(place(side)[axis] - way * back + 4 * side, side)
        return ref.at[lead, first, :, k] if axis == 0 else ref.at[lead, :, first, k]

    def step(*arrays):
        terms, weights, m, v = (arrays[i : i + 3] for i in (0, 3, 6, 9))
        layers = m[0].shape[0]
        rows = m[0].shape[1] * m[0].shape[2] // LANES // COLOURS
        by_block = (layers, side, side, COLOURS, rows, LANES)
        grads = [flat(t[0]).reshape(by_block) for t in terms]
        olds = [flat(w).reshape(by_block) for w in weights]
        own_m, own_v = ([flat(one).reshape(layers, COLOURS, rows, LANES) for one in ones] for ones in (m, v))
        x, zs, sums = communicate(side, grads, olds, own_m, own_v)
        ys = [[lax.ppermute(z, "dp", ring(k)) for k, z in enumerate(part)] for part in zs]

        new_m, new_v = [], []
        for one_m, one_v, g in zip(m, v, sums, strict=True):
            g = unflat(g.reshape(layers, COLOURS * rows, LANES), *one_m.shape[1:]).astype(jnp.float32)
            a, b = moments(one_m, one_v, g)
            new_m.append(a)
            new_v.append(b)

        end = len(weights) - 1

        def pieces(p, part, out, k, back):
            pairs = []
            for layer in range(layers):
                here = group(out, layer, k, back)
                cut = rows - LATE if p >= end and layer == layers - 1 else rows
                if p <= end:
                    pairs.append((part.at[:, pl.ds(layer * rows, cut)], here.at[:, pl.ds(0, cut)]))
                elif cut < rows:
                    pairs.append((part, here.at[:, pl.ds(cut, LATE)]))
            return pairs

        whole = []
        for i in range(len(weights)):
            used = (i, i + 1) if i == end else (i,)

            def placed(ins, out, i=i, used=used):
                pairs = []
                for k in range(COLOURS):
                    for back in range(hops - 1):
                        here = group(out, pl.ds(0, layers), k, back)
                        pairs.append((group(ins[0], pl.ds(i * layers, layers), k, back), here, True))
                    for j, p in enumerate(used):
                        pairs += [(*pair, True) for pair in pieces(p, ins[1 + j * COLOURS + k], out, k, hops - 1)]
                return pairs

            ins = [x, *(z for p in used for z in zs[p])]
            whole.append(copies(placed, ins, pltpu.HBM, by_block, layers * n * COLOURS * rows * LANES))

        for p, count in enumerate(part_rows(len(weights), layers, rows)):
            if p > 0:
                ys[p], whole = lax.optimization_barrier((ys[p], whole))

            def last(ins, out, p=p):
                return [(*pair, False) for k in range(COLOURS) for pair in pieces(p, ins[k], out, k, hops)]

            i = min(p, end)
            whole[i] = copies(last, ys[p], pltpu.VMEM, by_block, COLOURS * side * count * LANES, onto=whole[i])
        whole = [unflat(one.reshape(layers, n * COLOURS * rows, LANES), *w.shape[1:]) for one, w in zip(whole, weights, strict=True)]
        return (*whole, *new_m, *new_v)

    all_of, cut = P(None, None, None), P(None, "dp", None)
    return jax.shard_map(
        step,
        mesh=mesh,
        in_specs=(P(("rep", "dp"), None, None, None),) * 3 + (all_of,) * 3 + (cut,) * 6,
        out_specs=(P("rep", None, None),) * 3 + (P("rep", "dp", None),) * 6,
        check_vma=False,
    )
```
